32 devices in a mesh: fsdp: 2 (over core), ctx: 4 (over y, x), tp: 4 (over z).
Axes of the slice: x: 2, y: 2, z: 4, core: 2. Of those that a mesh axis runs over, the one named last changes fastest.
Arguments:
- tokens_in: bfloat16 [4, 2048, 768], P(None, ('fsdp', 'ctx', 'tp')), may hold values from -6 to 6
- cotangent: bfloat16 [4, 2048, 768], P(None, ('fsdp', 'ctx', 'tp')), may hold values from -6 to 6
- seq_lengths: int32 [4, 2, 3], P(None, 'fsdp'), may hold values from 1 to 512, 1024 in all within a row
- row_order: int32 [4, 2, 1024], P(None, 'fsdp'), may hold values from 0 to 1023, each once within a row
- w_query: bfloat16 [768, 768], P(('fsdp', 'ctx'), 'tp'), may hold values from -0.3125 to 0.3125
- b_query: bfloat16 [12, 64], P('tp', ('fsdp', 'ctx')), may hold values from -3 to 3
- w_key: bfloat16 [768, 768], P(('fsdp', 'ctx'), 'tp'), may hold values from -0.3125 to 0.3125
- w_value: bfloat16 [768, 768], P(('fsdp', 'ctx'), 'tp'), may hold values from -0.21875 to 0.21875
- b_value: bfloat16 [12, 64], P('tp', ('fsdp', 'ctx')), may hold values from -3 to 3
- w_out: bfloat16 [768, 768], P(('fsdp', 'ctx'), 'tp'), may hold values from -1 to 1
- b_out: bfloat16 [768], P(('fsdp', 'ctx')), may hold values from -3 to 3
- mid_gain: bfloat16 [768], P(('fsdp', 'ctx')), may hold values from 0.099609375 to 1.8984375
- mid_shift: bfloat16 [768], P(('fsdp', 'ctx')), may hold values from -3 to 3
- w_up: bfloat16 [768, 3072], P(('fsdp', 'ctx'), 'tp'), may hold values from -0.21875 to 0.21875
- b_up: bfloat16 [12, 256], P('tp', ('fsdp', 'ctx')), may hold values from -3 to 3
- w_down: bfloat16 [768, 3072], P(('fsdp', 'ctx'), 'tp'), may hold values from -0.15625 to 0.15625
- b_down: bfloat16 [768], P(('fsdp', 'ctx')), may hold values from -3 to 3
- end_gain: bfloat16 [768], P(('fsdp', 'ctx')), may hold values from 0.099609375 to 1.8984375
- end_shift: bfloat16 [768], P(('fsdp', 'ctx')), may hold values from -3 to 3
Outputs:
- layer_out: bfloat16 [4, 2048, 768], P(None, ('fsdp', 'ctx', 'tp'))
- input_grad: bfloat16 [4, 2048, 768], P(None, ('fsdp', 'ctx', 'tp'))
- grad_w_query: float32 [768, 768], P(('fsdp', 'ctx'), 'tp')
- grad_b_query: float32 [12, 64], P('tp', ('fsdp', 'ctx'))
- grad_w_key: float32 [768, 768], P(('fsdp', 'ctx'), 'tp')
- grad_w_value: float32 [768, 768], P(('fsdp', 'ctx'), 'tp')
- grad_b_value: float32 [12, 64], P('tp', ('fsdp', 'ctx'))
- grad_w_out: float32 [768, 768], P(('fsdp', 'ctx'), 'tp')
- grad_b_out: float32 [768], P(('fsdp', 'ctx'))
- grad_mid_gain: float32 [768], P(('fsdp', 'ctx'))
- grad_mid_shift: float32 [768], P(('fsdp', 'ctx'))
- grad_w_up: float32 [768, 3072], P(('fsdp', 'ctx'), 'tp')
- grad_b_up: float32 [12, 256], P('tp', ('fsdp', 'ctx'))
- grad_w_down: float32 [768, 3072], P(('fsdp', 'ctx'), 'tp')
- grad_b_down: float32 [768], P(('fsdp', 'ctx'))
- grad_end_gain: float32 [768], P(('fsdp', 'ctx'))
- grad_end_shift: float32 [768], P(('fsdp', 'ctx'))
The draws below stay inside these ranges and needn't reach their ends.
Inputs may be any that keep to these rules, and one draw needn't show every extreme that they name: `seq_lengths`: each row of 3 lengths sums to 1024, and its largest is exactly 512. `row_order`: each row holds every number of 0 to 1023 once.
All inputs are finite; a program needn't handle non-finite values.
Results may differ from the reference program's by a relative error of at most 0.02.
Values may be sent and summed in bfloat16 or wider, within the bound.
A program may use at most 128 MiB of HBM per device.

```python
import math
import jax
import jax.numpy as jnp
import numpy as np
from jax import lax

D = 768
H = 12
HD = 64
FF = 3072
MB = 4
NSEQ = 3
GROUP = 1024
SEQ_MAX = 512
TOKENS = 2048
HHD = 768
N_FSDP = 2


def block_levels(rng, extent, pieces, least, largest):
    factor_of, own = 1.0, jax.random.fold_in(rng, 6)
    for dim, blocks in pieces:
        steps = jnp.exp(jax.random.uniform(jax.random.fold_in(own, dim), (blocks,), jnp.float32, least / len(pieces), largest / len(pieces)))
        factor_of = factor_of * jnp.repeat(steps, extent[dim] // blocks).reshape([-1 if axis == dim else 1 for axis in range(len(extent))])
    return factor_of


def length_profile(number_of, total, most, lean):
    weights = [(1 << 20) // math.isqrt(grade ** lean) + 1 for grade in range(2, number_of + 1)]
    spare, holding = total - most - (number_of - 1), [1] * (number_of - 1)
    while spare > 0:
        candidates = [i for i in range(number_of - 1) if holding[i] < most]
        mass, budget = sum([weights[i] for i in candidates]), spare
        for i in candidates:
            addition = min(most - holding[i], max(1, budget * weights[i] // mass), spare)
            holding[i] = holding[i] + addition
            spare = spare - addition
    return np.array([most] + holding)


def uneven_parts(own_key, amount, total, most, slope):
    if amount == 2:
        one = jax.random.randint(own_key, (), max(1, total - most), min(most, total - 1) + 1)
        return jnp.stack([one, total - one])
    tallies = jnp.asarray(length_profile(amount, total, most, slope), jnp.int32)
    pairs = (amount - 1) // 2
    source_of, receiver = tallies[1:1 + 2 * pairs:2], tallies[2:2 + 2 * pairs:2]
    room = jnp.minimum(source_of - 1, most - receiver)
    shifted = jax.random.randint(jax.random.fold_in(own_key, 1), (pairs,), 0, 1 << 20) % (room + 1)
    tallies = tallies.at[1:1 + 2 * pairs:2].set(source_of - shifted).at[2:2 + 2 * pairs:2].set(receiver + shifted)
    return tallies[jax.random.permutation(jax.random.fold_in(own_key, 2), amount)]


def noise(key, extent, scale, limit, pieces=(), dtype=jnp.bfloat16):
    loudness = block_levels(key, extent, pieces, -0.22, 0.18) if pieces else 1.0
    values = jax.random.normal(key, extent, jnp.float32) * scale * loudness
    return jnp.minimum(jnp.maximum(values, -limit), limit).astype(dtype)


def setup_inputs(seed: int = 0) -> dict:
    splits = jax.random.split(jax.random.key(seed), 20)
    return {
        "tokens_in": noise(splits[0], (MB, TOKENS, D), 1.0, 6.0, ((1, 32),)),
        "cotangent": noise(splits[1], (MB, TOKENS, D), 1.0, 6.0, ((1, 32),)),
        "seq_lengths": jax.vmap(lambda own: uneven_parts(own, NSEQ, GROUP, SEQ_MAX, 1))(jax.random.split(splits[2], MB * N_FSDP)).reshape((MB, N_FSDP, NSEQ)).astype(jnp.int32),
        "row_order": jax.vmap(lambda own: jax.random.permutation(own, GROUP))(jax.random.split(splits[3], MB * N_FSDP)).reshape((MB, N_FSDP, GROUP)).astype(jnp.int32),
        "w_query": noise(splits[4], (D, HHD), (D // 2) ** -0.5, 0.3125, ((0, 8), (1, 4))),
        "b_query": noise(splits[5], (H, HD), 0.5, 3.0, ((0, 4), (1, 8))),
        "w_key": noise(splits[6], (D, HHD), (D // 2) ** -0.5, 0.3125, ((0, 8), (1, 4))),
        "w_value": noise(splits[7], (D, HHD), D ** -0.5, 0.21875, ((0, 8), (1, 4))),
        "b_value": noise(splits[8], (H, HD), 0.5, 3.0, ((0, 4), (1, 8))),
        "w_out": noise(splits[9], (D, HHD), (HD // 2) ** -0.5, 1.0, ((0, 8), (1, 4))),
        "b_out": noise(splits[10], (D,), 0.5, 3.0, ((0, 8),)),
        "mid_gain": jnp.clip(1.0 + 0.18 * jax.random.normal(splits[11], (D,), jnp.float32), 0.099609375, 1.8984375).astype(jnp.bfloat16),
        "mid_shift": noise(splits[12], (D,), 0.5, 3.0, ((0, 8),)),
        "w_up": noise(splits[13], (D, FF), D ** -0.5, 0.21875, ((0, 8), (1, 4))),
        "b_up": noise(splits[14], (H, FF // H), 0.5, 3.0, ((0, 4), (1, 8))),
        "w_down": noise(splits[15], (D, FF), (FF // 2) ** -0.5, 0.15625, ((0, 8), (1, 4))),
        "b_down": noise(splits[16], (D,), 0.5, 3.0, ((0, 8),)),
        "end_gain": jnp.clip(1.0 + 0.18 * jax.random.normal(splits[17], (D,), jnp.float32), 0.099609375, 1.8984375).astype(jnp.bfloat16),
        "end_shift": noise(splits[18], (D,), 0.5, 3.0, ((0, 8),)),
    }


epsilon = 1e-06
masked_score = -1e+30

@jax.custom_vjp
def low(v):
    return lax.optimization_barrier(v.astype(jnp.bfloat16)).astype(jnp.float32)

@jax.custom_vjp
def low_back(v):
    return v

def low_keep(v):
    return (low(v), None)

def low_pass(kept, grad):
    return (grad,)

def back_keep(v):
    return (v, None)

def back_low(kept, grad):
    return (low(grad),)
low.defvjp(low_keep, low_pass)
low_back.defvjp(back_keep, back_low)

def highest(former, latter):
    return jnp.dot(former, latter, precision=lax.Precision.HIGHEST, preferred_element_type=jnp.float32)

def layer_norm(values, gain_vec, shift_vec):
    centre = values - lax.optimization_barrier(jnp.mean(values, axis=-1, keepdims=True))
    spread = lax.optimization_barrier(jnp.mean(centre * centre, axis=-1, keepdims=True))
    return centre * lax.rsqrt(spread + epsilon) * gain_vec + shift_vec

def segment_ids(lengths, row_count):
    run_ends = jnp.cumsum(lengths)
    places = lax.iota(jnp.int32, row_count)
    return lax.optimization_barrier(jnp.sum((run_ends[None, :] <= places[:, None]).astype(jnp.int32), axis=1))

def group_forward(params, inputs):
    tokens, lengths, row_perm = inputs
    query_w, query_b, key_w, value_w, value_b, out_w, out_b, gain_mid, shift_mid, up_w, up_b, down_w, down_b, gain_end, shift_end = params
    group_rows = tokens.shape[0]
    head_count = query_b.shape[0]
    head_size = query_b.shape[1]
    segments = segment_ids(lengths, group_rows)
    same_seq = segments[:, None] == segments[None, :]
    queries = low(low_back(highest(tokens, query_w) + query_b.reshape(-1)))
    key_rows = low(low_back(highest(tokens, key_w)))
    value_rows = low(low_back(highest(tokens, value_w) + value_b.reshape(-1)))

    def split_heads(array):
        return array.reshape(group_rows, head_count, head_size).transpose(1, 0, 2)

    def one_head(triple):
        query_head, key_head, value_head = triple
        scores = low_back(highest(query_head, key_head.T) * 0.125)
        scores = jnp.where(same_seq, scores, masked_score)
        top_score = lax.optimization_barrier(jnp.max(scores, axis=-1, keepdims=True))
        expd = jnp.exp(scores - top_score)
        probs = expd / lax.optimization_barrier(jnp.sum(expd, axis=-1, keepdims=True))
        return highest(low(probs), value_head)
    attended = lax.map(jax.checkpoint(one_head), (split_heads(queries), split_heads(key_rows), split_heads(value_rows)))
    attended = attended.transpose(1, 0, 2).reshape(group_rows, head_count * head_size)
    attended = low(low_back(attended))
    middle = layer_norm(tokens + low_back(highest(attended, out_w.T)) + out_b, gain_mid, shift_mid)
    pre_act = low_back(highest(low(middle), up_w) + up_b.reshape(-1))
    activated = low(jax.nn.gelu(pre_act, approximate=False))
    result = layer_norm(middle + low_back(highest(activated, down_w.T)) + down_b, gain_end, shift_end)
    return jnp.take(result, row_perm, axis=0)

def reference(tokens_in, cotangent, seq_lengths, row_order, w_query, b_query, w_key, w_value, b_value, w_out, b_out, mid_gain, mid_shift, w_up, b_up, w_down, b_down, end_gain, end_shift):
    groups = MB * N_FSDP
    tokens = tokens_in.astype(jnp.float32).reshape(groups, GROUP, D)
    lengths = seq_lengths.reshape(groups, NSEQ)
    perms = row_order.reshape(groups, GROUP)
    params = tuple((member.astype(jnp.float32) for member in (w_query, b_query, w_key, w_value, b_value, w_out, b_out, mid_gain, mid_shift, w_up, b_up, w_down, b_down, end_gain, end_shift)))

    def forward(token_arr, param_set):

        def one_group(item):
            return jax.checkpoint(group_forward)(param_set, item)
        return lax.map(one_group, (token_arr, lengths, perms))
    outputs, pullback = jax.vjp(forward, tokens, params)
    grad_tokens, grads = pullback(cotangent.astype(jnp.float32).reshape(groups, GROUP, D))
    return (outputs.reshape(MB, TOKENS, D).astype(jnp.bfloat16), grad_tokens.reshape(MB, TOKENS, D).astype(jnp.bfloat16), grads[0], grads[1], grads[2], grads[3], grads[4], grads[5], grads[6], grads[7], grads[8], grads[9], grads[10], grads[11], grads[12], grads[13], grads[14])
```

```python
import jax
import jax.numpy as jnp
from jax import lax
from jax.sharding import PartitionSpec as P

EPS = 1e-06
MASKED = -1e30
ALL = ("fsdp", "ctx", "tp")
ROWS = ("fsdp", "ctx")
BF = jnp.bfloat16
F32 = jnp.float32


def mm(a, b):
    return jnp.dot(a, b, preferred_element_type=F32)


def mm_rt(a, b):
    return lax.dot_general(a, b, (((1,), (1,)), ((), ())), preferred_element_type=F32)


def mm_lt(a, b):
    return lax.dot_general(a, b, (((0,), (0,)), ((), ())), preferred_element_type=F32)


def norm(u):
    centre = u - jnp.mean(u, axis=-1, keepdims=True)
    inv = lax.rsqrt(jnp.mean(centre * centre, axis=-1, keepdims=True) + EPS)
    return centre * inv, inv


def norm_back(d, gain, n, inv):
    e = d * gain
    return (e - jnp.mean(e, axis=-1, keepdims=True) - n * jnp.mean(e * n, axis=-1, keepdims=True)) * inv


def phi_both(u):
    cdf = 0.5 * (1.0 + lax.erf(u * 0.7071067811865476))
    pdf = 0.3989422804014327 * jnp.exp(-0.5 * u * u)
    return cdf, pdf


def gather_group(block):
    width = block.shape[-1]
    mine = lax.all_to_all(block, "ctx", 0, 0, tiled=True)
    whole = lax.all_gather(mine, "tp", axis=1, tiled=False)
    return whole.reshape(-1, width)


def scatter_group(rows, own_rows):
    ctx_n, tp_n = lax.axis_size("ctx"), lax.axis_size("tp")
    width = rows.shape[-1]
    blocks = rows.reshape(ctx_n, tp_n * own_rows, width)
    mine = lax.psum_scatter(blocks, "tp", scatter_dimension=1, tiled=True)
    return lax.all_to_all(mine, "ctx", 0, 0, tiled=True)


def body(tokens_in, cotangent, seq_lengths, row_order, w_query, b_query, w_key, w_value, b_value,
         w_out, b_out, mid_gain, mid_shift, w_up, b_up, w_down, b_down, end_gain, end_shift):
    ctx_n, tp_n, fsdp_n = lax.axis_size("ctx"), lax.axis_size("tp"), lax.axis_size("fsdp")
    rows_n = ctx_n * fsdp_n
    c, t = lax.axis_index("ctx"), lax.axis_index("tp")
    micro, own_rows, width = tokens_in.shape
    group_rows = own_rows * ctx_n * tp_n
    half_rows = group_rows // 2
    parts = tp_n // 2
    my_rows = half_rows // parts
    half, quarter = t // parts, t % parts
    heads_l, head_l = b_query.shape
    heads, head = heads_l * tp_n, head_l * rows_n

    mats = (w_query, w_key, w_value, w_out, w_up, w_down)
    widths = [m.shape[1] for m in mats]
    packed = lax.all_gather(jnp.concatenate(mats, axis=1), ALL, axis=0, tiled=False)
    full, at = [], 0
    for wd in widths:
        piece = packed[:, :, at:at + wd].reshape(rows_n, tp_n, -1, wd)
        full.append(piece.transpose(0, 2, 1, 3).reshape(width, tp_n * wd))
        at += wd
    wq, wk, wv, wo, wu, wd_ = full
    vecs = (b_out, mid_gain, mid_shift, b_down, end_gain, end_shift)
    bias = (b_query, b_value, b_up)
    vec_all = lax.all_gather(jnp.stack(vecs), ROWS, axis=1, tiled=True).astype(F32)
    bias_all = lax.all_gather(jnp.concatenate(bias, axis=1), ALL, axis=0, tiled=False).astype(F32)

    def whole_bias(at, wd):
        piece = bias_all[:, :, at:at + wd].reshape(rows_n, tp_n, heads_l, wd)
        return piece.transpose(1, 2, 0, 3).reshape(-1)

    bq = whole_bias(0, head_l)
    bv = whole_bias(head_l, head_l)
    bu = whole_bias(2 * head_l, b_up.shape[1])
    bo, mg, ms, bd, eg, es = (vec_all[i] for i in range(6))

    lens = lax.dynamic_index_in_dim(seq_lengths[:, 0], c, 0, keepdims=False)
    order = lax.dynamic_index_in_dim(row_order[:, 0], c, 0, keepdims=False)
    places = lax.iota(jnp.int32, lens.shape[0])
    longest = jnp.argmax(lens)
    first = jnp.sum(jnp.where(places < longest, lens, 0))
    start = lax.rem(first + half * half_rows, group_rows)
    ends = jnp.cumsum(lens)
    nat = lax.rem(start + lax.iota(jnp.int32, half_rows), group_rows)
    seg = jnp.sum((ends[None, :] <= nat[:, None]).astype(jnp.int32), axis=1)
    q_at = quarter * my_rows
    nat_q = lax.dynamic_slice_in_dim(nat, q_at, my_rows)
    seg_q = lax.dynamic_slice_in_dim(seg, q_at, my_rows)

    x_group = gather_group(tokens_in)
    c_group = gather_group(cotangent)
    x_twice = jnp.concatenate([x_group, x_group[:half_rows]], axis=0)
    x_half = lax.dynamic_slice_in_dim(x_twice, start, half_rows, 0)
    x_mine = lax.dynamic_slice_in_dim(x_half, q_at, my_rows, 0)
    pick = (order[:, None] == nat_q[None, :]).astype(BF)
    pick_nat = (lax.iota(jnp.int32, group_rows)[:, None] == nat_q[None, :]).astype(BF)
    dy = mm_lt(pick, c_group)

    x = x_mine.astype(F32)
    q = (mm(x_mine, wq) + bq).astype(BF).reshape(my_rows, heads, head)
    k = mm(x_half, wk).astype(BF).reshape(half_rows, heads, head)
    v = (mm(x_half, wv) + bv).astype(BF).reshape(half_rows, heads, head)
    same = seg_q[:, None] == seg[None, :]
    s = jnp.einsum("qhd,khd->hqk", q, k, preferred_element_type=F32) * 0.125
    s = jnp.where(same[None], s, MASKED)
    p = jnp.exp(s - jnp.max(s, axis=-1, keepdims=True))
    p = p / jnp.sum(p, axis=-1, keepdims=True)
    pb = p.astype(BF)
    o = jnp.einsum("hqk,khd->qhd", pb, v, preferred_element_type=F32).astype(BF)
    o2 = o.reshape(my_rows, heads * head)
    r1 = x + mm_rt(o2, wo) + bo
    n1, inv1 = norm(r1)
    middle = n1 * mg + ms
    mid_b = middle.astype(BF)
    pre = mm(mid_b, wu) + bu
    cdf, pdf = phi_both(pre)
    act = (pre * cdf).astype(BF)
    r2 = middle + mm_rt(act, wd_) + bd
    n2, inv2 = norm(r2)
    y = n2 * eg + es

    d_r2 = norm_back(dy, eg, n2, inv2)
    df = d_r2.astype(BF)
    d_pre = (mm(df, wd_) * (cdf + pre * pdf)).astype(BF)
    g_down = mm_lt(df, act)
    g_up = mm_lt(mid_b, d_pre)
    d_mid = d_r2 + mm_rt(d_pre, wu)
    d_r1 = norm_back(d_mid, mg, n1, inv1)
    da = d_r1.astype(BF)
    g_out = mm_lt(da, o2)
    d_o = mm(da, wo).astype(BF).reshape(my_rows, heads, head)
    dp = jnp.einsum("qhd,khd->hqk", d_o, v, preferred_element_type=F32)
    ds = (p * (dp - jnp.sum(p * dp, axis=-1, keepdims=True))).astype(BF)
    d_q = (jnp.einsum("hqk,khd->qhd", ds, k, preferred_element_type=F32) * 0.125).astype(BF)
    d_k = jnp.einsum("hqk,qhd->khd", ds, q, preferred_element_type=F32) * 0.125
    d_v = jnp.einsum("hqk,qhd->khd", pb, d_o, preferred_element_type=F32)
    d_q = d_q.reshape(my_rows, heads * head)
    d_kv = jnp.concatenate([d_k.reshape(half_rows, -1), d_v.reshape(half_rows, -1)], axis=1).astype(BF)
    pairs = [[h * parts + j for j in range(parts)] for h in range(tp_n // parts)]
    d_kv = lax.psum_scatter(d_kv.astype(F32), "tp", scatter_dimension=0, tiled=True, axis_index_groups=pairs)
    d_k, d_v = jnp.split(d_kv.astype(BF), 2, axis=1)
    g_q = mm_lt(x_mine, d_q)
    g_k = mm_lt(x_mine, d_k)
    g_v = mm_lt(x_mine, d_v)
    d_x = (d_r1 + mm_rt(d_q, wq) + mm_rt(d_k, wk) + mm_rt(d_v, wv)).astype(BF)

    layer_out = scatter_group(mm(pick, y.astype(BF)).astype(BF), own_rows)
    input_grad = scatter_group(mm(pick_nat, d_x).astype(BF), own_rows)

    outs = []
    for g, wd in zip((g_q, g_k, g_v, g_out, g_up, g_down), widths):
        outs.append(g.astype(BF).reshape(rows_n, width // rows_n, tp_n, wd).transpose(0, 2, 1, 3))
    packed_g = jnp.concatenate(outs, axis=3)
    packed_g = packed_g.reshape(rows_n * tp_n, width // rows_n, -1)
    mine_g = lax.psum_scatter(packed_g, ALL, scatter_dimension=0, tiled=True)[0].astype(F32)
    gm, at = [], 0
    for wd in widths:
        gm.append(mine_g[:, at:at + wd])
        at += wd

    def total(a):
        return jnp.sum(a.astype(F32), axis=0)

    def split_bias(a, wd):
        return a.reshape(tp_n, heads_l, rows_n, wd).transpose(2, 0, 1, 3).reshape(rows_n * tp_n, heads_l, wd)

    small_b = jnp.concatenate([
        split_bias(total(d_q), head_l), split_bias(total(d_v), head_l), split_bias(total(d_pre), b_up.shape[1])],
        axis=2).reshape(rows_n * tp_n, -1)
    vec_g = jnp.stack([total(d_r1), total(d_mid * n1), total(d_mid), total(d_r2), total(dy * n2), total(dy)])
    small_v = vec_g.reshape(6, rows_n, 1, width // rows_n).transpose(1, 2, 0, 3)
    small_v = jnp.broadcast_to(small_v, (rows_n, tp_n, 6, width // rows_n)).reshape(rows_n * tp_n, -1)
    small = jnp.concatenate([small_b, small_v], axis=1)
    small = lax.psum_scatter(small, ALL, scatter_dimension=0, tiled=True)[0]
    nb = small_b.shape[1]
    sb = small[:nb].reshape(heads_l, -1)
    sv = small[nb:].reshape(6, -1)
    return (layer_out, input_grad, gm[0], sb[:, :head_l], gm[1], gm[2], sb[:, head_l:2 * head_l], gm[3],
            sv[0], sv[1], sv[2], gm[4], sb[:, 2 * head_l:], gm[5], sv[3], sv[4], sv[5])


def specs():
    tok = P(None, ALL, None)
    grp = P(None, "fsdp", None)
    mat = P(ROWS, "tp")
    bias = P("tp", ROWS)
    vec = P(ROWS)
    ins = (tok, tok, grp, grp, mat, bias, mat, mat, bias, mat, vec, vec, vec, mat, bias, mat, vec, vec, vec)
    return ins, (tok, tok) + ins[4:]


def solution(mesh):
    ins, outs = specs()
    return jax.shard_map(body, mesh=mesh, in_specs=ins, out_specs=outs, check_vma=False)
```

```python
import functools

import jax
import jax.numpy as jnp
from jax import lax
from jax.experimental import pallas as pl
from jax.experimental.pallas import tpu as pltpu
from jax.sharding import PartitionSpec as P

EPS = 1e-06
MASKED = -1e30
ALL = ("fsdp", "ctx", "tp")
ROWS = ("fsdp", "ctx")
BF = jnp.bfloat16
F32 = jnp.float32


MESH = pl.DeviceIdType.MESH
def mm(a, b):
    return jnp.dot(a, b, preferred_element_type=F32)


def mm_rt(a, b):
    return lax.dot_general(a, b, (((1,), (1,)), ((), ())), preferred_element_type=F32)


def mm_lt(a, b):
    return lax.dot_general(a, b, (((0,), (0,)), ((), ())), preferred_element_type=F32)


def norm(u):
    centre = u - jnp.mean(u, axis=-1, keepdims=True)
    inv = lax.rsqrt(jnp.mean(centre * centre, axis=-1, keepdims=True) + EPS)
    return centre * inv, inv


def norm_back(d, gain, n, inv):
    e = d * gain
    return (e - jnp.mean(e, axis=-1, keepdims=True) - n * jnp.mean(e * n, axis=-1, keepdims=True)) * inv


def phi_both(u):
    cdf = 0.5 * (1.0 + lax.erf(u * 0.7071067811865476))
    pdf = 0.3989422804014327 * jnp.exp(-0.5 * u * u)
    return cdf, pdf


def gather_group(block):
    width = block.shape[-1]
    mine = lax.all_to_all(block, "ctx", 0, 0, tiled=True)
    whole = lax.all_gather(mine, "tp", axis=1, tiled=False)
    return whole.reshape(-1, width)


def scatter_group(rows, own_rows):
    ctx_n, tp_n = lax.axis_size("ctx"), lax.axis_size("tp")
    width = rows.shape[-1]
    blocks = rows.reshape(ctx_n, tp_n * own_rows, width)
    mine = lax.psum_scatter(blocks, "tp", scatter_dimension=1, tiled=True)
    return lax.all_to_all(mine, "ctx", 0, 0, tiled=True)


def body(tokens_in, cotangent, seq_lengths, row_order, w_query, b_query, w_key, w_value, b_value,
         w_out, b_out, mid_gain, mid_shift, w_up, b_up, w_down, b_down, end_gain, end_shift):
    ctx_n, tp_n, fsdp_n = lax.axis_size("ctx"), lax.axis_size("tp"), lax.axis_size("fsdp")
    rows_n = ctx_n * fsdp_n
    c, t = lax.axis_index("ctx"), lax.axis_index("tp")
    micro, own_rows, width = tokens_in.shape
    group_rows = own_rows * ctx_n * tp_n
    half_rows = group_rows // 2
    parts = tp_n // 2
    my_rows = half_rows // parts
    half, quarter = t // parts, t % parts
    heads_l, head_l = b_query.shape
    heads, head = heads_l * tp_n, head_l * rows_n

    mats = (w_query, w_key, w_value, w_out, w_up, w_down)
    widths = [m.shape[1] for m in mats]
    packed = lax.all_gather(jnp.concatenate(mats, axis=1), ALL, axis=0, tiled=False)
    full, at = [], 0
    for wd in widths:
        piece = packed[:, :, at:at + wd].reshape(rows_n, tp_n, -1, wd)
        full.append(piece.transpose(0, 2, 1, 3).reshape(width, tp_n * wd))
        at += wd
    wq, wk, wv, wo, wu, wd_ = full
    vecs = (b_out, mid_gain, mid_shift, b_down, end_gain, end_shift)
    bias = (b_query, b_value, b_up)
    vec_all = lax.all_gather(jnp.stack(vecs), ROWS, axis=1, tiled=True).astype(F32)
    bias_all = lax.all_gather(jnp.concatenate(bias, axis=1), ALL, axis=0, tiled=False).astype(F32)

    def whole_bias(at, wd):
        piece = bias_all[:, :, at:at + wd].reshape(rows_n, tp_n, heads_l, wd)
        return piece.transpose(1, 2, 0, 3).reshape(-1)

    bq = whole_bias(0, head_l)
    bv = whole_bias(head_l, head_l)
    bu = whole_bias(2 * head_l, b_up.shape[1])
    bo, mg, ms, bd, eg, es = (vec_all[i] for i in range(6))

    lens = lax.dynamic_index_in_dim(seq_lengths[:, 0], c, 0, keepdims=False)
    order = lax.dynamic_index_in_dim(row_order[:, 0], c, 0, keepdims=False)
    places = lax.iota(jnp.int32, lens.shape[0])
    longest = jnp.argmax(lens)
    first = jnp.sum(jnp.where(places < longest, lens, 0))
    start = lax.rem(first + half * half_rows, group_rows)
    ends = jnp.cumsum(lens)
    nat = lax.rem(start + lax.iota(jnp.int32, half_rows), group_rows)
    seg = jnp.sum((ends[None, :] <= nat[:, None]).astype(jnp.int32), axis=1)
    q_at = quarter * my_rows
    nat_q = lax.dynamic_slice_in_dim(nat, q_at, my_rows)
    seg_q = lax.dynamic_slice_in_dim(seg, q_at, my_rows)

    x_group = gather_group(tokens_in)
    c_group = gather_group(cotangent)
    x_twice = jnp.concatenate([x_group, x_group[:half_rows]], axis=0)
    x_half = lax.dynamic_slice_in_dim(x_twice, start, half_rows, 0)
    x_mine = lax.dynamic_slice_in_dim(x_half, q_at, my_rows, 0)
    pick = (order[:, None] == nat_q[None, :]).astype(BF)
    pick_nat = (lax.iota(jnp.int32, group_rows)[:, None] == nat_q[None, :]).astype(BF)
    dy = mm_lt(pick, c_group)

    x = x_mine.astype(F32)
    q = (mm(x_mine, wq) + bq).astype(BF).reshape(my_rows, heads, head)
    k = mm(x_half, wk).astype(BF).reshape(half_rows, heads, head)
    v = (mm(x_half, wv) + bv).astype(BF).reshape(half_rows, heads, head)
    same = seg_q[:, None] == seg[None, :]
    s = jnp.einsum("qhd,khd->hqk", q, k, preferred_element_type=F32) * 0.125
    s = jnp.where(same[None], s, MASKED)
    p = jnp.exp(s - jnp.max(s, axis=-1, keepdims=True))
    p = p / jnp.sum(p, axis=-1, keepdims=True)
    pb = p.astype(BF)
    o = jnp.einsum("hqk,khd->qhd", pb, v, preferred_element_type=F32).astype(BF)
    o2 = o.reshape(my_rows, heads * head)
    r1 = x + mm_rt(o2, wo) + bo
    n1, inv1 = norm(r1)
    middle = n1 * mg + ms
    mid_b = middle.astype(BF)
    pre = mm(mid_b, wu) + bu
    cdf, pdf = phi_both(pre)
    act = (pre * cdf).astype(BF)
    r2 = middle + mm_rt(act, wd_) + bd
    n2, inv2 = norm(r2)
    y = n2 * eg + es

    d_r2 = norm_back(dy, eg, n2, inv2)
    df = d_r2.astype(BF)
    d_pre = (mm(df, wd_) * (cdf + pre * pdf)).astype(BF)
    g_down = mm_lt(df, act)
    g_up = mm_lt(mid_b, d_pre)
    d_mid = d_r2 + mm_rt(d_pre, wu)
    d_r1 = norm_back(d_mid, mg, n1, inv1)
    da = d_r1.astype(BF)
    g_out = mm_lt(da, o2)
    d_o = mm(da, wo).astype(BF).reshape(my_rows, heads, head)
    dp = jnp.einsum("qhd,khd->hqk", d_o, v, preferred_element_type=F32)
    ds = (p * (dp - jnp.sum(p * dp, axis=-1, keepdims=True))).astype(BF)
    d_q = (jnp.einsum("hqk,khd->qhd", ds, k, preferred_element_type=F32) * 0.125).astype(BF)
    d_k = jnp.einsum("hqk,qhd->khd", ds, q, preferred_element_type=F32) * 0.125
    d_v = jnp.einsum("hqk,qhd->khd", pb, d_o, preferred_element_type=F32)
    d_q = d_q.reshape(my_rows, heads * head)
    d_kv = jnp.concatenate([d_k.reshape(half_rows, -1), d_v.reshape(half_rows, -1)], axis=1).astype(BF)
    pairs = [[h * parts + j for j in range(parts)] for h in range(tp_n // parts)]
    d_kv = lax.psum_scatter(d_kv.astype(F32), "tp", scatter_dimension=0, tiled=True, axis_index_groups=pairs)
    d_k, d_v = jnp.split(d_kv.astype(BF), 2, axis=1)
    g_q = mm_lt(x_mine, d_q)
    g_k = mm_lt(x_mine, d_k)
    g_v = mm_lt(x_mine, d_v)
    d_x = (d_r1 + mm_rt(d_q, wq) + mm_rt(d_k, wk) + mm_rt(d_v, wv)).astype(BF)

    layer_out = scatter_group(mm(pick, y.astype(BF)).astype(BF), own_rows)
    input_grad = scatter_group(mm(pick_nat, d_x).astype(BF), own_rows)

    outs = []
    for g, wd in zip((g_q, g_k, g_v, g_out, g_up, g_down), widths):
        outs.append(g.astype(BF).reshape(rows_n, width // rows_n, tp_n, wd).transpose(0, 2, 1, 3))
    packed_g = jnp.concatenate(outs, axis=3)
    packed_g = packed_g.reshape(rows_n * tp_n, width // rows_n, -1)
    mine_g = lax.psum_scatter(packed_g, ALL, scatter_dimension=0, tiled=True)[0].astype(F32)
    gm, at = [], 0
    for wd in widths:
        gm.append(mine_g[:, at:at + wd])
        at += wd

    def total(a):
        return jnp.sum(a.astype(F32), axis=0)

    def split_bias(a, wd):
        return a.reshape(tp_n, heads_l, rows_n, wd).transpose(2, 0, 1, 3).reshape(rows_n * tp_n, heads_l, wd)

    small_b = jnp.concatenate([
        split_bias(total(d_q), head_l), split_bias(total(d_v), head_l), split_bias(total(d_pre), b_up.shape[1])],
        axis=2).reshape(rows_n * tp_n, -1)
    vec_g = jnp.stack([total(d_r1), total(d_mid * n1), total(d_mid), total(d_r2), total(dy * n2), total(dy)])
    small_v = vec_g.reshape(6, rows_n, 1, width // rows_n).transpose(1, 2, 0, 3)
    small_v = jnp.broadcast_to(small_v, (rows_n, tp_n, 6, width // rows_n)).reshape(rows_n * tp_n, -1)
    small = jnp.concatenate([small_b, small_v], axis=1)
    small = lax.psum_scatter(small, ALL, scatter_dimension=0, tiled=True)[0]
    nb = small_b.shape[1]
    sb = small[:nb].reshape(heads_l, -1)
    sv = small[nb:].reshape(6, -1)
    return (layer_out, input_grad, gm[0], sb[:, :head_l], gm[1], gm[2], sb[:, head_l:2 * head_l], gm[3],
            sv[0], sv[1], sv[2], gm[4], sb[:, 2 * head_l:], gm[5], sv[3], sv[4], sv[5])


def specs():
    tok = P(None, ALL, None)
    grp = P(None, "fsdp", None)
    mat = P(ROWS, "tp")
    bias = P("tp", ROWS)
    vec = P(ROWS)
    ins = (tok, tok, grp, grp, mat, bias, mat, mat, bias, mat, vec, vec, vec, mat, bias, mat, vec, vec, vec)
    return ins, (tok, tok) + ins[4:]


CHUNK = 32
VMEM_MAX = 62 * 1024 * 1024


def block_mat(ref, t):
    n, rows, width = ref.shape[1:]
    return ref[t].reshape(n * rows, width)


def row_facts(meta, group_n):
    c, t = lax.axis_index("ctx"), lax.axis_index("tp")
    lens = meta[4:5, :].astype(F32)
    lane = lax.broadcasted_iota(jnp.int32, lens.shape, 1)

    def one(k):
        return jnp.sum(jnp.where(lane == 3 * c + k, lens, 0.0), axis=1, keepdims=True).astype(jnp.int32)

    l0, l1 = one(0), one(1)
    half = group_n // 2
    first = jnp.where(l0 == half, 0, jnp.where(l1 == half, l0, l0 + l1))
    return first + (t % 2) * half, l0, l0 + l1


def wrap(v, group_n):
    return jnp.where(v >= group_n, v - group_n, v)


def pick_row(block, c):
    row = lax.broadcasted_iota(jnp.int32, block.shape, 0)
    return jnp.sum(jnp.where(row == c, block.astype(F32), 0.0), axis=0, keepdims=True).astype(jnp.int32)


def chunks(total, fn, size=CHUNK):
    def step(i, _):
        fn(pl.ds(pl.multiple_of(i * size, size), size))
        return 0
    lax.fori_loop(0, total // size, step, 0)


def each_t(fn):
    def step(t, _):
        fn(t)
        return 0
    lax.fori_loop(0, 4, step, 0)


def k1_kernel(head, gath, meta_ref, group, gg, dq_out, dkv_out, xm_out, da_out, op_out, dr1_out, y_out, vec_out,
              w_a, w_u, w_d, small, xh, dy, qkv, probs, sbuf, pb, pb2, acc, mid, midb, n1, inv1, gelu_d, act, n2, df, big, bias,
              g_u, g_d, sem):
    f, c, t_me = lax.axis_index("fsdp"), lax.axis_index("ctx"), lax.axis_index("tp")
    width = xh.shape[1]
    s_n, r_n, n_n = xh.shape[0], dy.shape[0], group.shape[1]
    wl = w_a.shape[2]
    hw = width // 4
    per_t = hw // head

    loads = [pltpu.make_async_copy(gath.at[:, :, pl.ds(wl * i, wl)], ref, sem.at[i])
             for i, ref in enumerate((w_a, w_u, w_d))]
    loads.append(pltpu.make_async_copy(gath.at[:, :, pl.ds(3 * wl, 16)], small, sem.at[3]))
    for d in (loads[3], loads[0], loads[1], loads[2]):
        d.start()

    meta = meta_ref[t_me // 2]
    start, e0, e1 = row_facts(meta, n_n)
    order = pick_row(meta[0:4, :], c)

    def half_rows(rows):
        nat = wrap(start + rows.start + lax.broadcasted_iota(jnp.int32, (rows.size, 1), 0), n_n)
        sel = (lax.broadcasted_iota(jnp.int32, (rows.size, n_n), 1) == nat).astype(F32).astype(BF)
        xh[rows, :] = mm(sel, group[0]).astype(BF)
    chunks(s_n, half_rows, 128)

    def quarter_rows(rows):
        nat = wrap(start + f * r_n + rows.start + lax.broadcasted_iota(jnp.int32, (rows.size, 1), 0), n_n)
        sel = (order == nat).astype(F32).astype(BF)
        dy[rows, :] = mm(sel, group[1])
    chunks(r_n, quarter_rows, 128)

    mine = pl.ds(pl.multiple_of(f * r_n, r_n), r_n)
    loads[3].wait()
    for t in range(4):
        bias[t] = jnp.sum(small[t].astype(F32), axis=0)
    vec = bias[0]
    bo, mg, ms, bd, eg, es = (vec[i:i + 1, :] for i in range(6))
    loads[0].wait()

    nat_row = wrap(start + lax.broadcasted_iota(jnp.int32, (1, s_n), 1), n_n)
    seg_row = (nat_row >= e0).astype(jnp.int32) + (nat_row >= e1).astype(jnp.int32)

    def forward_t(t):
        row6 = bias[t][6:7, :]
        qkv[t] = (mm(xh[...], block_mat(w_a, t)) + row6).astype(BF)
        q3 = qkv[t, mine, :]
        kv = qkv[t]
        outs = []
        for h in range(per_t):
            lo = hw + h * head
            sbuf[...] = mm_rt(q3[:, lo:lo + head], kv[:, lo + hw:lo + hw + head])
            at = t * per_t + h

            def soft(rows):
                nat = wrap(start + f * r_n + rows.start + lax.broadcasted_iota(jnp.int32, (rows.size, 1), 0), n_n)
                seg = (nat >= e0).astype(jnp.int32) + (nat >= e1).astype(jnp.int32)
                s = jnp.where(seg == seg_row, sbuf[rows, :] * 0.125, MASKED)
                p = jnp.exp(s - jnp.max(s, axis=1, keepdims=True))
                p = p / jnp.sum(p, axis=1, keepdims=True)
                probs[at, rows, :] = p
                pb[rows, :] = p.astype(BF)
            chunks(r_n, soft)
            outs.append(mm(pb[...], kv[:, lo + 2 * hw:lo + 2 * hw + head]).astype(BF))
        outs.append(jnp.zeros((r_n, width - hw), BF))
        op_out[t] = jnp.concatenate(outs, axis=1)
    each_t(forward_t)

    xm_out[...] = xh[mine, :]
    acc[...] = xm_out[...].astype(F32) + bo

    def out_t(t):
        acc[...] += mm_rt(op_out[t], block_mat(w_a, t))
    each_t(out_t)

    def norm_rows(u):
        centre = u - jnp.mean(u, axis=-1, keepdims=True)
        inv = lax.rsqrt(jnp.mean(centre * centre, axis=-1, keepdims=True) + EPS)
        return centre * inv, inv

    def first_norm(rows):
        n, inv = norm_rows(acc[rows, :])
        n1[rows, :] = n
        inv1[rows, :] = jnp.broadcast_to(inv, (rows.size, 128))
        m = n * mg + ms
        mid[rows, :] = m
        midb[rows, :] = m.astype(BF)
        acc[rows, :] = m + bd
    chunks(r_n, first_norm)

    loads[1].wait()
    loads[2].wait()

    def ffn_t(t):
        row7 = bias[t][7:8, :]
        big[...] = mm(midb[...], block_mat(w_u, t))

        def gelu(rows):
            u = big[rows, :] + row7
            cdf = 0.5 * (1.0 + lax.erf(u * 0.7071067811865476))
            pdf = 0.3989422804014327 * jnp.exp(-0.5 * u * u)
            act[t, rows, :] = (u * cdf).astype(BF)
            gelu_d[t, rows, :] = cdf + u * pdf
        chunks(r_n, gelu, 16)
        acc[...] += mm_rt(act[t], block_mat(w_d, t))
    each_t(ffn_t)

    vec_out[...] = jnp.zeros_like(vec_out)

    def add_vec(i, v):
        vec_out[i] += jnp.sum(v.reshape(-1, 8, v.shape[1]), axis=0)

    def second_norm(rows):
        n, inv = norm_rows(acc[rows, :])
        y_out[rows, :] = (n * eg + es).astype(BF)
        g = dy[rows, :]
        e = g * eg
        d = (e - jnp.mean(e, axis=-1, keepdims=True) - n * jnp.mean(e * n, axis=-1, keepdims=True)) * inv
        add_vec(3, d)
        add_vec(4, g * n)
        add_vec(5, g)
        df[rows, :] = d.astype(BF)
        acc[rows, :] = d
    chunks(r_n, second_norm)

    def ffn_back_t(t):
        big[...] = mm(df[...], block_mat(w_d, t))

        def times(rows):
            d = (big[rows, :] * gelu_d[t, rows, :]).astype(BF)
            n2[rows, :] = d
            add_vec(8 + t, d.astype(F32))
        chunks(r_n, times)
        acc[...] += mm_rt(n2[...], block_mat(w_u, t))
        g_d[t] = mm_lt(df[...], act[t]).astype(BF).reshape(g_d.shape[1:])
        g_u[t] = mm_lt(midb[...], n2[...]).astype(BF).reshape(g_u.shape[1:])
    each_t(ffn_back_t)
    stores = [pltpu.make_async_copy(g_u, gg.at[:, :, pl.ds(wl, wl)], sem.at[4]),
              pltpu.make_async_copy(g_d, gg.at[:, :, pl.ds(2 * wl, wl)], sem.at[5])]
    for d in stores:
        d.start()

    def first_norm_back(rows):
        g, n = acc[rows, :], n1[rows, :]
        e = g * mg
        d = (e - jnp.mean(e, axis=-1, keepdims=True) - n * jnp.mean(e * n, axis=-1, keepdims=True)) * inv1[rows, :][:, 0:1]
        add_vec(0, d)
        add_vec(1, g * n)
        add_vec(2, g)
        dr1_out[rows, :] = d
        da_out[rows, :] = d.astype(BF)
    chunks(r_n, first_norm_back)

    def attn_back_t(t):
        do = mm(da_out[...], block_mat(w_a, t)).astype(BF)
        q3 = qkv[t, mine, :]
        kv = qkv[t]
        dqs, dks, dvs = [], [], []
        for h in range(per_t):
            lo = hw + h * head
            at = t * per_t + h
            do_h = do[:, h * head:(h + 1) * head]
            sbuf[...] = mm_rt(do_h, kv[:, lo + 2 * hw:lo + 2 * hw + head])

            p, d = probs[at], sbuf[...]
            pb[...] = (p * (d - jnp.sum(p * d, axis=1, keepdims=True))).astype(BF)
            pb2[...] = p.astype(BF)
            dvs.append(mm_lt(pb2[...], do_h))
            dqs.append(mm(pb[...], kv[:, lo + hw:lo + hw + head]) * 0.125)
            dks.append(mm_lt(pb[...], q3[:, lo:lo + head]) * 0.125)
        dq_out[t] = jnp.concatenate([a.astype(BF) for a in dqs], axis=1)
        dkv_out[t] = jnp.concatenate([a.astype(BF) for a in dks + dvs], axis=1)
    each_t(attn_back_t)
    for d in stores:
        d.wait()


def k1(gath, meta, group, head):
    n_t, n_fc, rows, width = gath.shape
    wl = (rows - 16) // 3
    n_n = group.shape[1]
    s_n, r_n = n_n // 2, n_n // 4
    hw = width // 4
    heads = width // head
    v = pltpu.VMEM
    sds = jax.ShapeDtypeStruct
    vm = pl.BlockSpec(memory_space=pltpu.VMEM)
    any_ = pl.BlockSpec(memory_space=pl.ANY)
    wshape = (n_t, n_fc, wl, width)
    return pl.pallas_call(
        functools.partial(k1_kernel, head),
        out_shape=(sds(gath.shape, BF), sds((n_t, r_n, hw), BF), sds((n_t, s_n, 2 * hw), BF), sds((r_n, width), BF),
                   sds((r_n, width), BF), sds((n_t, r_n, width), BF), sds((r_n, width), F32), sds((r_n, width), BF),
                   sds((16, 8, width), F32)),
        in_specs=[any_, vm, vm],
        out_specs=(any_,) + (vm,) * 8,
        scratch_shapes=[
            v(wshape, BF), v(wshape, BF), v(wshape, BF), v((n_t, n_fc, 16, width), BF),
            v((s_n, width), BF), v((r_n, width), F32), v((n_t, s_n, width), BF), v((heads, r_n, s_n), F32),
            v((r_n, s_n), F32), v((r_n, s_n), BF), v((r_n, s_n), BF), v((r_n, width), F32), v((r_n, width), F32), v((r_n, width), BF),
            v((r_n, width), F32), v((r_n, 128), F32), v((n_t, r_n, width), F32), v((n_t, r_n, width), BF),
            v((r_n, width), BF), v((r_n, width), BF), v((r_n, width), F32), v((n_t, 16, width), F32),
            v(wshape, BF), v(wshape, BF), pltpu.SemaphoreType.DMA((6,))],
        compiler_params=pltpu.CompilerParams(vmem_limit_bytes=VMEM_MAX),
        name="layer_main",
    )(gath, meta, group)


def k2_kernel(gath, meta_ref, dq, dkv, dkv_in, xm, da, op, dr1, y, vec, gg_in, gg, place,
              w_a, g_a, g_s, acc, dqkv, sem):
    f, c, t_me = lax.axis_index("fsdp"), lax.axis_index("ctx"), lax.axis_index("tp")
    r_n, width = xm.shape
    n_n = place.shape[1]
    wl = w_a.shape[2]
    hw = width // 4
    load = pltpu.make_async_copy(gath.at[:, :, pl.ds(0, wl)], w_a, sem.at[0])
    load.start()
    meta = meta_ref[t_me // 2]
    start, _, _ = row_facts(meta, n_n)
    order = pick_row(meta[8:12, :], c)
    nat = wrap(start + f * r_n + lax.broadcasted_iota(jnp.int32, (r_n, 1), 0), n_n)
    mine = pl.ds(pl.multiple_of(f * r_n, r_n), r_n)
    acc[...] = dr1[...]
    load.wait()
    lane16 = lax.broadcasted_iota(jnp.int32, (16, width), 0)
    sums = jnp.sum(vec[...], axis=1)

    def grads_t(t):
        both = (dkv[t, mine, :].astype(F32) + dkv_in[t].astype(F32)).astype(BF)
        dqkv[...] = jnp.concatenate([jnp.zeros((r_n, hw), BF), dq[t], both], axis=1)
        d = dqkv[...]
        acc[...] += mm_rt(d, block_mat(w_a, t))
        g_a[t] = (mm_lt(xm[...], d) + mm_lt(da[...], op[t])).astype(BF).reshape(g_a.shape[1:])
        base = jnp.where(lane16 < 6, sums, 0.0)
        base = base + jnp.where(lane16 == 6, jnp.sum(d.astype(F32), axis=0, keepdims=True), 0.0)
        base = base + jnp.where(lane16 == 7, jnp.sum(vec[8 + t], axis=0, keepdims=True), 0.0)
        g_s[t] = jnp.broadcast_to(base.astype(BF)[None], g_s.shape[1:])
    each_t(grads_t)
    stores = [pltpu.make_async_copy(g_a, gg.at[:, :, pl.ds(0, wl)], sem.at[1]),
              pltpu.make_async_copy(g_s, gg.at[:, :, pl.ds(3 * wl, 16)], sem.at[2])]
    for d in stores:
        d.start()
    pick = (order == nat).astype(F32).astype(BF)
    place[0] = mm_lt(pick, y[...]).astype(BF)
    lane = lax.broadcasted_iota(jnp.int32, (1, n_n), 1)
    block = n_n // 16
    at = ((lane // block) % 4) * (4 * block) + (lane // (4 * block)) * block + lane % block
    pick2 = (at == nat).astype(F32).astype(BF)
    place[1] = mm_lt(pick2, acc[...].astype(BF)).astype(BF)
    for d in stores:
        d.wait()


def k2(gath, meta, dq, dkv, dkv_in, xm, da, op, dr1, y, vec, gg):
    n_t, n_fc, rows, width = gath.shape
    wl = (rows - 16) // 3
    r_n = xm.shape[0]
    n_n = 4 * r_n
    v = pltpu.VMEM
    vm = pl.BlockSpec(memory_space=pltpu.VMEM)
    any_ = pl.BlockSpec(memory_space=pl.ANY)
    wshape = (n_t, n_fc, wl, width)
    return pl.pallas_call(
        k2_kernel,
        out_shape=(jax.ShapeDtypeStruct(gg.shape, BF), jax.ShapeDtypeStruct((2, n_n, width), BF)),
        in_specs=[any_] + [vm] * 10 + [any_],
        out_specs=(any_, vm),
        input_output_aliases={11: 0},
        scratch_shapes=[v(wshape, BF), v(wshape, BF), v((n_t, n_fc, 16, width), BF), v((r_n, width), F32),
                        v((r_n, width), BF), pltpu.SemaphoreType.DMA((3,))],
        compiler_params=pltpu.CompilerParams(vmem_limit_bytes=VMEM_MAX),
        name="layer_tail",
    )(gath, meta, dq, dkv, dkv_in, xm, da, op, dr1, y, vec, gg)


def comm_in_kernel(cut, tok, cot, pack, meta, gath, group, meta_all, held, *sems):
    (sem_l, s_e, r_e, s_xg, r_xg, s_xf, s_z, r_z, s_x0, r_x0, s_y0, r_y0, s_y1, r_y1, s_x1, r_x1,
     s_c, r_c, s_c0, r_c0, s_c1, r_c1, s_m, r_m) = sems
    f, c, t = lax.axis_index("fsdp"), lax.axis_index("ctx"), lax.axis_index("tp")
    rows = pack.shape[0]
    h0, h1 = pl.ds(0, cut), pl.ds(cut, rows - cut)
    slot = f * 4 + c
    partner = (1 - f, c, t)
    cx = c + 1 - 2 * (c % 2)
    cy = (c + 2) % 4
    cd = (cx + 2) % 4
    x_nb, y_nb = (f, cx, t), (f, cy, t)
    near, far = 1 + f, 3 * f
    is_near, is_far = t == near, t == far
    receiver = (t // 2) == f

    barrier = pltpu.get_barrier_semaphore()
    peers = [partner] + [(f, (c + i) % 4, t) for i in (1, 2, 3)] + [(f, c, (t + i) % 4) for i in (1, 2, 3)]
    for p in peers:
        pl.semaphore_signal(barrier, inc=1, device_id=p, device_id_type=MESH)
    pl.semaphore_wait(barrier, len(peers))

    pending = []

    def send(src, dst, ssem, rsem, dev, pred=None):
        d = pltpu.make_async_remote_copy(src_ref=src, dst_ref=dst, send_sem=ssem, recv_sem=rsem,
                                         device_id=dev, device_id_type=MESH)
        if pred is None:
            d.start()
        else:
            pl.when(pred)(d.start)
        pending.append((pred, d))

    def arrived(dst, rsem, pred=None):
        d = pltpu.make_async_remote_copy(src_ref=dst, dst_ref=dst, send_sem=s_e.at[0, 0], recv_sem=rsem,
                                         device_id=partner, device_id_type=MESH)
        if pred is None:
            d.wait_recv()
        else:
            pl.when(pred)(d.wait_recv)

    def both(a, b):
        return b if a is None else jnp.logical_and(a, b)

    def first_sends(ten, ref):
        for i in (1, 2, 3):
            to = (c + i) % 4
            send(ref.at[to], held.at[ten, c], s_e.at[ten, i], r_e.at[ten, c], (f, to, t))

    first_sends(0, tok)
    local = [pltpu.make_async_copy(tok.at[c], held.at[0, c], sem_l.at[0]),
             pltpu.make_async_copy(cot.at[c], held.at[1, c], sem_l.at[1]),
             pltpu.make_async_copy(pack, gath.at[t, slot], sem_l.at[2])]
    for d in local:
        d.start()
    send(meta, meta_all.at[f], s_m.at[0], r_m.at[0], partner)
    own_meta = pltpu.make_async_copy(meta, meta_all.at[f], sem_l.at[5])
    own_meta.start()

    def have_column(src, tt, pred=None):
        send(src.at[h0], gath.at[tt, slot, h0], s_x0.at[tt], r_x0.at[tt], x_nb, pred)
        send(src.at[h1], gath.at[tt, slot, h1], s_y1.at[tt], r_y1.at[tt], y_nb, pred)
        send(src.at[h0], gath.at[tt, slot, h0], s_y0.at[0, tt], r_y0.at[0, tt], y_nb, pred)
        send(src.at[h1], gath.at[tt, slot, h1], s_x1.at[0, tt], r_x1.at[0, tt], x_nb, pred)
        send(src, gath.at[tt, slot], s_c.at[tt], r_c.at[tt], partner, pred)

    send(pack, gath.at[t, slot], s_z.at[0, t], r_z.at[t], (f, c, (t + 1) % 4), t < 3)
    send(pack, gath.at[t, slot], s_z.at[1, t], r_z.at[t], (f, c, (t + 3) % 4), t > 0)
    have_column(pack, t)
    first_sends(1, cot)

    def second_sends(ten):
        local[ten].wait()
        for i in (1, 2, 3):
            frm = (c + i) % 4
            arrived(held.at[ten, frm], r_e.at[ten, frm])
        blk = held.at[ten]
        dst = group.at[ten, :, t]
        to = jnp.where(is_near, far, near)
        send(blk, dst, s_xg.at[ten, t], r_xg.at[ten, t], (f, c, to))
        send(blk, dst, s_xf.at[ten, 0, t], r_xg.at[ten, t], partner, receiver)
        keep = pltpu.make_async_copy(blk, dst, sem_l.at[3 + ten])
        pl.when(receiver)(keep.start)
        return keep

    keeps = [second_sends(0)]

    def z_step(d):
        for sign in (-1, 1):
            tt = t + sign * d
            there = tt >= 0 if sign < 0 else tt <= 3
            tt = (tt + 4) % 4
            arrived(gath.at[tt, slot], r_z.at[tt], there)
            on = t < 3 if sign < 0 else t > 0
            nxt = (t + 1) % 4 if sign < 0 else (t + 3) % 4
            if d < 3:
                send(gath.at[tt, slot], gath.at[tt, slot], s_z.at[(1 - sign) // 2 * 0 + (0 if sign < 0 else 1), tt],
                     r_z.at[tt], (f, c, nxt), both(there, on))
            have_column(gath.at[tt, slot], tt, there)

    def relay(ten):
        for i in (1, 2, 3):
            tt = (t + i) % 4
            arrived(group.at[ten, :, tt], r_xg.at[ten, tt], receiver)
            send(group.at[ten, :, tt], group.at[ten, :, tt], s_xg.at[ten, tt], r_xg.at[ten, tt], (f, c, far),
                 jnp.logical_and(is_near, tt != far))
            send(group.at[ten, :, tt], group.at[ten, :, tt], s_xf.at[ten, 0, tt], r_xg.at[ten, tt], partner, receiver)

    z_step(1)
    relay(0)
    keeps.append(second_sends(1))
    z_step(2)
    z_step(3)
    relay(1)

    columns = [(t, None)]
    for d in (1, 2, 3):
        columns.append(((t - d + 4) % 4, t - d >= 0))
        columns.append(((t + d) % 4, t + d <= 3))
    for tt, pred in columns:
        a = gath.at[tt, f * 4 + cx, h0]
        arrived(a, r_x0.at[tt], pred)
        send(a, a, s_y0.at[1, tt], r_y0.at[1, tt], y_nb, pred)
        send(a, a, s_c0.at[0, tt], r_c0.at[0, tt], partner, pred)
        b = gath.at[tt, f * 4 + cy, h1]
        arrived(b, r_y1.at[tt], pred)
        send(b, b, s_x1.at[1, tt], r_x1.at[1, tt], x_nb, pred)
        send(b, b, s_c1.at[0, tt], r_c1.at[0, tt], partner, pred)
    for step in (0, 1):
        for tt, pred in columns:
            a = gath.at[tt, f * 4 + (cy if step == 0 else cd), h0]
            arrived(a, r_y0.at[step, tt], pred)
            send(a, a, s_c0.at[1 + step, tt], r_c0.at[1 + step, tt], partner, pred)
            b = gath.at[tt, f * 4 + (cx if step == 0 else cd), h1]
            arrived(b, r_x1.at[step, tt], pred)
            send(b, b, s_c1.at[1 + step, tt], r_c1.at[1 + step, tt], partner, pred)

    other = (1 - f) * 4
    for tt in range(4):
        arrived(gath.at[tt, other + c], r_c.at[tt])
        for j, cc in enumerate((cx, cy, cd)):
            arrived(gath.at[tt, other + cc, h0], r_c0.at[j, tt])
        for j, cc in enumerate((cy, cx, cd)):
            arrived(gath.at[tt, other + cc, h1], r_c1.at[j, tt])
    for ten in (0, 1):
        for tt in range(4):
            arrived(group.at[ten, :, tt], r_xg.at[ten, tt], jnp.logical_not(receiver))
        pl.when(receiver)(keeps[ten].wait)
    arrived(meta_all.at[1 - f], r_m.at[0])
    own_meta.wait()
    local[2].wait()
    for pred, d in pending:
        if pred is None:
            d.wait_send()
        else:
            pl.when(pred)(d.wait_send)


def comm_in(tok, cot, pack, meta, cut):
    dma = pltpu.SemaphoreType.DMA
    rows, width = pack.shape
    own = tok.shape[1]
    sems = [dma((6,)), dma((2, 4)), dma((2, 4)), dma((2, 4)), dma((2, 4)), dma((2, 1, 4)), dma((2, 4)), dma((4,)),
            dma((4,)), dma((4,)), dma((2, 4)), dma((2, 4)), dma((4,)), dma((4,)), dma((2, 4)), dma((2, 4)),
            dma((4,)), dma((4,)), dma((3, 4)), dma((3, 4)), dma((3, 4)), dma((3, 4)), dma((1,)), dma((1,))]
    any_ = pl.BlockSpec(memory_space=pl.ANY)
    return pl.pallas_call(
        functools.partial(comm_in_kernel, cut),
        out_shape=(jax.ShapeDtypeStruct((4, 8, rows, width), BF),
                   jax.ShapeDtypeStruct((2, 4, 4, own, width), BF), jax.ShapeDtypeStruct((2,) + meta.shape, jnp.int32)),
        in_specs=[any_, any_, pl.BlockSpec(memory_space=pltpu.VMEM), pl.BlockSpec(memory_space=pltpu.VMEM)],
        out_specs=(any_, any_, any_),
        scratch_shapes=[pltpu.VMEM((2, 4, own, width), BF)] + sems,
        compiler_params=pltpu.CompilerParams(collective_id=0, has_side_effects=True),
        name="comm_in",
    )(tok, cot, pack, meta)


def swap_kernel(dkv, got, ssem, rsem):
    f, c, t = lax.axis_index("fsdp"), lax.axis_index("ctx"), lax.axis_index("tp")
    partner = (1 - f, c, t)
    barrier = pltpu.get_barrier_semaphore()
    pl.semaphore_signal(barrier, inc=1, device_id=partner, device_id_type=MESH)
    pl.semaphore_wait(barrier, 1)
    n = got.shape[1]
    d = pltpu.make_async_remote_copy(src_ref=dkv.at[:, pl.ds(pl.multiple_of((1 - f) * n, n), n)], dst_ref=got, send_sem=ssem, recv_sem=rsem,
                                     device_id=partner, device_id_type=MESH)
    d.start()
    d.wait()


def swap(dkv):
    n_t, s_n, w = dkv.shape
    vm = pl.BlockSpec(memory_space=pltpu.VMEM)
    return pl.pallas_call(
        swap_kernel, out_shape=jax.ShapeDtypeStruct((n_t, s_n // 2, w), BF), in_specs=[vm], out_specs=vm,
        scratch_shapes=[pltpu.SemaphoreType.DMA, pltpu.SemaphoreType.DMA],
        compiler_params=pltpu.CompilerParams(collective_id=1, has_side_effects=True), name="core_swap")(dkv)


def comm_out_kernel(cut, gg, place, total, rows_out, own, got0, got1, got2, got3, pl1, pl2, final, *sems):
    (sem_l, s0, r0, s1, r1, s2, r2, s3, r3, su, ru, s_o, r_o) = sems
    f, c, t = lax.axis_index("fsdp"), lax.axis_index("ctx"), lax.axis_index("tp")
    rows = got0.shape[2]
    h0, h1 = pl.ds(0, cut), pl.ds(cut, rows - cut)
    partner = (1 - f, c, t)
    cx = c + 1 - 2 * (c % 2)
    cy = (c + 2) % 4
    cd = (cx + 2) % 4
    x_nb, y_nb = (f, cx, t), (f, cy, t)
    par = t % 2
    z_nb = (f, c, t + 1 - 2 * par)
    to_f, to_t = t // 2, 2 * f + par
    stays = to_f == f

    barrier = pltpu.get_barrier_semaphore()
    peers = [partner] + [(f, (c + i) % 4, t) for i in (1, 2, 3)] + [(f, c, (t + i) % 4) for i in (1, 2, 3)]
    for p in peers:
        pl.semaphore_signal(barrier, inc=1, device_id=p, device_id_type=MESH)

    @pl.when(jnp.logical_not(stays))
    def _():
        for i in range(4):
            pl.semaphore_signal(barrier, inc=1, device_id=(to_f, (c + i) % 4, to_t), device_id_type=MESH)
        pl.semaphore_wait(barrier, len(peers) + 4)

    @pl.when(stays)
    def _():
        pl.semaphore_wait(barrier, len(peers))

    pending = []

    def send(src, dst, ssem, rsem, dev, pred=None):
        d = pltpu.make_async_remote_copy(src_ref=src, dst_ref=dst, send_sem=ssem, recv_sem=rsem,
                                         device_id=dev, device_id_type=MESH)
        if pred is None:
            d.start()
        else:
            pl.when(pred)(d.start)
        pending.append((pred, d))

    def arrived(dst, rsem):
        pltpu.make_async_remote_copy(src_ref=dst, dst_ref=dst, send_sem=su.at[0], recv_sem=rsem,
                                     device_id=partner, device_id_type=MESH).wait_recv()

    turn = [(t + 2) % 4, (t + 1) % 4, (t + 3) % 4, t]
    own_base = pl.ds(pl.multiple_of(f * 4, 4), 4)
    loads = []
    for i, tt in enumerate(turn):
        d = pltpu.make_async_copy(gg.at[tt, own_base], own.at[tt], sem_l.at[i])
        d.start()
        loads.append(d)
    lo = pl.multiple_of(2 * f, 2)
    hi = pl.multiple_of(2 - 2 * f, 2)
    send(place.at[:, pl.ds(hi, 2)], pl1, su.at[0], ru.at[0], partner)
    for tt in turn:
        for i in (1, 2, 3, 0):
            cc = (c + i) % 4
            send(gg.at[tt, 4 * (1 - f) + cc], got0.at[tt, cc], s0.at[tt, cc], r0.at[tt, cc], partner)

    def add_into(dst, src, total_rows, step=16):
        def go(i, _):
            r = pl.ds(pl.multiple_of(i * step, step), step)
            dst[r, :] = dst[r, :] + src[r, :]
            return 0
        lax.fori_loop(0, total_rows // step, go, 0, unroll=2 if (total_rows // step) % 2 == 0 else 1)

    blocks = pl1.shape[2]
    arrived(pl1, ru.at[0])
    for ten in range(2):
        for k in (0, 1):
            for j in range(4):
                add_into(pl1.at[ten, k, j], place.at[ten, lo + k, j], pl1.shape[3])
    send(pl1.at[:, 1 - par], pl2, su.at[1], ru.at[1], z_nb)

    for i, tt in enumerate(turn):
        loads[i].wait()
        for k in (1, 2, 3, 0):
            cc = (c + k) % 4
            arrived(got0.at[tt, cc], r0.at[tt, cc])
            add_into(own.at[tt, cc], got0.at[tt, cc], rows)
        for k, cc in enumerate((cy, cd)):
            send(own.at[tt, cc, h0], got1.at[tt, k, h0], s1.at[0, k, tt], r1.at[0, k, tt], y_nb)
        for k, cc in enumerate((cx, cd)):
            send(own.at[tt, cc, h1], got1.at[tt, k, h1], s1.at[1, k, tt], r1.at[1, k, tt], x_nb)

    arrived(pl2, ru.at[1])
    for ten in range(2):
        for j in range(4):
            add_into(pl2.at[ten, j], pl1.at[ten, par, j], pl2.shape[2])
    moves = []
    for ten in range(2):
        for i in range(4):
            cc = (c + i) % 4
            src, dst = pl2.at[ten, cc], rows_out.at[ten, c]
            away = jnp.logical_not(stays) if i == 0 else None
            send(src, dst, s_o.at[ten, i], r_o.at[ten, c], (to_f, cc, to_t), away)
        moves.append(pltpu.make_async_copy(pl2.at[ten, c], rows_out.at[ten, c], sem_l.at[4 + ten]))
        pl.when(stays)(moves[ten].start)

    def half_add(dst, src, off, n):
        def go(i, _):
            r = pl.ds(pl.multiple_of(off + i * 16, 16), 16)
            dst[r, :] = dst[r, :] + src[r, :]
            return 0
        lax.fori_loop(0, n // 16, go, 0)

    for tt in turn:
        arrived(got1.at[tt, 0, h0], r1.at[0, 0, tt])
        half_add(own.at[tt, c], got1.at[tt, 0], 0, cut)
        arrived(got1.at[tt, 1, h0], r1.at[0, 1, tt])
        half_add(own.at[tt, cx], got1.at[tt, 1], 0, cut)
        arrived(got1.at[tt, 0, h1], r1.at[1, 0, tt])
        half_add(own.at[tt, c], got1.at[tt, 0], cut, rows - cut)
        arrived(got1.at[tt, 1, h1], r1.at[1, 1, tt])
        half_add(own.at[tt, cy], got1.at[tt, 1], cut, rows - cut)
        send(own.at[tt, cx, h0], got2.at[tt, h0], s2.at[0, tt], r2.at[0, tt], x_nb)
        send(own.at[tt, cy, h1], got2.at[tt, h1], s2.at[1, tt], r2.at[1, tt], y_nb)

    for i, tt in enumerate(turn):
        arrived(got2.at[tt, h0], r2.at[0, tt])
        arrived(got2.at[tt, h1], r2.at[1, tt])
        add_into(own.at[tt, c], got2.at[tt], rows)
        if i < 3:
            send(own.at[tt, c], got3.at[t], s3.at[tt], r3.at[t], (f, c, tt))
    keep = pltpu.make_async_copy(own.at[t, c], got3.at[t], sem_l.at[6])
    keep.start()
    keep.wait()
    for tt in turn[:3]:
        arrived(got3.at[tt], r3.at[tt])

    def go(i, _):
        r = pl.ds(pl.multiple_of(i * 16, 16), 16)
        a, b, e, g = (got3[k, r, :].astype(F32) for k in range(4))
        total[r, :] = ((a + b) + e) + g
        return 0
    lax.fori_loop(0, rows // 16, go, 0)

    for ten in range(2):
        for i in range(4):
            cc = (c + i) % 4
            if i == 0:
                @pl.when(jnp.logical_not(stays))
                def _(ten=ten, cc=cc):
                    arrived(rows_out.at[ten, cc], r_o.at[ten, cc])
                pl.when(stays)(moves[ten].wait)
            else:
                arrived(rows_out.at[ten, cc], r_o.at[ten, cc])
    for pred, d in pending:
        if pred is None:
            d.wait_send()
        else:
            pl.when(pred)(d.wait_send)


def comm_out(gg, place, cut):
    dma = pltpu.SemaphoreType.DMA
    n_t, n_fc, rows, width = gg.shape
    n_n = place.shape[1]
    block = n_n // 16
    place = place.reshape(2, 4, 4, block, width)
    v = pltpu.VMEM
    vm = pl.BlockSpec(memory_space=pltpu.VMEM)
    any_ = pl.BlockSpec(memory_space=pl.ANY)
    return pl.pallas_call(
        functools.partial(comm_out_kernel, cut),
        out_shape=(jax.ShapeDtypeStruct((rows, width), F32), jax.ShapeDtypeStruct((2, 4, block, width), BF)),
        in_specs=[any_, vm],
        out_specs=(vm, vm),
        scratch_shapes=[v((4, 4, rows, width), BF), v((4, 4, rows, width), BF), v((4, 2, rows, width), BF),
                        v((4, rows, width), BF), v((4, rows, width), BF), v((2, 2, 4, block, width), BF),
                        v((2, 4, block, width), BF), v((8, 128), F32),
                        dma((7,)), dma((4, 4)), dma((4, 4)), dma((2, 2, 4)), dma((2, 2, 4)), dma((2, 4)), dma((2, 4)),
                        dma((4,)), dma((4,)), dma((2,)), dma((2,)), dma((2, 4)), dma((2, 4))],
        compiler_params=pltpu.CompilerParams(collective_id=2, has_side_effects=True, vmem_limit_bytes=62 * 1024 * 1024),
        name="comm_out",
    )(gg, place)


def quad_body(tokens_in, cotangent, seq_lengths, row_order, w_query, b_query, w_key, w_value, b_value,
              w_out, b_out, mid_gain, mid_shift, w_up, b_up, w_down, b_down, end_gain, end_shift):
    f, c = lax.axis_index("fsdp"), lax.axis_index("ctx")
    fc = f * 4 + c
    own, width = tokens_in.shape[1:]
    wl = w_query.shape[0]
    heads_l, head_l = b_query.shape
    head = head_l * 8
    up_l = b_up.shape[1]
    hw = width // 4
    mat_a = jnp.concatenate([w_out, w_query, w_key, w_value], axis=1)

    vecs = jnp.stack([b_out, mid_gain, mid_shift, b_down, end_gain, end_shift])
    col = lax.broadcasted_iota(jnp.int32, (1, width), 1)
    row_v = jnp.where(col // wl == fc, jnp.tile(vecs, (1, 8)), 0)
    part = (col % head) // head_l == fc
    three = jnp.stack([jnp.zeros_like(b_query), b_query, jnp.zeros_like(b_query), b_value])
    row_a = jnp.where(part, jnp.tile(three, (1, 1, 8)).reshape(1, width), 0)
    row_u = jnp.where((col % (8 * up_l)) // up_l == fc, jnp.tile(b_up, (1, 8)).reshape(1, width), 0)
    small = jnp.concatenate([row_v, row_a, row_u, jnp.zeros((8, width), BF)], axis=0)
    pack = jnp.concatenate([mat_a, w_up, w_down, small], axis=0)

    order = row_order[:, 0]
    n_n = order.shape[1]
    moved = order.reshape(4, 4, 4, own).transpose(0, 2, 1, 3).reshape(4, n_n)
    lens = jnp.pad(seq_lengths[:, 0].reshape(1, -1), ((0, 3), (0, n_n - 12)))
    meta_own = jnp.concatenate([order, lens, moved, jnp.zeros((4, n_n), jnp.int32)], axis=0)

    cut = (pack.shape[0] // 32) * 16
    gath, group, meta = comm_in(tokens_in, cotangent, pack, meta_own, cut)
    group = group.reshape(2, n_n, width)
    gg, dq, dkv, xm, da, op, dr1, y, vec = k1(gath, meta, group, head)
    dkv_in = swap(dkv)
    gg, place = k2(gath, meta, dq, dkv, dkv_in, xm, da, op, dr1, y, vec, gg)
    total, rows = comm_out(gg, place, cut)

    g_a, g_up, g_down = total[:wl], total[wl:2 * wl], total[2 * wl:3 * wl]
    sv = lax.dynamic_slice(total[3 * wl:3 * wl + 6], (0, fc * wl), (6, wl))
    ba = total[3 * wl + 6].reshape(4, heads_l, head)
    gb = lax.dynamic_slice(ba, (0, 0, fc * head_l), (4, heads_l, head_l))
    gu = lax.dynamic_slice(total[3 * wl + 7].reshape(heads_l, -1), (0, fc * up_l), (heads_l, up_l))
    return (rows[0], rows[1], g_a[:, hw:2 * hw], gb[1], g_a[:, 2 * hw:3 * hw], g_a[:, 3 * hw:], gb[3], g_a[:, :hw],
            sv[0], sv[1], sv[2], g_up, gu, g_down, sv[3], sv[4], sv[5])


def solution(mesh):
    ins, outs = specs()
    small_mesh = (mesh.shape["fsdp"], mesh.shape["ctx"], mesh.shape["tp"]) == (2, 4, 4)
    fn = quad_body if small_mesh else body
    return jax.shard_map(fn, mesh=mesh, in_specs=ins, out_specs=outs, check_vma=False)
```

```python
import functools

import jax
import jax.numpy as jnp
from jax import lax
from jax.experimental import pallas as pl
from jax.experimental.pallas import tpu as pltpu
from jax.sharding import PartitionSpec as P

EPS = 1e-06
MASKED = -1e30
ALL = ("fsdp", "ctx", "tp")
ROWS = ("fsdp", "ctx")
BF = jnp.bfloat16
F32 = jnp.float32


MESH = pl.DeviceIdType.MESH
def mm(a, b):
    return jnp.dot(a, b, preferred_element_type=F32)


def mm_rt(a, b):
    return lax.dot_general(a, b, (((1,), (1,)), ((), ())), preferred_element_type=F32)


def mm_lt(a, b):
    return lax.dot_general(a, b, (((0,), (0,)), ((), ())), preferred_element_type=F32)


def norm(u):
    centre = u - jnp.mean(u, axis=-1, keepdims=True)
    inv = lax.rsqrt(jnp.mean(centre * centre, axis=-1, keepdims=True) + EPS)
    return centre * inv, inv


def norm_back(d, gain, n, inv):
    e = d * gain
    return (e - jnp.mean(e, axis=-1, keepdims=True) - n * jnp.mean(e * n, axis=-1, keepdims=True)) * inv


def phi_both(u):
    cdf = 0.5 * (1.0 + lax.erf(u * 0.7071067811865476))
    pdf = 0.3989422804014327 * jnp.exp(-0.5 * u * u)
    return cdf, pdf


def gather_group(block):
    width = block.shape[-1]
    mine = lax.all_to_all(block, "ctx", 0, 0, tiled=True)
    whole = lax.all_gather(mine, "tp", axis=1, tiled=False)
    return whole.reshape(-1, width)


def scatter_group(rows, own_rows):
    ctx_n, tp_n = lax.axis_size("ctx"), lax.axis_size("tp")
    width = rows.shape[-1]
    blocks = rows.reshape(ctx_n, tp_n * own_rows, width)
    mine = lax.psum_scatter(blocks, "tp", scatter_dimension=1, tiled=True)
    return lax.all_to_all(mine, "ctx", 0, 0, tiled=True)


def body(tokens_in, cotangent, seq_lengths, row_order, w_query, b_query, w_key, w_value, b_value,
         w_out, b_out, mid_gain, mid_shift, w_up, b_up, w_down, b_down, end_gain, end_shift):
    ctx_n, tp_n, fsdp_n = lax.axis_size("ctx"), lax.axis_size("tp"), lax.axis_size("fsdp")
    rows_n = ctx_n * fsdp_n
    c, t = lax.axis_index("ctx"), lax.axis_index("tp")
    micro, own_rows, width = tokens_in.shape
    group_rows = own_rows * ctx_n * tp_n
    half_rows = group_rows // 2
    parts = tp_n // 2
    my_rows = half_rows // parts
    half, quarter = t // parts, t % parts
    heads_l, head_l = b_query.shape
    heads, head = heads_l * tp_n, head_l * rows_n

    mats = (w_query, w_key, w_value, w_out, w_up, w_down)
    widths = [m.shape[1] for m in mats]
    packed = lax.all_gather(jnp.concatenate(mats, axis=1), ALL, axis=0, tiled=False)
    full, at = [], 0
    for wd in widths:
        piece = packed[:, :, at:at + wd].reshape(rows_n, tp_n, -1, wd)
        full.append(piece.transpose(0, 2, 1, 3).reshape(width, tp_n * wd))
        at += wd
    wq, wk, wv, wo, wu, wd_ = full
    vecs = (b_out, mid_gain, mid_shift, b_down, end_gain, end_shift)
    bias = (b_query, b_value, b_up)
    vec_all = lax.all_gather(jnp.stack(vecs), ROWS, axis=1, tiled=True).astype(F32)
    bias_all = lax.all_gather(jnp.concatenate(bias, axis=1), ALL, axis=0, tiled=False).astype(F32)

    def whole_bias(at, wd):
        piece = bias_all[:, :, at:at + wd].reshape(rows_n, tp_n, heads_l, wd)
        return piece.transpose(1, 2, 0, 3).reshape(-1)

    bq = whole_bias(0, head_l)
    bv = whole_bias(head_l, head_l)
    bu = whole_bias(2 * head_l, b_up.shape[1])
    bo, mg, ms, bd, eg, es = (vec_all[i] for i in range(6))

    lens = lax.dynamic_index_in_dim(seq_lengths[:, 0], c, 0, keepdims=False)
    order = lax.dynamic_index_in_dim(row_order[:, 0], c, 0, keepdims=False)
    places = lax.iota(jnp.int32, lens.shape[0])
    longest = jnp.argmax(lens)
    first = jnp.sum(jnp.where(places < longest, lens, 0))
    start = lax.rem(first + half * half_rows, group_rows)
    ends = jnp.cumsum(lens)
    nat = lax.rem(start + lax.iota(jnp.int32, half_rows), group_rows)
    seg = jnp.sum((ends[None, :] <= nat[:, None]).astype(jnp.int32), axis=1)
    q_at = quarter * my_rows
    nat_q = lax.dynamic_slice_in_dim(nat, q_at, my_rows)
    seg_q = lax.dynamic_slice_in_dim(seg, q_at, my_rows)

    x_group = gather_group(tokens_in)
    c_group = gather_group(cotangent)
    x_twice = jnp.concatenate([x_group, x_group[:half_rows]], axis=0)
    x_half = lax.dynamic_slice_in_dim(x_twice, start, half_rows, 0)
    x_mine = lax.dynamic_slice_in_dim(x_half, q_at, my_rows, 0)
    pick = (order[:, None] == nat_q[None, :]).astype(BF)
    pick_nat = (lax.iota(jnp.int32, group_rows)[:, None] == nat_q[None, :]).astype(BF)
    dy = mm_lt(pick, c_group)

    x = x_mine.astype(F32)
    q = (mm(x_mine, wq) + bq).astype(BF).reshape(my_rows, heads, head)
    k = mm(x_half, wk).astype(BF).reshape(half_rows, heads, head)
    v = (mm(x_half, wv) + bv).astype(BF).reshape(half_rows, heads, head)
    same = seg_q[:, None] == seg[None, :]
    s = jnp.einsum("qhd,khd->hqk", q, k, preferred_element_type=F32) * 0.125
    s = jnp.where(same[None], s, MASKED)
    p = jnp.exp(s - jnp.max(s, axis=-1, keepdims=True))
    p = p / jnp.sum(p, axis=-1, keepdims=True)
    pb = p.astype(BF)
    o = jnp.einsum("hqk,khd->qhd", pb, v, preferred_element_type=F32).astype(BF)
    o2 = o.reshape(my_rows, heads * head)
    r1 = x + mm_rt(o2, wo) + bo
    n1, inv1 = norm(r1)
    middle = n1 * mg + ms
    mid_b = middle.astype(BF)
    pre = mm(mid_b, wu) + bu
    cdf, pdf = phi_both(pre)
    act = (pre * cdf).astype(BF)
    r2 = middle + mm_rt(act, wd_) + bd
    n2, inv2 = norm(r2)
    y = n2 * eg + es

    d_r2 = norm_back(dy, eg, n2, inv2)
    df = d_r2.astype(BF)
    d_pre = (mm(df, wd_) * (cdf + pre * pdf)).astype(BF)
    g_down = mm_lt(df, act)
    g_up = mm_lt(mid_b, d_pre)
    d_mid = d_r2 + mm_rt(d_pre, wu)
    d_r1 = norm_back(d_mid, mg, n1, inv1)
    da = d_r1.astype(BF)
    g_out = mm_lt(da, o2)
    d_o = mm(da, wo).astype(BF).reshape(my_rows, heads, head)
    dp = jnp.einsum("qhd,khd->hqk", d_o, v, preferred_element_type=F32)
    ds = (p * (dp - jnp.sum(p * dp, axis=-1, keepdims=True))).astype(BF)
    d_q = (jnp.einsum("hqk,khd->qhd", ds, k, preferred_element_type=F32) * 0.125).astype(BF)
    d_k = jnp.einsum("hqk,qhd->khd", ds, q, preferred_element_type=F32) * 0.125
    d_v = jnp.einsum("hqk,qhd->khd", pb, d_o, preferred_element_type=F32)
    d_q = d_q.reshape(my_rows, heads * head)
    d_kv = jnp.concatenate([d_k.reshape(half_rows, -1), d_v.reshape(half_rows, -1)], axis=1).astype(BF)
    pairs = [[h * parts + j for j in range(parts)] for h in range(tp_n // parts)]
    d_kv = lax.psum_scatter(d_kv.astype(F32), "tp", scatter_dimension=0, tiled=True, axis_index_groups=pairs)
    d_k, d_v = jnp.split(d_kv.astype(BF), 2, axis=1)
    g_q = mm_lt(x_mine, d_q)
    g_k = mm_lt(x_mine, d_k)
    g_v = mm_lt(x_mine, d_v)
    d_x = (d_r1 + mm_rt(d_q, wq) + mm_rt(d_k, wk) + mm_rt(d_v, wv)).astype(BF)

    layer_out = scatter_group(mm(pick, y.astype(BF)).astype(BF), own_rows)
    input_grad = scatter_group(mm(pick_nat, d_x).astype(BF), own_rows)

    outs = []
    for g, wd in zip((g_q, g_k, g_v, g_out, g_up, g_down), widths):
        outs.append(g.astype(BF).reshape(rows_n, width // rows_n, tp_n, wd).transpose(0, 2, 1, 3))
    packed_g = jnp.concatenate(outs, axis=3)
    packed_g = packed_g.reshape(rows_n * tp_n, width // rows_n, -1)
    mine_g = lax.psum_scatter(packed_g, ALL, scatter_dimension=0, tiled=True)[0].astype(F32)
    gm, at = [], 0
    for wd in widths:
        gm.append(mine_g[:, at:at + wd])
        at += wd

    def total(a):
        return jnp.sum(a.astype(F32), axis=0)

    def split_bias(a, wd):
        return a.reshape(tp_n, heads_l, rows_n, wd).transpose(2, 0, 1, 3).reshape(rows_n * tp_n, heads_l, wd)

    small_b = jnp.concatenate([
        split_bias(total(d_q), head_l), split_bias(total(d_v), head_l), split_bias(total(d_pre), b_up.shape[1])],
        axis=2).reshape(rows_n * tp_n, -1)
    vec_g = jnp.stack([total(d_r1), total(d_mid * n1), total(d_mid), total(d_r2), total(dy * n2), total(dy)])
    small_v = vec_g.reshape(6, rows_n, 1, width // rows_n).transpose(1, 2, 0, 3)
    small_v = jnp.broadcast_to(small_v, (rows_n, tp_n, 6, width // rows_n)).reshape(rows_n * tp_n, -1)
    small = jnp.concatenate([small_b, small_v], axis=1)
    small = lax.psum_scatter(small, ALL, scatter_dimension=0, tiled=True)[0]
    nb = small_b.shape[1]
    sb = small[:nb].reshape(heads_l, -1)
    sv = small[nb:].reshape(6, -1)
    return (layer_out, input_grad, gm[0], sb[:, :head_l], gm[1], gm[2], sb[:, head_l:2 * head_l], gm[3],
            sv[0], sv[1], sv[2], gm[4], sb[:, 2 * head_l:], gm[5], sv[3], sv[4], sv[5])


def specs():
    tok = P(None, ALL, None)
    grp = P(None, "fsdp", None)
    mat = P(ROWS, "tp")
    bias = P("tp", ROWS)
    vec = P(ROWS)
    ins = (tok, tok, grp, grp, mat, bias, mat, mat, bias, mat, vec, vec, vec, mat, bias, mat, vec, vec, vec)
    return ins, (tok, tok) + ins[4:]


CHUNK = 32
VMEM_MAX = 62 * 1024 * 1024


def block_mat(ref, t):
    n, rows, width = ref.shape[1:]
    return ref[t].reshape(n * rows, width)


def row_facts(meta, group_n):
    c, t = lax.axis_index("ctx"), lax.axis_index("tp")
    lens = meta[4:5, :].astype(F32)
    lane = lax.broadcasted_iota(jnp.int32, lens.shape, 1)

    def one(k):
        return jnp.sum(jnp.where(lane == 3 * c + k, lens, 0.0), axis=1, keepdims=True).astype(jnp.int32)

    l0, l1 = one(0), one(1)
    half = group_n // 2
    first = jnp.where(l0 == half, 0, jnp.where(l1 == half, l0, l0 + l1))
    return first + (t % 2) * half, l0, l0 + l1


def wrap(v, group_n):
    return jnp.where(v >= group_n, v - group_n, v)


def pick_row(block, c):
    row = lax.broadcasted_iota(jnp.int32, block.shape, 0)
    return jnp.sum(jnp.where(row == c, block.astype(F32), 0.0), axis=0, keepdims=True).astype(jnp.int32)


def chunks(total, fn, size=CHUNK):
    def step(i, _):
        fn(pl.ds(pl.multiple_of(i * size, size), size))
        return 0
    lax.fori_loop(0, total // size, step, 0)


def each_t(fn):
    def step(t, _):
        fn(t)
        return 0
    lax.fori_loop(0, 4, step, 0)


def k1_kernel(head, gath, meta_ref, group, gg, dq_out, dkv_out, xm_out, da_out, op_out, dr1_out, y_out, vec_out,
              w_a, w_u, w_d, small, xh, dy, qkv, probs, sbuf, pb, pb2, acc, mid, midb, n1, inv1, gelu_d, act, n2, df, big, bias,
              g_u, g_d, sem):
    f, c, t_me = lax.axis_index("fsdp"), lax.axis_index("ctx"), lax.axis_index("tp")
    width = xh.shape[1]
    s_n, r_n, n_n = xh.shape[0], dy.shape[0], group.shape[1]
    wl = w_a.shape[2]
    hw = width // 4
    per_t = hw // head

    loads = [pltpu.make_async_copy(gath.at[:, :, pl.ds(wl * i, wl)], ref, sem.at[i])
             for i, ref in enumerate((w_a, w_u, w_d))]
    loads.append(pltpu.make_async_copy(gath.at[:, :, pl.ds(3 * wl, 16)], small, sem.at[3]))
    for d in (loads[3], loads[0], loads[1], loads[2]):
        d.start()

    meta = meta_ref[t_me // 2]
    start, e0, e1 = row_facts(meta, n_n)
    order = pick_row(meta[0:4, :], c)

    def half_rows(rows):
        nat = wrap(start + rows.start + lax.broadcasted_iota(jnp.int32, (rows.size, 1), 0), n_n)
        sel = (lax.broadcasted_iota(jnp.int32, (rows.size, n_n), 1) == nat).astype(F32).astype(BF)
        xh[rows, :] = mm(sel, group[0]).astype(BF)
    chunks(s_n, half_rows, 128)

    def quarter_rows(rows):
        nat = wrap(start + f * r_n + rows.start + lax.broadcasted_iota(jnp.int32, (rows.size, 1), 0), n_n)
        sel = (order == nat).astype(F32).astype(BF)
        dy[rows, :] = mm(sel, group[1])
    chunks(r_n, quarter_rows, 128)

    mine = pl.ds(pl.multiple_of(f * r_n, r_n), r_n)
    loads[3].wait()
    for t in range(4):
        bias[t] = jnp.sum(small[t].astype(F32), axis=0)
    vec = bias[0]
    bo, mg, ms, bd, eg, es = (vec[i:i + 1, :] for i in range(6))
    loads[0].wait()

    nat_row = wrap(start + lax.broadcasted_iota(jnp.int32, (1, s_n), 1), n_n)
    seg_row = (nat_row >= e0).astype(jnp.int32) + (nat_row >= e1).astype(jnp.int32)
    nat_q = wrap(start + f * r_n + lax.broadcasted_iota(jnp.int32, (r_n, 1), 0), n_n)
    same = ((nat_q >= e0).astype(jnp.int32) + (nat_q >= e1).astype(jnp.int32)) == seg_row

    def forward_t(t):
        row6 = bias[t][6:7, :]
        qkv[t] = (mm(xh[...], block_mat(w_a, t)) + row6).astype(BF)
        q3 = qkv[t, mine, :]
        kv = qkv[t]
        outs = []
        for h in range(per_t):
            lo = hw + h * head
            sbuf[...] = mm_rt(q3[:, lo:lo + head], kv[:, lo + hw:lo + hw + head])
            at = t * per_t + h

            s = jnp.where(same, sbuf[...] * 0.125, MASKED)
            p = jnp.exp(s - jnp.max(s, axis=1, keepdims=True))
            p = p * (1.0 / jnp.sum(p, axis=1, keepdims=True))
            probs[at] = p
            pb[...] = p.astype(BF)
            outs.append(mm(pb[...], kv[:, lo + 2 * hw:lo + 2 * hw + head]).astype(BF))
        outs.append(jnp.zeros((r_n, width - hw), BF))
        op_out[t] = jnp.concatenate(outs, axis=1)
    each_t(forward_t)

    xm_out[...] = xh[mine, :]
    acc[...] = xm_out[...].astype(F32) + bo

    def out_t(t):
        acc[...] += mm_rt(op_out[t], block_mat(w_a, t))
    each_t(out_t)

    def norm_rows(u):
        centre = u - jnp.mean(u, axis=-1, keepdims=True)
        inv = lax.rsqrt(jnp.mean(centre * centre, axis=-1, keepdims=True) + EPS)
        return centre * inv, inv

    def first_norm(rows):
        n, inv = norm_rows(acc[rows, :])
        n1[rows, :] = n
        inv1[rows, :] = jnp.broadcast_to(inv, (rows.size, 128))
        m = n * mg + ms
        mid[rows, :] = m
        midb[rows, :] = m.astype(BF)
        acc[rows, :] = m + bd
    chunks(r_n, first_norm)

    loads[1].wait()
    loads[2].wait()

    def ffn_t(t):
        row7 = bias[t][7:8, :]
        big[...] = mm(midb[...], block_mat(w_u, t))

        def gelu(rows):
            u = big[rows, :] + row7
            cdf = 0.5 * (1.0 + lax.erf(u * 0.7071067811865476))
            pdf = 0.3989422804014327 * jnp.exp(-0.5 * u * u)
            act[t, rows, :] = (u * cdf).astype(BF)
            gelu_d[t, rows, :] = cdf + u * pdf
        chunks(r_n, gelu, 16)
        acc[...] += mm_rt(act[t], block_mat(w_d, t))
    each_t(ffn_t)

    vec_out[...] = jnp.zeros_like(vec_out)

    def add_vec(i, v):
        vec_out[i] += jnp.sum(v.reshape(-1, 8, v.shape[1]), axis=0)

    def second_norm(rows):
        n, inv = norm_rows(acc[rows, :])
        y_out[rows, :] = (n * eg + es).astype(BF)
        g = dy[rows, :]
        e = g * eg
        d = (e - jnp.mean(e, axis=-1, keepdims=True) - n * jnp.mean(e * n, axis=-1, keepdims=True)) * inv
        add_vec(3, d)
        add_vec(4, g * n)
        add_vec(5, g)
        df[rows, :] = d.astype(BF)
        acc[rows, :] = d
    chunks(r_n, second_norm)

    def ffn_back_t(t):
        big[...] = mm(df[...], block_mat(w_d, t))

        def times(rows):
            d = (big[rows, :] * gelu_d[t, rows, :]).astype(BF)
            n2[rows, :] = d
            add_vec(8 + t, d.astype(F32))
        chunks(r_n, times)
        acc[...] += mm_rt(n2[...], block_mat(w_u, t))
        g_d[t] = mm_lt(df[...], act[t]).astype(BF).reshape(g_d.shape[1:])
        g_u[t] = mm_lt(midb[...], n2[...]).astype(BF).reshape(g_u.shape[1:])
    each_t(ffn_back_t)
    stores = [pltpu.make_async_copy(g_u, gg.at[:, :, pl.ds(wl, wl)], sem.at[4]),
              pltpu.make_async_copy(g_d, gg.at[:, :, pl.ds(2 * wl, wl)], sem.at[5])]
    for d in stores:
        d.start()

    def first_norm_back(rows):
        g, n = acc[rows, :], n1[rows, :]
        e = g * mg
        d = (e - jnp.mean(e, axis=-1, keepdims=True) - n * jnp.mean(e * n, axis=-1, keepdims=True)) * inv1[rows, :][:, 0:1]
        add_vec(0, d)
        add_vec(1, g * n)
        add_vec(2, g)
        dr1_out[rows, :] = d
        da_out[rows, :] = d.astype(BF)
    chunks(r_n, first_norm_back)

    def attn_back_t(t):
        do = mm(da_out[...], block_mat(w_a, t)).astype(BF)
        q3 = qkv[t, mine, :]
        kv = qkv[t]
        dqs, dks, dvs = [], [], []
        for h in range(per_t):
            lo = hw + h * head
            at = t * per_t + h
            do_h = do[:, h * head:(h + 1) * head]
            sbuf[...] = mm_rt(do_h, kv[:, lo + 2 * hw:lo + 2 * hw + head])

            p, d = probs[at], sbuf[...]
            pb[...] = (p * (d - jnp.sum(p * d, axis=1, keepdims=True))).astype(BF)
            pb2[...] = p.astype(BF)
            dvs.append(mm_lt(pb2[...], do_h))
            dqs.append(mm(pb[...], kv[:, lo + hw:lo + hw + head]) * 0.125)
            dks.append(mm_lt(pb[...], q3[:, lo:lo + head]) * 0.125)
        dq_out[t] = jnp.concatenate([a.astype(BF) for a in dqs], axis=1)
        dkv_out[t] = jnp.concatenate([a.astype(BF) for a in dks + dvs], axis=1)
    each_t(attn_back_t)
    for d in stores:
        d.wait()


def k1(gath, meta, group, head):
    n_t, n_fc, rows, width = gath.shape
    wl = (rows - 16) // 3
    n_n = group.shape[1]
    s_n, r_n = n_n // 2, n_n // 4
    hw = width // 4
    heads = width // head
    v = pltpu.VMEM
    sds = jax.ShapeDtypeStruct
    vm = pl.BlockSpec(memory_space=pltpu.VMEM)
    any_ = pl.BlockSpec(memory_space=pl.ANY)
    wshape = (n_t, n_fc, wl, width)
    return pl.pallas_call(
        functools.partial(k1_kernel, head),
        out_shape=(sds(gath.shape, BF), sds((n_t, r_n, hw), BF), sds((n_t, s_n, 2 * hw), BF), sds((r_n, width), BF),
                   sds((r_n, width), BF), sds((n_t, r_n, width), BF), sds((r_n, width), F32), sds((r_n, width), BF),
                   sds((16, 8, width), F32)),
        in_specs=[any_, vm, vm],
        out_specs=(any_,) + (vm,) * 8,
        scratch_shapes=[
            v(wshape, BF), v(wshape, BF), v(wshape, BF), v((n_t, n_fc, 16, width), BF),
            v((s_n, width), BF), v((r_n, width), F32), v((n_t, s_n, width), BF), v((heads, r_n, s_n), F32),
            v((r_n, s_n), F32), v((r_n, s_n), BF), v((r_n, s_n), BF), v((r_n, width), F32), v((r_n, width), F32), v((r_n, width), BF),
            v((r_n, width), F32), v((r_n, 128), F32), v((n_t, r_n, width), F32), v((n_t, r_n, width), BF),
            v((r_n, width), BF), v((r_n, width), BF), v((r_n, width), F32), v((n_t, 16, width), F32),
            v(wshape, BF), v(wshape, BF), pltpu.SemaphoreType.DMA((6,))],
        compiler_params=pltpu.CompilerParams(vmem_limit_bytes=VMEM_MAX),
        name="layer_main",
    )(gath, meta, group)


def k2_kernel(gath, meta_ref, dq, dkv, dkv_in, xm, da, op, dr1, y, vec, gg_in, gg, place,
              w_a, g_a, g_s, acc, dqkv, sem):
    f, c, t_me = lax.axis_index("fsdp"), lax.axis_index("ctx"), lax.axis_index("tp")
    r_n, width = xm.shape
    n_n = place.shape[1]
    wl = w_a.shape[2]
    hw = width // 4
    load = pltpu.make_async_copy(gath.at[:, :, pl.ds(0, wl)], w_a, sem.at[0])
    load.start()
    meta = meta_ref[t_me // 2]
    start, _, _ = row_facts(meta, n_n)
    order = pick_row(meta[8:12, :], c)
    nat = wrap(start + f * r_n + lax.broadcasted_iota(jnp.int32, (r_n, 1), 0), n_n)
    mine = pl.ds(pl.multiple_of(f * r_n, r_n), r_n)
    acc[...] = dr1[...]
    load.wait()
    lane16 = lax.broadcasted_iota(jnp.int32, (16, width), 0)
    sums = jnp.sum(vec[...], axis=1)

    def grads_t(t):
        both = (dkv[t, mine, :].astype(F32) + dkv_in[t].astype(F32)).astype(BF)
        dqkv[...] = jnp.concatenate([jnp.zeros((r_n, hw), BF), dq[t], both], axis=1)
        d = dqkv[...]
        acc[...] += mm_rt(d, block_mat(w_a, t))
        g_a[t] = (mm_lt(xm[...], d) + mm_lt(da[...], op[t])).astype(BF).reshape(g_a.shape[1:])
        base = jnp.where(lane16 < 6, sums, 0.0)
        base = base + jnp.where(lane16 == 6, jnp.sum(d.astype(F32), axis=0, keepdims=True), 0.0)
        base = base + jnp.where(lane16 == 7, jnp.sum(vec[8 + t], axis=0, keepdims=True), 0.0)
        g_s[t] = jnp.broadcast_to(base.astype(BF)[None], g_s.shape[1:])
    each_t(grads_t)
    stores = [pltpu.make_async_copy(g_a, gg.at[:, :, pl.ds(0, wl)], sem.at[1]),
              pltpu.make_async_copy(g_s, gg.at[:, :, pl.ds(3 * wl, 16)], sem.at[2])]
    for d in stores:
        d.start()
    pick = (order == nat).astype(F32).astype(BF)
    place[0] = mm_lt(pick, y[...]).astype(BF)
    lane = lax.broadcasted_iota(jnp.int32, (1, n_n), 1)
    block = n_n // 16
    at = ((lane // block) % 4) * (4 * block) + (lane // (4 * block)) * block + lane % block
    pick2 = (at == nat).astype(F32).astype(BF)
    place[1] = mm_lt(pick2, acc[...].astype(BF)).astype(BF)
    for d in stores:
        d.wait()


def k2(gath, meta, dq, dkv, dkv_in, xm, da, op, dr1, y, vec, gg):
    n_t, n_fc, rows, width = gath.shape
    wl = (rows - 16) // 3
    r_n = xm.shape[0]
    n_n = 4 * r_n
    v = pltpu.VMEM
    vm = pl.BlockSpec(memory_space=pltpu.VMEM)
    any_ = pl.BlockSpec(memory_space=pl.ANY)
    wshape = (n_t, n_fc, wl, width)
    return pl.pallas_call(
        k2_kernel,
        out_shape=(jax.ShapeDtypeStruct(gg.shape, BF), jax.ShapeDtypeStruct((2, n_n, width), BF)),
        in_specs=[any_] + [vm] * 10 + [any_],
        out_specs=(any_, vm),
        input_output_aliases={11: 0},
        scratch_shapes=[v(wshape, BF), v(wshape, BF), v((n_t, n_fc, 16, width), BF), v((r_n, width), F32),
                        v((r_n, width), BF), pltpu.SemaphoreType.DMA((3,))],
        compiler_params=pltpu.CompilerParams(vmem_limit_bytes=VMEM_MAX),
        name="layer_tail",
    )(gath, meta, dq, dkv, dkv_in, xm, da, op, dr1, y, vec, gg)


def comm_in_kernel(cut, tok, cot, pack, meta, gath, group, meta_all, held, *sems):
    (sem_l, s_e, r_e, s_xg, r_xg, s_xf, s_z, r_z, s_x0, r_x0, s_y0, r_y0, s_y1, r_y1, s_x1, r_x1,
     s_c, r_c, s_c0, r_c0, s_c1, r_c1, s_m, r_m) = sems
    f, c, t = lax.axis_index("fsdp"), lax.axis_index("ctx"), lax.axis_index("tp")
    rows = pack.shape[0]
    h0, h1 = pl.ds(0, cut), pl.ds(cut, rows - cut)
    slot = f * 4 + c
    partner = (1 - f, c, t)
    cx = c + 1 - 2 * (c % 2)
    cy = (c + 2) % 4
    cd = (cx + 2) % 4
    x_nb, y_nb = (f, cx, t), (f, cy, t)
    near, far = 1 + f, 3 * f
    is_near, is_far = t == near, t == far
    receiver = (t // 2) == f

    barrier = pltpu.get_barrier_semaphore()
    peers = [partner] + [(f, (c + i) % 4, t) for i in (1, 2, 3)] + [(f, c, (t + i) % 4) for i in (1, 2, 3)]
    for p in peers:
        pl.semaphore_signal(barrier, inc=1, device_id=p, device_id_type=MESH)
    pl.semaphore_wait(barrier, len(peers))

    pending = []

    def send(src, dst, ssem, rsem, dev, pred=None):
        d = pltpu.make_async_remote_copy(src_ref=src, dst_ref=dst, send_sem=ssem, recv_sem=rsem,
                                         device_id=dev, device_id_type=MESH)
        if pred is None:
            d.start()
        else:
            pl.when(pred)(d.start)
        pending.append((pred, d))

    def arrived(dst, rsem, pred=None):
        d = pltpu.make_async_remote_copy(src_ref=dst, dst_ref=dst, send_sem=s_e.at[0, 0], recv_sem=rsem,
                                         device_id=partner, device_id_type=MESH)
        if pred is None:
            d.wait_recv()
        else:
            pl.when(pred)(d.wait_recv)

    def both(a, b):
        return b if a is None else jnp.logical_and(a, b)

    def first_sends(ten, ref):
        for i in (1, 2, 3):
            to = (c + i) % 4
            send(ref.at[to], held.at[ten, c], s_e.at[ten, i], r_e.at[ten, c], (f, to, t))

    first_sends(0, tok)
    local = [pltpu.make_async_copy(tok.at[c], held.at[0, c], sem_l.at[0]),
             pltpu.make_async_copy(cot.at[c], held.at[1, c], sem_l.at[1]),
             pltpu.make_async_copy(pack, gath.at[t, slot], sem_l.at[2])]
    for d in local:
        d.start()
    send(meta, meta_all.at[f], s_m.at[0], r_m.at[0], partner)
    own_meta = pltpu.make_async_copy(meta, meta_all.at[f], sem_l.at[5])
    own_meta.start()

    def have_column(src, tt, pred=None):
        send(src.at[h0], gath.at[tt, slot, h0], s_x0.at[tt], r_x0.at[tt], x_nb, pred)
        send(src.at[h1], gath.at[tt, slot, h1], s_y1.at[tt], r_y1.at[tt], y_nb, pred)
        send(src.at[h0], gath.at[tt, slot, h0], s_y0.at[0, tt], r_y0.at[0, tt], y_nb, pred)
        send(src.at[h1], gath.at[tt, slot, h1], s_x1.at[0, tt], r_x1.at[0, tt], x_nb, pred)
        send(src, gath.at[tt, slot], s_c.at[tt], r_c.at[tt], partner, pred)

    send(pack, gath.at[t, slot], s_z.at[0, t], r_z.at[t], (f, c, (t + 1) % 4), t < 3)
    send(pack, gath.at[t, slot], s_z.at[1, t], r_z.at[t], (f, c, (t + 3) % 4), t > 0)
    have_column(pack, t)
    first_sends(1, cot)

    def second_sends(ten):
        local[ten].wait()
        for i in (1, 2, 3):
            frm = (c + i) % 4
            arrived(held.at[ten, frm], r_e.at[ten, frm])
        blk = held.at[ten]
        dst = group.at[ten, :, t]
        to = jnp.where(is_near, far, near)
        send(blk, dst, s_xg.at[ten, t], r_xg.at[ten, t], (f, c, to))
        send(blk, dst, s_xf.at[ten, 0, t], r_xg.at[ten, t], partner, receiver)
        keep = pltpu.make_async_copy(blk, dst, sem_l.at[3 + ten])
        pl.when(receiver)(keep.start)
        return keep

    keeps = [second_sends(0)]

    def z_step(d):
        for sign in (-1, 1):
            tt = t + sign * d
            there = tt >= 0 if sign < 0 else tt <= 3
            tt = (tt + 4) % 4
            arrived(gath.at[tt, slot], r_z.at[tt], there)
            on = t < 3 if sign < 0 else t > 0
            nxt = (t + 1) % 4 if sign < 0 else (t + 3) % 4
            if d < 3:
                send(gath.at[tt, slot], gath.at[tt, slot], s_z.at[(1 - sign) // 2 * 0 + (0 if sign < 0 else 1), tt],
                     r_z.at[tt], (f, c, nxt), both(there, on))
            have_column(gath.at[tt, slot], tt, there)

    def relay(ten):
        for i in (1, 2, 3):
            tt = (t + i) % 4
            arrived(group.at[ten, :, tt], r_xg.at[ten, tt], receiver)
            send(group.at[ten, :, tt], group.at[ten, :, tt], s_xg.at[ten, tt], r_xg.at[ten, tt], (f, c, far),
                 jnp.logical_and(is_near, tt != far))
            send(group.at[ten, :, tt], group.at[ten, :, tt], s_xf.at[ten, 0, tt], r_xg.at[ten, tt], partner, receiver)

    z_step(1)
    relay(0)
    keeps.append(second_sends(1))
    z_step(2)
    z_step(3)
    relay(1)

    columns = [(t, None)]
    for d in (1, 2, 3):
        columns.append(((t - d + 4) % 4, t - d >= 0))
        columns.append(((t + d) % 4, t + d <= 3))
    for tt, pred in columns:
        a = gath.at[tt, f * 4 + cx, h0]
        arrived(a, r_x0.at[tt], pred)
        send(a, a, s_y0.at[1, tt], r_y0.at[1, tt], y_nb, pred)
        send(a, a, s_c0.at[0, tt], r_c0.at[0, tt], partner, pred)
        b = gath.at[tt, f * 4 + cy, h1]
        arrived(b, r_y1.at[tt], pred)
        send(b, b, s_x1.at[1, tt], r_x1.at[1, tt], x_nb, pred)
        send(b, b, s_c1.at[0, tt], r_c1.at[0, tt], partner, pred)
    for step in (0, 1):
        for tt, pred in columns:
            a = gath.at[tt, f * 4 + (cy if step == 0 else cd), h0]
            arrived(a, r_y0.at[step, tt], pred)
            send(a, a, s_c0.at[1 + step, tt], r_c0.at[1 + step, tt], partner, pred)
            b = gath.at[tt, f * 4 + (cx if step == 0 else cd), h1]
            arrived(b, r_x1.at[step, tt], pred)
            send(b, b, s_c1.at[1 + step, tt], r_c1.at[1 + step, tt], partner, pred)

    other = (1 - f) * 4
    for tt in range(4):
        arrived(gath.at[tt, other + c], r_c.at[tt])
        for j, cc in enumerate((cx, cy, cd)):
            arrived(gath.at[tt, other + cc, h0], r_c0.at[j, tt])
        for j, cc in enumerate((cy, cx, cd)):
            arrived(gath.at[tt, other + cc, h1], r_c1.at[j, tt])
    for ten in (0, 1):
        for tt in range(4):
            arrived(group.at[ten, :, tt], r_xg.at[ten, tt], jnp.logical_not(receiver))
        pl.when(receiver)(keeps[ten].wait)
    arrived(meta_all.at[1 - f], r_m.at[0])
    own_meta.wait()
    local[2].wait()
    for pred, d in pending:
        if pred is None:
            d.wait_send()
        else:
            pl.when(pred)(d.wait_send)


def comm_in(tok, cot, pack, meta, cut):
    dma = pltpu.SemaphoreType.DMA
    rows, width = pack.shape
    own = tok.shape[1]
    sems = [dma((6,)), dma((2, 4)), dma((2, 4)), dma((2, 4)), dma((2, 4)), dma((2, 1, 4)), dma((2, 4)), dma((4,)),
            dma((4,)), dma((4,)), dma((2, 4)), dma((2, 4)), dma((4,)), dma((4,)), dma((2, 4)), dma((2, 4)),
            dma((4,)), dma((4,)), dma((3, 4)), dma((3, 4)), dma((3, 4)), dma((3, 4)), dma((1,)), dma((1,))]
    any_ = pl.BlockSpec(memory_space=pl.ANY)
    return pl.pallas_call(
        functools.partial(comm_in_kernel, cut),
        out_shape=(jax.ShapeDtypeStruct((4, 8, rows, width), BF),
                   jax.ShapeDtypeStruct((2, 4, 4, own, width), BF), jax.ShapeDtypeStruct((2,) + meta.shape, jnp.int32)),
        in_specs=[any_, any_, pl.BlockSpec(memory_space=pltpu.VMEM), pl.BlockSpec(memory_space=pltpu.VMEM)],
        out_specs=(any_, any_, any_),
        scratch_shapes=[pltpu.VMEM((2, 4, own, width), BF)] + sems,
        compiler_params=pltpu.CompilerParams(collective_id=0, has_side_effects=True),
        name="comm_in",
    )(tok, cot, pack, meta)


def swap_kernel(dkv, got, ssem, rsem):
    f, c, t = lax.axis_index("fsdp"), lax.axis_index("ctx"), lax.axis_index("tp")
    partner = (1 - f, c, t)
    barrier = pltpu.get_barrier_semaphore()
    pl.semaphore_signal(barrier, inc=1, device_id=partner, device_id_type=MESH)
    pl.semaphore_wait(barrier, 1)
    n = got.shape[1]
    d = pltpu.make_async_remote_copy(src_ref=dkv.at[:, pl.ds(pl.multiple_of((1 - f) * n, n), n)], dst_ref=got, send_sem=ssem, recv_sem=rsem,
                                     device_id=partner, device_id_type=MESH)
    d.start()
    d.wait()


def swap(dkv):
    n_t, s_n, w = dkv.shape
    vm = pl.BlockSpec(memory_space=pltpu.VMEM)
    return pl.pallas_call(
        swap_kernel, out_shape=jax.ShapeDtypeStruct((n_t, s_n // 2, w), BF), in_specs=[vm], out_specs=vm,
        scratch_shapes=[pltpu.SemaphoreType.DMA, pltpu.SemaphoreType.DMA],
        compiler_params=pltpu.CompilerParams(collective_id=1, has_side_effects=True), name="core_swap")(dkv)


def comm_out_kernel(cut, gg, place, total, rows_out, own, got0, got1, got2, got3, pl1, pl2, final, *sems):
    (sem_l, s0, r0, s1, r1, s2, r2, s3, r3, su, ru, s_o, r_o) = sems
    f, c, t = lax.axis_index("fsdp"), lax.axis_index("ctx"), lax.axis_index("tp")
    rows = got0.shape[2]
    h0, h1 = pl.ds(0, cut), pl.ds(cut, rows - cut)
    partner = (1 - f, c, t)
    cx = c + 1 - 2 * (c % 2)
    cy = (c + 2) % 4
    cd = (cx + 2) % 4
    x_nb, y_nb = (f, cx, t), (f, cy, t)
    par = t % 2
    z_nb = (f, c, t + 1 - 2 * par)
    to_f, to_t = t // 2, 2 * f + par
    stays = to_f == f

    barrier = pltpu.get_barrier_semaphore()
    peers = [partner] + [(f, (c + i) % 4, t) for i in (1, 2, 3)] + [(f, c, (t + i) % 4) for i in (1, 2, 3)]
    for p in peers:
        pl.semaphore_signal(barrier, inc=1, device_id=p, device_id_type=MESH)

    @pl.when(jnp.logical_not(stays))
    def _():
        for i in range(4):
            pl.semaphore_signal(barrier, inc=1, device_id=(to_f, (c + i) % 4, to_t), device_id_type=MESH)
        pl.semaphore_wait(barrier, len(peers) + 4)

    @pl.when(stays)
    def _():
        pl.semaphore_wait(barrier, len(peers))

    pending = []

    def send(src, dst, ssem, rsem, dev, pred=None):
        d = pltpu.make_async_remote_copy(src_ref=src, dst_ref=dst, send_sem=ssem, recv_sem=rsem,
                                         device_id=dev, device_id_type=MESH)
        if pred is None:
            d.start()
        else:
            pl.when(pred)(d.start)
        pending.append((pred, d))

    def arrived(dst, rsem):
        pltpu.make_async_remote_copy(src_ref=dst, dst_ref=dst, send_sem=su.at[0], recv_sem=rsem,
                                     device_id=partner, device_id_type=MESH).wait_recv()

    turn = [(t + 2) % 4, (t + 1) % 4, (t + 3) % 4, t]
    own_base = pl.ds(pl.multiple_of(f * 4, 4), 4)
    loads = []
    for i, tt in enumerate(turn):
        d = pltpu.make_async_copy(gg.at[tt, own_base], own.at[tt], sem_l.at[i])
        d.start()
        loads.append(d)
    lo = pl.multiple_of(2 * f, 2)
    hi = pl.multiple_of(2 - 2 * f, 2)
    send(place.at[:, pl.ds(hi, 2)], pl1, su.at[0], ru.at[0], partner)
    for tt in turn:
        for i in (1, 2, 3, 0):
            cc = (c + i) % 4
            send(gg.at[tt, 4 * (1 - f) + cc], got0.at[tt, cc], s0.at[tt, cc], r0.at[tt, cc], partner)

    def add_into(dst, src, total_rows, step=16):
        def go(i, _):
            r = pl.ds(pl.multiple_of(i * step, step), step)
            dst[r, :] = dst[r, :] + src[r, :]
            return 0
        lax.fori_loop(0, total_rows // step, go, 0, unroll=2 if (total_rows // step) % 2 == 0 else 1)

    def half_add(dst, src, off, n):
        def go(i, _):
            r = pl.ds(pl.multiple_of(off + i * 16, 16), 16)
            dst[r, :] = dst[r, :] + src[r, :]
            return 0
        lax.fori_loop(0, n // 16, go, 0)

    def roles(i):
        return (cy, cx, y_nb, x_nb) if i % 2 == 0 else (cx, cy, x_nb, y_nb)

    def stage1(i):
        tt = turn[i]
        ca, cb, a_nb, b_nb = roles(i)
        loads[i].wait()
        for k in (1, 2, 3, 0):
            cc = (c + k) % 4
            arrived(got0.at[tt, cc], r0.at[tt, cc])
            add_into(own.at[tt, cc], got0.at[tt, cc], rows)
        for k, cc in enumerate((ca, cd)):
            send(own.at[tt, cc, h0], got1.at[tt, k, h0], s1.at[0, k, tt], r1.at[0, k, tt], a_nb)
        for k, cc in enumerate((cb, cd)):
            send(own.at[tt, cc, h1], got1.at[tt, k, h1], s1.at[1, k, tt], r1.at[1, k, tt], b_nb)

    def stage2(i):
        tt = turn[i]
        ca, cb, a_nb, b_nb = roles(i)
        arrived(got1.at[tt, 1, h0], r1.at[0, 1, tt])
        half_add(own.at[tt, cb], got1.at[tt, 1], 0, cut)
        arrived(got1.at[tt, 1, h1], r1.at[1, 1, tt])
        half_add(own.at[tt, ca], got1.at[tt, 1], cut, rows - cut)
        send(own.at[tt, cb, h0], got2.at[tt, h0], s2.at[0, tt], r2.at[0, tt], b_nb)
        send(own.at[tt, ca, h1], got2.at[tt, h1], s2.at[1, tt], r2.at[1, tt], a_nb)
        arrived(got1.at[tt, 0, h0], r1.at[0, 0, tt])
        half_add(own.at[tt, c], got1.at[tt, 0], 0, cut)
        arrived(got1.at[tt, 0, h1], r1.at[1, 0, tt])
        half_add(own.at[tt, c], got1.at[tt, 0], cut, rows - cut)

    def stage3(i):
        tt = turn[i]
        arrived(got2.at[tt, h0], r2.at[0, tt])
        arrived(got2.at[tt, h1], r2.at[1, tt])
        add_into(own.at[tt, c], got2.at[tt], rows)
        if i < 3:
            send(own.at[tt, c], got3.at[t], s3.at[tt], r3.at[t], (f, c, tt))

    stage1(0)
    stage1(1)
    arrived(pl1, ru.at[0])
    for ten in range(2):
        for k in (0, 1):
            for j in range(4):
                add_into(pl1.at[ten, k, j], place.at[ten, lo + k, j], pl1.shape[3])
    send(pl1.at[:, 1 - par], pl2, su.at[1], ru.at[1], z_nb)
    stage2(0)
    stage1(2)
    stage2(1)
    stage3(0)
    stage1(3)

    arrived(pl2, ru.at[1])
    for ten in range(2):
        for j in range(4):
            add_into(pl2.at[ten, j], pl1.at[ten, par, j], pl2.shape[2])
    moves = []
    for ten in range(2):
        for i in range(4):
            cc = (c + i) % 4
            src, dst = pl2.at[ten, cc], rows_out.at[ten, c]
            away = jnp.logical_not(stays) if i == 0 else None
            send(src, dst, s_o.at[ten, i], r_o.at[ten, c], (to_f, cc, to_t), away)
        moves.append(pltpu.make_async_copy(pl2.at[ten, c], rows_out.at[ten, c], sem_l.at[4 + ten]))
        pl.when(stays)(moves[ten].start)

    stage2(2)
    stage3(1)
    stage2(3)
    stage3(2)
    stage3(3)
    keep = pltpu.make_async_copy(own.at[t, c], got3.at[t], sem_l.at[6])
    keep.start()
    keep.wait()
    for tt in turn[:3]:
        arrived(got3.at[tt], r3.at[tt])

    def go(i, _):
        r = pl.ds(pl.multiple_of(i * 16, 16), 16)
        a, b, e, g = (got3[k, r, :].astype(F32) for k in range(4))
        total[r, :] = ((a + b) + e) + g
        return 0
    lax.fori_loop(0, rows // 16, go, 0)

    for ten in range(2):
        for i in range(4):
            cc = (c + i) % 4
            if i == 0:
                @pl.when(jnp.logical_not(stays))
                def _(ten=ten, cc=cc):
                    arrived(rows_out.at[ten, cc], r_o.at[ten, cc])
                pl.when(stays)(moves[ten].wait)
            else:
                arrived(rows_out.at[ten, cc], r_o.at[ten, cc])
    for pred, d in pending:
        if pred is None:
            d.wait_send()
        else:
            pl.when(pred)(d.wait_send)


def comm_out(gg, place, cut):
    dma = pltpu.SemaphoreType.DMA
    n_t, n_fc, rows, width = gg.shape
    n_n = place.shape[1]
    block = n_n // 16
    place = place.reshape(2, 4, 4, block, width)
    v = pltpu.VMEM
    vm = pl.BlockSpec(memory_space=pltpu.VMEM)
    any_ = pl.BlockSpec(memory_space=pl.ANY)
    return pl.pallas_call(
        functools.partial(comm_out_kernel, cut),
        out_shape=(jax.ShapeDtypeStruct((rows, width), F32), jax.ShapeDtypeStruct((2, 4, block, width), BF)),
        in_specs=[any_, vm],
        out_specs=(vm, vm),
        scratch_shapes=[v((4, 4, rows, width), BF), v((4, 4, rows, width), BF), v((4, 2, rows, width), BF),
                        v((4, rows, width), BF), v((4, rows, width), BF), v((2, 2, 4, block, width), BF),
                        v((2, 4, block, width), BF), v((8, 128), F32),
                        dma((7,)), dma((4, 4)), dma((4, 4)), dma((2, 2, 4)), dma((2, 2, 4)), dma((2, 4)), dma((2, 4)),
                        dma((4,)), dma((4,)), dma((2,)), dma((2,)), dma((2, 4)), dma((2, 4))],
        compiler_params=pltpu.CompilerParams(collective_id=2, has_side_effects=True, vmem_limit_bytes=62 * 1024 * 1024),
        name="comm_out",
    )(gg, place)


def quad_body(tokens_in, cotangent, seq_lengths, row_order, w_query, b_query, w_key, w_value, b_value,
              w_out, b_out, mid_gain, mid_shift, w_up, b_up, w_down, b_down, end_gain, end_shift):
    f, c = lax.axis_index("fsdp"), lax.axis_index("ctx")
    fc = f * 4 + c
    own, width = tokens_in.shape[1:]
    wl = w_query.shape[0]
    heads_l, head_l = b_query.shape
    head = head_l * 8
    up_l = b_up.shape[1]
    hw = width // 4
    mat_a = jnp.concatenate([w_out, w_query, w_key, w_value], axis=1)

    vecs = jnp.stack([b_out, mid_gain, mid_shift, b_down, end_gain, end_shift])
    col = lax.broadcasted_iota(jnp.int32, (1, width), 1)
    row_v = jnp.where(col // wl == fc, jnp.tile(vecs, (1, 8)), 0)
    part = (col % head) // head_l == fc
    three = jnp.stack([jnp.zeros_like(b_query), b_query, jnp.zeros_like(b_query), b_value])
    row_a = jnp.where(part, jnp.tile(three, (1, 1, 8)).reshape(1, width), 0)
    row_u = jnp.where((col % (8 * up_l)) // up_l == fc, jnp.tile(b_up, (1, 8)).reshape(1, width), 0)
    small = jnp.concatenate([row_v, row_a, row_u, jnp.zeros((8, width), BF)], axis=0)
    pack = jnp.concatenate([mat_a, w_up, w_down, small], axis=0)

    order = row_order[:, 0]
    n_n = order.shape[1]
    moved = order.reshape(4, 4, 4, own).transpose(0, 2, 1, 3).reshape(4, n_n)
    lens = jnp.pad(seq_lengths[:, 0].reshape(1, -1), ((0, 3), (0, n_n - 12)))
    meta_own = jnp.concatenate([order, lens, moved, jnp.zeros((4, n_n), jnp.int32)], axis=0)

    cut = (pack.shape[0] // 32) * 16
    gath, group, meta = comm_in(tokens_in, cotangent, pack, meta_own, cut)
    group = group.reshape(2, n_n, width)
    gg, dq, dkv, xm, da, op, dr1, y, vec = k1(gath, meta, group, head)
    dkv_in = swap(dkv)
    gg, place = k2(gath, meta, dq, dkv, dkv_in, xm, da, op, dr1, y, vec, gg)
    total, rows = comm_out(gg, place, cut)

    g_a, g_up, g_down = total[:wl], total[wl:2 * wl], total[2 * wl:3 * wl]
    sv = lax.dynamic_slice(total[3 * wl:3 * wl + 6], (0, fc * wl), (6, wl))
    ba = total[3 * wl + 6].reshape(4, heads_l, head)
    gb = lax.dynamic_slice(ba, (0, 0, fc * head_l), (4, heads_l, head_l))
    gu = lax.dynamic_slice(total[3 * wl + 7].reshape(heads_l, -1), (0, fc * up_l), (heads_l, up_l))
    return (rows[0], rows[1], g_a[:, hw:2 * hw], gb[1], g_a[:, 2 * hw:3 * hw], g_a[:, 3 * hw:], gb[3], g_a[:, :hw],
            sv[0], sv[1], sv[2], g_up, gu, g_down, sv[3], sv[4], sv[5])


def solution(mesh):
    ins, outs = specs()
    small_mesh = (mesh.shape["fsdp"], mesh.shape["ctx"], mesh.shape["tp"]) == (2, 4, 4)
    fn = quad_body if small_mesh else body
    return jax.shard_map(fn, mesh=mesh, in_specs=ins, out_specs=outs, check_vma=False)
```

```python
import functools

import jax
import jax.numpy as jnp
from jax import lax
from jax.experimental import pallas as pl
from jax.experimental.pallas import tpu as pltpu
from jax.sharding import PartitionSpec as P

EPS = 1e-06
MASKED = -1e30
ALL = ("fsdp", "ctx", "tp")
ROWS = ("fsdp", "ctx")
BF = jnp.bfloat16
F32 = jnp.float32


MESH = pl.DeviceIdType.MESH
def mm(a, b):
    return jnp.dot(a, b, preferred_element_type=F32)


def mm_rt(a, b):
    return lax.dot_general(a, b, (((1,), (1,)), ((), ())), preferred_element_type=F32)


def mm_lt(a, b):
    return lax.dot_general(a, b, (((0,), (0,)), ((), ())), preferred_element_type=F32)


def norm(u):
    centre = u - jnp.mean(u, axis=-1, keepdims=True)
    inv = lax.rsqrt(jnp.mean(centre * centre, axis=-1, keepdims=True) + EPS)
    return centre * inv, inv


def norm_back(d, gain, n, inv):
    e = d * gain
    return (e - jnp.mean(e, axis=-1, keepdims=True) - n * jnp.mean(e * n, axis=-1, keepdims=True)) * inv


def phi_both(u):
    cdf = 0.5 * (1.0 + lax.erf(u * 0.7071067811865476))
    pdf = 0.3989422804014327 * jnp.exp(-0.5 * u * u)
    return cdf, pdf


def gather_group(block):
    width = block.shape[-1]
    mine = lax.all_to_all(block, "ctx", 0, 0, tiled=True)
    whole = lax.all_gather(mine, "tp", axis=1, tiled=False)
    return whole.reshape(-1, width)


def scatter_group(rows, own_rows):
    ctx_n, tp_n = lax.axis_size("ctx"), lax.axis_size("tp")
    width = rows.shape[-1]
    blocks = rows.reshape(ctx_n, tp_n * own_rows, width)
    mine = lax.psum_scatter(blocks, "tp", scatter_dimension=1, tiled=True)
    return lax.all_to_all(mine, "ctx", 0, 0, tiled=True)


def body(tokens_in, cotangent, seq_lengths, row_order, w_query, b_query, w_key, w_value, b_value,
         w_out, b_out, mid_gain, mid_shift, w_up, b_up, w_down, b_down, end_gain, end_shift):
    ctx_n, tp_n, fsdp_n = lax.axis_size("ctx"), lax.axis_size("tp"), lax.axis_size("fsdp")
    rows_n = ctx_n * fsdp_n
    c, t = lax.axis_index("ctx"), lax.axis_index("tp")
    micro, own_rows, width = tokens_in.shape
    group_rows = own_rows * ctx_n * tp_n
    half_rows = group_rows // 2
    parts = tp_n // 2
    my_rows = half_rows // parts
    half, quarter = t // parts, t % parts
    heads_l, head_l = b_query.shape
    heads, head = heads_l * tp_n, head_l * rows_n

    mats = (w_query, w_key, w_value, w_out, w_up, w_down)
    widths = [m.shape[1] for m in mats]
    packed = lax.all_gather(jnp.concatenate(mats, axis=1), ALL, axis=0, tiled=False)
    full, at = [], 0
    for wd in widths:
        piece = packed[:, :, at:at + wd].reshape(rows_n, tp_n, -1, wd)
        full.append(piece.transpose(0, 2, 1, 3).reshape(width, tp_n * wd))
        at += wd
    wq, wk, wv, wo, wu, wd_ = full
    vecs = (b_out, mid_gain, mid_shift, b_down, end_gain, end_shift)
    bias = (b_query, b_value, b_up)
    vec_all = lax.all_gather(jnp.stack(vecs), ROWS, axis=1, tiled=True).astype(F32)
    bias_all = lax.all_gather(jnp.concatenate(bias, axis=1), ALL, axis=0, tiled=False).astype(F32)

    def whole_bias(at, wd):
        piece = bias_all[:, :, at:at + wd].reshape(rows_n, tp_n, heads_l, wd)
        return piece.transpose(1, 2, 0, 3).reshape(-1)

    bq = whole_bias(0, head_l)
    bv = whole_bias(head_l, head_l)
    bu = whole_bias(2 * head_l, b_up.shape[1])
    bo, mg, ms, bd, eg, es = (vec_all[i] for i in range(6))

    lens = lax.dynamic_index_in_dim(seq_lengths[:, 0], c, 0, keepdims=False)
    order = lax.dynamic_index_in_dim(row_order[:, 0], c, 0, keepdims=False)
    places = lax.iota(jnp.int32, lens.shape[0])
    longest = jnp.argmax(lens)
    first = jnp.sum(jnp.where(places < longest, lens, 0))
    start = lax.rem(first + half * half_rows, group_rows)
    ends = jnp.cumsum(lens)
    nat = lax.rem(start + lax.iota(jnp.int32, half_rows), group_rows)
    seg = jnp.sum((ends[None, :] <= nat[:, None]).astype(jnp.int32), axis=1)
    q_at = quarter * my_rows
    nat_q = lax.dynamic_slice_in_dim(nat, q_at, my_rows)
    seg_q = lax.dynamic_slice_in_dim(seg, q_at, my_rows)

    x_group = gather_group(tokens_in)
    c_group = gather_group(cotangent)
    x_twice = jnp.concatenate([x_group, x_group[:half_rows]], axis=0)
    x_half = lax.dynamic_slice_in_dim(x_twice, start, half_rows, 0)
    x_mine = lax.dynamic_slice_in_dim(x_half, q_at, my_rows, 0)
    pick = (order[:, None] == nat_q[None, :]).astype(BF)
    pick_nat = (lax.iota(jnp.int32, group_rows)[:, None] == nat_q[None, :]).astype(BF)
    dy = mm_lt(pick, c_group)

    x = x_mine.astype(F32)
    q = (mm(x_mine, wq) + bq).astype(BF).reshape(my_rows, heads, head)
    k = mm(x_half, wk).astype(BF).reshape(half_rows, heads, head)
    v = (mm(x_half, wv) + bv).astype(BF).reshape(half_rows, heads, head)
    same = seg_q[:, None] == seg[None, :]
    s = jnp.einsum("qhd,khd->hqk", q, k, preferred_element_type=F32) * 0.125
    s = jnp.where(same[None], s, MASKED)
    p = jnp.exp(s - jnp.max(s, axis=-1, keepdims=True))
    p = p / jnp.sum(p, axis=-1, keepdims=True)
    pb = p.astype(BF)
    o = jnp.einsum("hqk,khd->qhd", pb, v, preferred_element_type=F32).astype(BF)
    o2 = o.reshape(my_rows, heads * head)
    r1 = x + mm_rt(o2, wo) + bo
    n1, inv1 = norm(r1)
    middle = n1 * mg + ms
    mid_b = middle.astype(BF)
    pre = mm(mid_b, wu) + bu
    cdf, pdf = phi_both(pre)
    act = (pre * cdf).astype(BF)
    r2 = middle + mm_rt(act, wd_) + bd
    n2, inv2 = norm(r2)
    y = n2 * eg + es

    d_r2 = norm_back(dy, eg, n2, inv2)
    df = d_r2.astype(BF)
    d_pre = (mm(df, wd_) * (cdf + pre * pdf)).astype(BF)
    g_down = mm_lt(df, act)
    g_up = mm_lt(mid_b, d_pre)
    d_mid = d_r2 + mm_rt(d_pre, wu)
    d_r1 = norm_back(d_mid, mg, n1, inv1)
    da = d_r1.astype(BF)
    g_out = mm_lt(da, o2)
    d_o = mm(da, wo).astype(BF).reshape(my_rows, heads, head)
    dp = jnp.einsum("qhd,khd->hqk", d_o, v, preferred_element_type=F32)
    ds = (p * (dp - jnp.sum(p * dp, axis=-1, keepdims=True))).astype(BF)
    d_q = (jnp.einsum("hqk,khd->qhd", ds, k, preferred_element_type=F32) * 0.125).astype(BF)
    d_k = jnp.einsum("hqk,qhd->khd", ds, q, preferred_element_type=F32) * 0.125
    d_v = jnp.einsum("hqk,qhd->khd", pb, d_o, preferred_element_type=F32)
    d_q = d_q.reshape(my_rows, heads * head)
    d_kv = jnp.concatenate([d_k.reshape(half_rows, -1), d_v.reshape(half_rows, -1)], axis=1).astype(BF)
    pairs = [[h * parts + j for j in range(parts)] for h in range(tp_n // parts)]
    d_kv = lax.psum_scatter(d_kv.astype(F32), "tp", scatter_dimension=0, tiled=True, axis_index_groups=pairs)
    d_k, d_v = jnp.split(d_kv.astype(BF), 2, axis=1)
    g_q = mm_lt(x_mine, d_q)
    g_k = mm_lt(x_mine, d_k)
    g_v = mm_lt(x_mine, d_v)
    d_x = (d_r1 + mm_rt(d_q, wq) + mm_rt(d_k, wk) + mm_rt(d_v, wv)).astype(BF)

    layer_out = scatter_group(mm(pick, y.astype(BF)).astype(BF), own_rows)
    input_grad = scatter_group(mm(pick_nat, d_x).astype(BF), own_rows)

    outs = []
    for g, wd in zip((g_q, g_k, g_v, g_out, g_up, g_down), widths):
        outs.append(g.astype(BF).reshape(rows_n, width // rows_n, tp_n, wd).transpose(0, 2, 1, 3))
    packed_g = jnp.concatenate(outs, axis=3)
    packed_g = packed_g.reshape(rows_n * tp_n, width // rows_n, -1)
    mine_g = lax.psum_scatter(packed_g, ALL, scatter_dimension=0, tiled=True)[0].astype(F32)
    gm, at = [], 0
    for wd in widths:
        gm.append(mine_g[:, at:at + wd])
        at += wd

    def total(a):
        return jnp.sum(a.astype(F32), axis=0)

    def split_bias(a, wd):
        return a.reshape(tp_n, heads_l, rows_n, wd).transpose(2, 0, 1, 3).reshape(rows_n * tp_n, heads_l, wd)

    small_b = jnp.concatenate([
        split_bias(total(d_q), head_l), split_bias(total(d_v), head_l), split_bias(total(d_pre), b_up.shape[1])],
        axis=2).reshape(rows_n * tp_n, -1)
    vec_g = jnp.stack([total(d_r1), total(d_mid * n1), total(d_mid), total(d_r2), total(dy * n2), total(dy)])
    small_v = vec_g.reshape(6, rows_n, 1, width // rows_n).transpose(1, 2, 0, 3)
    small_v = jnp.broadcast_to(small_v, (rows_n, tp_n, 6, width // rows_n)).reshape(rows_n * tp_n, -1)
    small = jnp.concatenate([small_b, small_v], axis=1)
    small = lax.psum_scatter(small, ALL, scatter_dimension=0, tiled=True)[0]
    nb = small_b.shape[1]
    sb = small[:nb].reshape(heads_l, -1)
    sv = small[nb:].reshape(6, -1)
    return (layer_out, input_grad, gm[0], sb[:, :head_l], gm[1], gm[2], sb[:, head_l:2 * head_l], gm[3],
            sv[0], sv[1], sv[2], gm[4], sb[:, 2 * head_l:], gm[5], sv[3], sv[4], sv[5])


def specs():
    tok = P(None, ALL, None)
    grp = P(None, "fsdp", None)
    mat = P(ROWS, "tp")
    bias = P("tp", ROWS)
    vec = P(ROWS)
    ins = (tok, tok, grp, grp, mat, bias, mat, mat, bias, mat, vec, vec, vec, mat, bias, mat, vec, vec, vec)
    return ins, (tok, tok) + ins[4:]


CHUNK = 32
VMEM_MAX = 62 * 1024 * 1024


def block_mat(ref, t):
    n, rows, width = ref.shape[1:]
    return ref[t].reshape(n * rows, width)


def row_facts(meta, group_n):
    c, t = lax.axis_index("ctx"), lax.axis_index("tp")
    lens = meta[4:5, :].astype(F32)
    lane = lax.broadcasted_iota(jnp.int32, lens.shape, 1)

    def one(k):
        return jnp.sum(jnp.where(lane == 3 * c + k, lens, 0.0), axis=1, keepdims=True).astype(jnp.int32)

    l0, l1 = one(0), one(1)
    half = group_n // 2
    first = jnp.where(l0 == half, 0, jnp.where(l1 == half, l0, l0 + l1))
    return first + (t % 2) * half, l0, l0 + l1


def wrap(v, group_n):
    return jnp.where(v >= group_n, v - group_n, v)


def pick_row(block, c):
    row = lax.broadcasted_iota(jnp.int32, block.shape, 0)
    return jnp.sum(jnp.where(row == c, block.astype(F32), 0.0), axis=0, keepdims=True).astype(jnp.int32)


def chunks(total, fn, size=CHUNK):
    def step(i, _):
        fn(pl.ds(pl.multiple_of(i * size, size), size))
        return 0
    lax.fori_loop(0, total // size, step, 0)


def each_t(fn):
    def step(t, _):
        fn(t)
        return 0
    lax.fori_loop(0, 4, step, 0)


def k1_kernel(head, gath, meta_ref, group, gg, dq_out, dkv_out, xm_out, da_out, op_out, dr1_out, y_out, vec_out,
              w_a, w_u, w_d, small, xh, dy, qkv, probs, sbuf, pb, pb2, acc, mid, midb, n1, inv1, gelu_d, act, n2, df, big, bias,
              g_u, g_d, sem):
    f, c, t_me = lax.axis_index("fsdp"), lax.axis_index("ctx"), lax.axis_index("tp")
    width = xh.shape[1]
    s_n, r_n, n_n = xh.shape[0], dy.shape[0], group.shape[1]
    wl = w_a.shape[2]
    hw = width // 4
    per_t = hw // head

    loads = [pltpu.make_async_copy(gath.at[:, :, pl.ds(wl * i, wl)], ref, sem.at[i])
             for i, ref in enumerate((w_a, w_u, w_d))]
    loads.append(pltpu.make_async_copy(gath.at[:, :, pl.ds(3 * wl, 16)], small, sem.at[3]))
    for d in (loads[3], loads[0], loads[1], loads[2]):
        d.start()

    meta = meta_ref[t_me // 2]
    start, e0, e1 = row_facts(meta, n_n)
    order = pick_row(meta[0:4, :], c)

    def half_rows(rows):
        nat = wrap(start + rows.start + lax.broadcasted_iota(jnp.int32, (rows.size, 1), 0), n_n)
        sel = (lax.broadcasted_iota(jnp.int32, (rows.size, n_n), 1) == nat).astype(F32).astype(BF)
        xh[rows, :] = mm(sel, group[0]).astype(BF)
    chunks(s_n, half_rows, 128)

    def quarter_rows(rows):
        nat = wrap(start + f * r_n + rows.start + lax.broadcasted_iota(jnp.int32, (rows.size, 1), 0), n_n)
        sel = (order == nat).astype(F32).astype(BF)
        dy[rows, :] = mm(sel, group[1])
    chunks(r_n, quarter_rows, 128)

    mine = pl.ds(pl.multiple_of(f * r_n, r_n), r_n)
    loads[3].wait()
    for t in range(4):
        bias[t] = jnp.sum(small[t].astype(F32), axis=0)
    vec = bias[0]
    bo, mg, ms, bd, eg, es = (vec[i:i + 1, :] for i in range(6))
    loads[0].wait()

    nat_row = wrap(start + lax.broadcasted_iota(jnp.int32, (1, s_n), 1), n_n)
    seg_row = (nat_row >= e0).astype(jnp.int32) + (nat_row >= e1).astype(jnp.int32)
    nat_q = wrap(start + f * r_n + lax.broadcasted_iota(jnp.int32, (r_n, 1), 0), n_n)
    same = ((nat_q >= e0).astype(jnp.int32) + (nat_q >= e1).astype(jnp.int32)) == seg_row

    def forward_t(t):
        row6 = bias[t][6:7, :]
        qkv[t] = (mm(xh[...], block_mat(w_a, t)) + row6).astype(BF)
        q3 = qkv[t, mine, :]
        kv = qkv[t]
        outs = []
        for h in range(per_t):
            lo = hw + h * head
            sbuf[...] = mm_rt(q3[:, lo:lo + head], kv[:, lo + hw:lo + hw + head])
            at = t * per_t + h

            s = jnp.where(same, sbuf[...] * 0.125, MASKED)
            p = jnp.exp(s - jnp.max(s, axis=1, keepdims=True))
            p = p * (1.0 / jnp.sum(p, axis=1, keepdims=True))
            probs[at] = p
            pb[...] = p.astype(BF)
            outs.append(mm(pb[...], kv[:, lo + 2 * hw:lo + 2 * hw + head]).astype(BF))
        outs.append(jnp.zeros((r_n, width - hw), BF))
        op_out[t] = jnp.concatenate(outs, axis=1)
    each_t(forward_t)

    xm_out[...] = xh[mine, :]
    acc[...] = xm_out[...].astype(F32) + bo

    def out_t(t):
        acc[...] += mm_rt(op_out[t], block_mat(w_a, t))
    each_t(out_t)

    def norm_rows(u):
        centre = u - jnp.mean(u, axis=-1, keepdims=True)
        inv = lax.rsqrt(jnp.mean(centre * centre, axis=-1, keepdims=True) + EPS)
        return centre * inv, inv

    def first_norm(rows):
        n, inv = norm_rows(acc[rows, :])
        n1[rows, :] = n
        inv1[rows, :] = jnp.broadcast_to(inv, (rows.size, 128))
        m = n * mg + ms
        mid[rows, :] = m
        midb[rows, :] = m.astype(BF)
        acc[rows, :] = m + bd
    chunks(r_n, first_norm)

    loads[1].wait()
    loads[2].wait()

    def ffn_t(t):
        row7 = bias[t][7:8, :]
        big[...] = mm(midb[...], block_mat(w_u, t))

        def gelu(rows):
            u = big[rows, :] + row7
            cdf = 0.5 * (1.0 + lax.erf(u * 0.7071067811865476))
            pdf = 0.3989422804014327 * jnp.exp(-0.5 * u * u)
            act[t, rows, :] = (u * cdf).astype(BF)
            gelu_d[t, rows, :] = cdf + u * pdf
        chunks(r_n, gelu, 16)
        acc[...] += mm_rt(act[t], block_mat(w_d, t))
    each_t(ffn_t)

    vec_out[...] = jnp.zeros_like(vec_out)

    def add_vec(i, v):
        vec_out[i] += jnp.sum(v.reshape(-1, 8, v.shape[1]), axis=0)

    def second_norm(rows):
        n, inv = norm_rows(acc[rows, :])
        y_out[rows, :] = (n * eg + es).astype(BF)
        g = dy[rows, :]
        e = g * eg
        d = (e - jnp.mean(e, axis=-1, keepdims=True) - n * jnp.mean(e * n, axis=-1, keepdims=True)) * inv
        add_vec(3, d)
        add_vec(4, g * n)
        add_vec(5, g)
        df[rows, :] = d.astype(BF)
        acc[rows, :] = d
    chunks(r_n, second_norm)

    def ffn_back_t(t):
        big[...] = mm(df[...], block_mat(w_d, t))

        def times(rows):
            d = (big[rows, :] * gelu_d[t, rows, :]).astype(BF)
            n2[rows, :] = d
            add_vec(8 + t, d.astype(F32))
        chunks(r_n, times)
        acc[...] += mm_rt(n2[...], block_mat(w_u, t))
        g_d[t] = mm_lt(df[...], act[t]).astype(BF).reshape(g_d.shape[1:])
        g_u[t] = mm_lt(midb[...], n2[...]).astype(BF).reshape(g_u.shape[1:])
    each_t(ffn_back_t)
    stores = [pltpu.make_async_copy(g_u, gg.at[:, :, pl.ds(0, wl)], sem.at[4]),
              pltpu.make_async_copy(g_d, gg.at[:, :, pl.ds(wl, wl)], sem.at[5])]
    for d in stores:
        d.start()

    def first_norm_back(rows):
        g, n = acc[rows, :], n1[rows, :]
        e = g * mg
        d = (e - jnp.mean(e, axis=-1, keepdims=True) - n * jnp.mean(e * n, axis=-1, keepdims=True)) * inv1[rows, :][:, 0:1]
        add_vec(0, d)
        add_vec(1, g * n)
        add_vec(2, g)
        dr1_out[rows, :] = d
        da_out[rows, :] = d.astype(BF)
    chunks(r_n, first_norm_back)

    def attn_back_t(t):
        do = mm(da_out[...], block_mat(w_a, t)).astype(BF)
        q3 = qkv[t, mine, :]
        kv = qkv[t]
        dqs, dks, dvs = [], [], []
        for h in range(per_t):
            lo = hw + h * head
            at = t * per_t + h
            do_h = do[:, h * head:(h + 1) * head]
            sbuf[...] = mm_rt(do_h, kv[:, lo + 2 * hw:lo + 2 * hw + head])

            p, d = probs[at], sbuf[...]
            pb[...] = (p * (d - jnp.sum(p * d, axis=1, keepdims=True))).astype(BF)
            pb2[...] = p.astype(BF)
            dvs.append(mm_lt(pb2[...], do_h))
            dqs.append(mm(pb[...], kv[:, lo + hw:lo + hw + head]) * 0.125)
            dks.append(mm_lt(pb[...], q3[:, lo:lo + head]) * 0.125)
        dq_out[t] = jnp.concatenate([a.astype(BF) for a in dqs], axis=1)
        dkv_out[t] = jnp.concatenate([a.astype(BF) for a in dks + dvs], axis=1)
    each_t(attn_back_t)
    for d in stores:
        d.wait()


def k1(gath, meta, group, head):
    n_t, n_fc, rows, width = gath.shape
    wl = (rows - 16) // 3
    n_n = group.shape[1]
    s_n, r_n = n_n // 2, n_n // 4
    hw = width // 4
    heads = width // head
    v = pltpu.VMEM
    sds = jax.ShapeDtypeStruct
    vm = pl.BlockSpec(memory_space=pltpu.VMEM)
    any_ = pl.BlockSpec(memory_space=pl.ANY)
    wshape = (n_t, n_fc, wl, width)
    return pl.pallas_call(
        functools.partial(k1_kernel, head),
        out_shape=(sds((n_t, n_fc, 2 * wl, width), BF), sds((n_t, r_n, hw), BF), sds((n_t, s_n, 2 * hw), BF), sds((r_n, width), BF),
                   sds((r_n, width), BF), sds((n_t, r_n, width), BF), sds((r_n, width), F32), sds((r_n, width), BF),
                   sds((16, 8, width), F32)),
        in_specs=[any_, vm, vm],
        out_specs=(any_,) + (vm,) * 8,
        scratch_shapes=[
            v(wshape, BF), v(wshape, BF), v(wshape, BF), v((n_t, n_fc, 16, width), BF),
            v((s_n, width), BF), v((r_n, width), F32), v((n_t, s_n, width), BF), v((heads, r_n, s_n), F32),
            v((r_n, s_n), F32), v((r_n, s_n), BF), v((r_n, s_n), BF), v((r_n, width), F32), v((r_n, width), F32), v((r_n, width), BF),
            v((r_n, width), F32), v((r_n, 128), F32), v((n_t, r_n, width), F32), v((n_t, r_n, width), BF),
            v((r_n, width), BF), v((r_n, width), BF), v((r_n, width), F32), v((n_t, 16, width), F32),
            v(wshape, BF), v(wshape, BF), pltpu.SemaphoreType.DMA((6,))],
        compiler_params=pltpu.CompilerParams(vmem_limit_bytes=VMEM_MAX),
        name="layer_main",
    )(gath, meta, group)


def comm_in_kernel(cut, tok, cot, pack, meta, gath, group, meta_all, held, *sems):
    (sem_l, s_e, r_e, s_xg, r_xg, s_xf, s_z, r_z, s_x0, r_x0, s_y0, r_y0, s_y1, r_y1, s_x1, r_x1,
     s_c, r_c, s_c0, r_c0, s_c1, r_c1, s_m, r_m) = sems
    f, c, t = lax.axis_index("fsdp"), lax.axis_index("ctx"), lax.axis_index("tp")
    rows = pack.shape[0]
    h0, h1 = pl.ds(0, cut), pl.ds(cut, rows - cut)
    slot = f * 4 + c
    partner = (1 - f, c, t)
    cx = c + 1 - 2 * (c % 2)
    cy = (c + 2) % 4
    cd = (cx + 2) % 4
    x_nb, y_nb = (f, cx, t), (f, cy, t)
    near, far = 1 + f, 3 * f
    is_near, is_far = t == near, t == far
    receiver = (t // 2) == f

    barrier = pltpu.get_barrier_semaphore()
    peers = [partner] + [(f, (c + i) % 4, t) for i in (1, 2, 3)] + [(f, c, (t + i) % 4) for i in (1, 2, 3)]
    for p in peers:
        pl.semaphore_signal(barrier, inc=1, device_id=p, device_id_type=MESH)
    pl.semaphore_wait(barrier, len(peers))

    pending = []

    def send(src, dst, ssem, rsem, dev, pred=None):
        d = pltpu.make_async_remote_copy(src_ref=src, dst_ref=dst, send_sem=ssem, recv_sem=rsem,
                                         device_id=dev, device_id_type=MESH)
        if pred is None:
            d.start()
        else:
            pl.when(pred)(d.start)
        pending.append((pred, d))

    def arrived(dst, rsem, pred=None):
        d = pltpu.make_async_remote_copy(src_ref=dst, dst_ref=dst, send_sem=s_e.at[0, 0], recv_sem=rsem,
                                         device_id=partner, device_id_type=MESH)
        if pred is None:
            d.wait_recv()
        else:
            pl.when(pred)(d.wait_recv)

    def both(a, b):
        return b if a is None else jnp.logical_and(a, b)

    def first_sends(ten, ref):
        for i in (1, 2, 3):
            to = (c + i) % 4
            send(ref.at[to], held.at[ten, c], s_e.at[ten, i], r_e.at[ten, c], (f, to, t))

    first_sends(0, tok)
    local = [pltpu.make_async_copy(tok.at[c], held.at[0, c], sem_l.at[0]),
             pltpu.make_async_copy(cot.at[c], held.at[1, c], sem_l.at[1]),
             pltpu.make_async_copy(pack, gath.at[t, slot], sem_l.at[2])]
    for d in local:
        d.start()
    send(meta, meta_all.at[f], s_m.at[0], r_m.at[0], partner)
    own_meta = pltpu.make_async_copy(meta, meta_all.at[f], sem_l.at[5])
    own_meta.start()

    def have_column(src, tt, pred=None):
        send(src.at[h0], gath.at[tt, slot, h0], s_x0.at[tt], r_x0.at[tt], x_nb, pred)
        send(src.at[h1], gath.at[tt, slot, h1], s_y1.at[tt], r_y1.at[tt], y_nb, pred)
        send(src.at[h0], gath.at[tt, slot, h0], s_y0.at[0, tt], r_y0.at[0, tt], y_nb, pred)
        send(src.at[h1], gath.at[tt, slot, h1], s_x1.at[0, tt], r_x1.at[0, tt], x_nb, pred)
        send(src, gath.at[tt, slot], s_c.at[tt], r_c.at[tt], partner, pred)

    send(pack, gath.at[t, slot], s_z.at[0, t], r_z.at[t], (f, c, (t + 1) % 4), t < 3)
    send(pack, gath.at[t, slot], s_z.at[1, t], r_z.at[t], (f, c, (t + 3) % 4), t > 0)
    have_column(pack, t)
    first_sends(1, cot)

    def second_sends(ten):
        local[ten].wait()
        for i in (1, 2, 3):
            frm = (c + i) % 4
            arrived(held.at[ten, frm], r_e.at[ten, frm])
        blk = held.at[ten]
        dst = group.at[ten, :, t]
        to = jnp.where(is_near, far, near)
        send(blk, dst, s_xg.at[ten, t], r_xg.at[ten, t], (f, c, to))
        send(blk, dst, s_xf.at[ten, 0, t], r_xg.at[ten, t], partner, receiver)
        keep = pltpu.make_async_copy(blk, dst, sem_l.at[3 + ten])
        pl.when(receiver)(keep.start)
        return keep

    keeps = [second_sends(0)]

    def z_step(d):
        for sign in (-1, 1):
            tt = t + sign * d
            there = tt >= 0 if sign < 0 else tt <= 3
            tt = (tt + 4) % 4
            arrived(gath.at[tt, slot], r_z.at[tt], there)
            on = t < 3 if sign < 0 else t > 0
            nxt = (t + 1) % 4 if sign < 0 else (t + 3) % 4
            if d < 3:
                send(gath.at[tt, slot], gath.at[tt, slot], s_z.at[(1 - sign) // 2 * 0 + (0 if sign < 0 else 1), tt],
                     r_z.at[tt], (f, c, nxt), both(there, on))
            have_column(gath.at[tt, slot], tt, there)

    def relay(ten):
        for i in (1, 2, 3):
            tt = (t + i) % 4
            arrived(group.at[ten, :, tt], r_xg.at[ten, tt], receiver)
            send(group.at[ten, :, tt], group.at[ten, :, tt], s_xg.at[ten, tt], r_xg.at[ten, tt], (f, c, far),
                 jnp.logical_and(is_near, tt != far))
            send(group.at[ten, :, tt], group.at[ten, :, tt], s_xf.at[ten, 0, tt], r_xg.at[ten, tt], partner, receiver)

    z_step(1)
    relay(0)
    keeps.append(second_sends(1))
    z_step(2)
    z_step(3)
    relay(1)

    columns = [(t, None)]
    for d in (1, 2, 3):
        columns.append(((t - d + 4) % 4, t - d >= 0))
        columns.append(((t + d) % 4, t + d <= 3))
    for tt, pred in columns:
        a = gath.at[tt, f * 4 + cx, h0]
        arrived(a, r_x0.at[tt], pred)
        send(a, a, s_y0.at[1, tt], r_y0.at[1, tt], y_nb, pred)
        send(a, a, s_c0.at[0, tt], r_c0.at[0, tt], partner, pred)
        b = gath.at[tt, f * 4 + cy, h1]
        arrived(b, r_y1.at[tt], pred)
        send(b, b, s_x1.at[1, tt], r_x1.at[1, tt], x_nb, pred)
        send(b, b, s_c1.at[0, tt], r_c1.at[0, tt], partner, pred)
    for step in (0, 1):
        for tt, pred in columns:
            a = gath.at[tt, f * 4 + (cy if step == 0 else cd), h0]
            arrived(a, r_y0.at[step, tt], pred)
            send(a, a, s_c0.at[1 + step, tt], r_c0.at[1 + step, tt], partner, pred)
            b = gath.at[tt, f * 4 + (cx if step == 0 else cd), h1]
            arrived(b, r_x1.at[step, tt], pred)
            send(b, b, s_c1.at[1 + step, tt], r_c1.at[1 + step, tt], partner, pred)

    other = (1 - f) * 4
    for tt in range(4):
        arrived(gath.at[tt, other + c], r_c.at[tt])
        for j, cc in enumerate((cx, cy, cd)):
            arrived(gath.at[tt, other + cc, h0], r_c0.at[j, tt])
        for j, cc in enumerate((cy, cx, cd)):
            arrived(gath.at[tt, other + cc, h1], r_c1.at[j, tt])
    for ten in (0, 1):
        for tt in range(4):
            arrived(group.at[ten, :, tt], r_xg.at[ten, tt], jnp.logical_not(receiver))
        pl.when(receiver)(keeps[ten].wait)
    arrived(meta_all.at[1 - f], r_m.at[0])
    own_meta.wait()
    local[2].wait()
    for pred, d in pending:
        if pred is None:
            d.wait_send()
        else:
            pl.when(pred)(d.wait_send)


def comm_in(tok, cot, pack, meta, cut):
    dma = pltpu.SemaphoreType.DMA
    rows, width = pack.shape
    own = tok.shape[1]
    sems = [dma((6,)), dma((2, 4)), dma((2, 4)), dma((2, 4)), dma((2, 4)), dma((2, 1, 4)), dma((2, 4)), dma((4,)),
            dma((4,)), dma((4,)), dma((2, 4)), dma((2, 4)), dma((4,)), dma((4,)), dma((2, 4)), dma((2, 4)),
            dma((4,)), dma((4,)), dma((3, 4)), dma((3, 4)), dma((3, 4)), dma((3, 4)), dma((1,)), dma((1,))]
    any_ = pl.BlockSpec(memory_space=pl.ANY)
    return pl.pallas_call(
        functools.partial(comm_in_kernel, cut),
        out_shape=(jax.ShapeDtypeStruct((4, 8, rows, width), BF),
                   jax.ShapeDtypeStruct((2, 4, 4, own, width), BF), jax.ShapeDtypeStruct((2,) + meta.shape, jnp.int32)),
        in_specs=[any_, any_, pl.BlockSpec(memory_space=pltpu.VMEM), pl.BlockSpec(memory_space=pltpu.VMEM)],
        out_specs=(any_, any_, any_),
        scratch_shapes=[pltpu.VMEM((2, 4, own, width), BF)] + sems,
        compiler_params=pltpu.CompilerParams(collective_id=0, has_side_effects=True),
        name="comm_in",
    )(tok, cot, pack, meta)


def tail_out_kernel(gath, meta_ref, dq, dkv, xm, da, op, dr1, y, vec, gg, tot_a, tot_w, rows_out,
                    w_a, g_a, acc, dqkv, dkv_in, place, pl1, pl2, own, w0, w1, w2, w3, a0, a1, a2, a3,
                    sem_l, s_d, r_d, s_u, r_u, s_o, r_o,
                    ws0, wr0, ws1, wr1, ws2, wr2, ws3, wr3, as0, ar0, as1, ar1, as2, ar2, as3, ar3):
    f, c, t = lax.axis_index("fsdp"), lax.axis_index("ctx"), lax.axis_index("tp")
    r_n, width = xm.shape
    n_n = 4 * r_n
    hw = width // 4
    wl = w_a.shape[2]
    partner = (1 - f, c, t)
    cx = c + 1 - 2 * (c % 2)
    cy = (c + 2) % 4
    cd = (cx + 2) % 4
    x_nb, y_nb = (f, cx, t), (f, cy, t)
    par = t % 2
    z_nb = (f, c, t + 1 - 2 * par)
    to_f, to_t = t // 2, 2 * f + par
    stays = to_f == f

    load_a = pltpu.make_async_copy(gath.at[:, :, pl.ds(0, wl)], w_a, sem_l.at[0])
    load_a.start()
    turn = [(t + 2) % 4, (t + 1) % 4, (t + 3) % 4, t]
    loads = []
    for i, tt in enumerate(turn):
        d = pltpu.make_async_copy(gg.at[tt, pl.ds(pl.multiple_of(f * 4, 4), 4)], own.at[tt], sem_l.at[1 + i])
        d.start()
        loads.append(d)

    barrier = pltpu.get_barrier_semaphore()
    peers = [partner] + [(f, (c + i) % 4, t) for i in (1, 2, 3)] + [(f, c, (t + i) % 4) for i in (1, 2, 3)]
    for p in peers:
        pl.semaphore_signal(barrier, inc=1, device_id=p, device_id_type=MESH)

    @pl.when(jnp.logical_not(stays))
    def _():
        for i in range(4):
            pl.semaphore_signal(barrier, inc=1, device_id=(to_f, (c + i) % 4, to_t), device_id_type=MESH)
        pl.semaphore_wait(barrier, len(peers) + 4)

    @pl.when(stays)
    def _():
        pl.semaphore_wait(barrier, len(peers))

    pending = []

    def send(src, dst, ssem, rsem, dev, pred=None):
        d = pltpu.make_async_remote_copy(src_ref=src, dst_ref=dst, send_sem=ssem, recv_sem=rsem,
                                         device_id=dev, device_id_type=MESH)
        if pred is None:
            d.start()
        else:
            pl.when(pred)(d.start)
        pending.append((pred, d))

    def arrived(dst, rsem):
        pltpu.make_async_remote_copy(src_ref=dst, dst_ref=dst, send_sem=s_d, recv_sem=rsem,
                                     device_id=partner, device_id_type=MESH).wait_recv()

    def add_into(dst, src, off, n):
        def go(i, _):
            r = pl.ds(pl.multiple_of(off + i * 16, 16), 16)
            dst[r, :] = dst[r, :] + src[r, :]
            return 0
        lax.fori_loop(0, n // 16, go, 0)

    def make_pass(mine, theirs, g0, g1, g2, g3, cut, sems):
        q0, p0, q1, p1, q2, p2, q3, p3 = sems
        rows = g0.shape[2]
        h0, h1 = pl.ds(0, cut), pl.ds(cut, rows - cut)

        def roles(i):
            return (cy, cx, y_nb, x_nb) if i % 2 == 0 else (cx, cy, x_nb, y_nb)

        def stage0(i):
            tt = turn[i]
            for k in (1, 2, 3, 0):
                cc = (c + k) % 4
                send(theirs(tt, cc), g0.at[tt, cc], q0.at[tt, cc], p0.at[tt, cc], partner)

        def stage1(i):
            tt = turn[i]
            ca, cb, a_nb, b_nb = roles(i)
            for k in (1, 2, 3, 0):
                cc = (c + k) % 4
                arrived(g0.at[tt, cc], p0.at[tt, cc])
                add_into(mine(tt, cc), g0.at[tt, cc], 0, rows)
            for k, cc in enumerate((ca, cd)):
                send(mine(tt, cc).at[h0], g1.at[tt, k, h0], q1.at[0, k, tt], p1.at[0, k, tt], a_nb)
            for k, cc in enumerate((cb, cd)):
                send(mine(tt, cc).at[h1], g1.at[tt, k, h1], q1.at[1, k, tt], p1.at[1, k, tt], b_nb)

        def stage2(i):
            tt = turn[i]
            ca, cb, a_nb, b_nb = roles(i)
            arrived(g1.at[tt, 1, h0], p1.at[0, 1, tt])
            add_into(mine(tt, cb), g1.at[tt, 1], 0, cut)
            arrived(g1.at[tt, 1, h1], p1.at[1, 1, tt])
            add_into(mine(tt, ca), g1.at[tt, 1], cut, rows - cut)
            send(mine(tt, cb).at[h0], g2.at[tt, h0], q2.at[0, tt], p2.at[0, tt], b_nb)
            send(mine(tt, ca).at[h1], g2.at[tt, h1], q2.at[1, tt], p2.at[1, tt], a_nb)
            arrived(g1.at[tt, 0, h0], p1.at[0, 0, tt])
            add_into(mine(tt, c), g1.at[tt, 0], 0, cut)
            arrived(g1.at[tt, 0, h1], p1.at[1, 0, tt])
            add_into(mine(tt, c), g1.at[tt, 0], cut, rows - cut)

        def stage3(i):
            tt = turn[i]
            arrived(g2.at[tt, h0], p2.at[0, tt])
            arrived(g2.at[tt, h1], p2.at[1, tt])
            add_into(mine(tt, c), g2.at[tt], 0, rows)
            if i < 3:
                send(mine(tt, c), g3.at[t], q3.at[tt], p3.at[t], (f, c, tt))

        def finish(total, ls):
            keep = pltpu.make_async_copy(mine(t, c), g3.at[t], ls)
            keep.start()
            keep.wait()
            for tt in turn[:3]:
                arrived(g3.at[tt], p3.at[tt])

            def go(i, _):
                r = pl.ds(pl.multiple_of(i * 16, 16), 16)
                a, b, e, g = (g3[k, r, :].astype(F32) for k in range(4))
                total[r, :] = ((a + b) + e) + g
                return 0
            lax.fori_loop(0, rows // 16, go, 0)
        return stage0, stage1, stage2, stage3, finish

    wp = make_pass(lambda tt, cc: own.at[tt, cc], lambda tt, cc: gg.at[tt, 4 * (1 - f) + cc],
                   w0, w1, w2, w3, own.shape[2] // 2, (ws0, wr0, ws1, wr1, ws2, wr2, ws3, wr3))
    a_rows = g_a.shape[2]
    ap = make_pass(lambda tt, cc: g_a.at[tt, 4 * f + cc], lambda tt, cc: g_a.at[tt, 4 * (1 - f) + cc],
                   a0, a1, a2, a3, (a_rows // 32) * 16, (as0, ar0, as1, ar1, as2, ar2, as3, ar3))

    lo = pl.multiple_of(2 * f, 2)
    hi = pl.multiple_of(2 - 2 * f, 2)
    block = place.shape[3]
    moves = [pltpu.make_async_copy(pl2.at[ten, c], rows_out.at[ten, c], sem_l.at[5 + ten]) for ten in range(2)]

    def rows1(ten):
        send(place.at[ten, pl.ds(hi, 2)], pl1.at[ten], s_u.at[0, ten], r_u.at[0, ten], partner)

    def rows2(ten):
        arrived(pl1.at[ten], r_u.at[0, ten])
        for k in (0, 1):
            for j in range(4):
                add_into(pl1.at[ten, k, j], place.at[ten, lo + k, j], 0, block)
        send(pl1.at[ten, 1 - par], pl2.at[ten], s_u.at[1, ten], r_u.at[1, ten], z_nb)

    def rows3(ten):
        arrived(pl2.at[ten], r_u.at[1, ten])
        for j in range(4):
            add_into(pl2.at[ten, j], pl1.at[ten, par, j], 0, block)
        for i in range(4):
            cc = (c + i) % 4
            away = jnp.logical_not(stays) if i == 0 else None
            send(pl2.at[ten, cc], rows_out.at[ten, c], s_o.at[ten, i], r_o.at[ten, c], (to_f, cc, to_t), away)
        pl.when(stays)(moves[ten].start)

    meta = meta_ref[t // 2]
    start, _, _ = row_facts(meta, n_n)
    nat = wrap(start + f * r_n + lax.broadcasted_iota(jnp.int32, (r_n, 1), 0), n_n)
    mine_rows = pl.ds(pl.multiple_of(f * r_n, r_n), r_n)
    lane16 = lax.broadcasted_iota(jnp.int32, (16, width), 0)

    def grads_t(k):
        both = (dkv[k, mine_rows, :].astype(F32) + dkv_in[k].astype(F32)).astype(BF)
        dqkv[...] = jnp.concatenate([jnp.zeros((r_n, hw), BF), dq[k], both], axis=1)
        d = dqkv[...]
        acc[...] += mm_rt(d, block_mat(w_a, k))
        g_a[k, :, 0:wl, :] = (mm_lt(xm[...], d) + mm_lt(da[...], op[k])).astype(BF).reshape(g_a.shape[1], wl, width)
        sums = jnp.sum(vec[...], axis=1)
        base = jnp.where(lane16 < 6, sums, 0.0)
        base = base + jnp.where(lane16 == 6, jnp.sum(d.astype(F32), axis=0, keepdims=True), 0.0)
        base = base + jnp.where(lane16 == 7, jnp.sum(vec[8 + k], axis=0, keepdims=True), 0.0)
        g_a[k, :, wl:wl + 16, :] = jnp.broadcast_to(base.astype(BF)[None], (g_a.shape[1], 16, width))

    def two(first):
        def step(k, _):
            grads_t(k)
            return 0
        lax.fori_loop(first, first + 2, step, 0)

    n_d = dkv_in.shape[1]
    send(dkv.at[:, pl.ds(pl.multiple_of((1 - f) * n_d, n_d), n_d)], dkv_in, s_d, r_d, partner)
    wp[0](0)
    wp[0](1)
    order = pick_row(meta[8:12, :], c)
    pick = (order == nat).astype(F32).astype(BF)
    place[0] = mm_lt(pick, y[...]).astype(BF).reshape(place.shape[1:])
    acc[...] = dr1[...]
    wp[0](2)
    rows1(0)
    wp[0](3)
    loads[0].wait()
    wp[1](0)
    loads[1].wait()
    wp[1](1)
    arrived(dkv_in, r_d)
    load_a.wait()
    two(0)
    rows2(0)
    wp[2](0)
    loads[2].wait()
    wp[1](2)
    two(2)
    wp[2](1)
    wp[3](0)
    loads[3].wait()
    wp[1](3)
    rows3(0)
    for i in range(4):
        ap[0](i)
    lane = lax.broadcasted_iota(jnp.int32, (1, n_n), 1)
    at = ((lane // block) % 4) * (4 * block) + (lane // (4 * block)) * block + lane % block
    pick2 = (at == nat).astype(F32).astype(BF)
    place[1] = mm_lt(pick2, acc[...].astype(BF)).astype(BF).reshape(place.shape[1:])
    wp[2](2)
    wp[3](1)
    rows1(1)
    ap[1](0)
    wp[2](3)
    wp[3](2)
    rows2(1)
    ap[1](1)
    ap[2](0)
    wp[3](3)
    rows3(1)
    ap[1](2)
    ap[2](1)
    ap[3](0)
    ap[1](3)
    wp[4](tot_w, sem_l.at[7])
    ap[2](2)
    ap[3](1)
    ap[2](3)
    ap[3](2)
    ap[3](3)
    ap[4](tot_a, sem_l.at[8])

    for ten in range(2):
        for i in range(4):
            cc = (c + i) % 4
            if i == 0:
                @pl.when(jnp.logical_not(stays))
                def _(ten=ten, cc=cc):
                    arrived(rows_out.at[ten, cc], r_o.at[ten, cc])
                pl.when(stays)(moves[ten].wait)
            else:
                arrived(rows_out.at[ten, cc], r_o.at[ten, cc])
    for pred, d in pending:
        if pred is None:
            d.wait_send()
        else:
            pl.when(pred)(d.wait_send)


def tail_out(gath, meta, dq, dkv, xm, da, op, dr1, y, vec, gg):
    n_t, n_fc, rows, width = gath.shape
    wl = (rows - 16) // 3
    r_n = xm.shape[0]
    block = r_n // 4
    v = pltpu.VMEM
    dma = pltpu.SemaphoreType.DMA
    vm = pl.BlockSpec(memory_space=pltpu.VMEM)
    any_ = pl.BlockSpec(memory_space=pl.ANY)
    ra, rw = wl + 16, 2 * wl
    def bufs(n):
        return [v((4, 4, n, width), BF), v((4, 2, n, width), BF), v((4, n, width), BF), v((4, n, width), BF)]
    pass_sems = [dma((4, 4)), dma((4, 4)), dma((2, 2, 4)), dma((2, 2, 4)), dma((2, 4)), dma((2, 4)), dma((4,)), dma((4,))]
    return pl.pallas_call(
        tail_out_kernel,
        out_shape=(jax.ShapeDtypeStruct((ra, width), F32), jax.ShapeDtypeStruct((rw, width), F32),
                   jax.ShapeDtypeStruct((2, 4, block, width), BF)),
        in_specs=[any_] + [vm] * 9 + [any_],
        out_specs=(vm, vm, vm),
        scratch_shapes=[v((n_t, n_fc, wl, width), BF), v((n_t, n_fc, ra, width), BF), v((r_n, width), F32),
                        v((r_n, width), BF), v((n_t, r_n, dkv.shape[2]), BF), v((2, 4, 4, block, width), BF),
                        v((2, 2, 4, block, width), BF), v((2, 4, block, width), BF), v((4, 4, rw, width), BF)]
        + bufs(rw) + bufs(ra)
        + [dma((9,)), dma, dma, dma((2, 2)), dma((2, 2)), dma((2, 4)), dma((2, 4))] + pass_sems + pass_sems,
        compiler_params=pltpu.CompilerParams(collective_id=2, has_side_effects=True, vmem_limit_bytes=VMEM_MAX),
        name="tail_out",
    )(gath, meta, dq, dkv, xm, da, op, dr1, y, vec, gg)


def quad_body(tokens_in, cotangent, seq_lengths, row_order, w_query, b_query, w_key, w_value, b_value,
              w_out, b_out, mid_gain, mid_shift, w_up, b_up, w_down, b_down, end_gain, end_shift):
    f, c = lax.axis_index("fsdp"), lax.axis_index("ctx")
    fc = f * 4 + c
    own, width = tokens_in.shape[1:]
    wl = w_query.shape[0]
    heads_l, head_l = b_query.shape
    head = head_l * 8
    up_l = b_up.shape[1]
    hw = width // 4
    mat_a = jnp.concatenate([w_out, w_query, w_key, w_value], axis=1)

    vecs = jnp.stack([b_out, mid_gain, mid_shift, b_down, end_gain, end_shift])
    col = lax.broadcasted_iota(jnp.int32, (1, width), 1)
    row_v = jnp.where(col // wl == fc, jnp.tile(vecs, (1, 8)), 0)
    part = (col % head) // head_l == fc
    three = jnp.stack([jnp.zeros_like(b_query), b_query, jnp.zeros_like(b_query), b_value])
    row_a = jnp.where(part, jnp.tile(three, (1, 1, 8)).reshape(1, width), 0)
    row_u = jnp.where((col % (8 * up_l)) // up_l == fc, jnp.tile(b_up, (1, 8)).reshape(1, width), 0)
    small = jnp.concatenate([row_v, row_a, row_u, jnp.zeros((8, width), BF)], axis=0)
    pack = jnp.concatenate([mat_a, w_up, w_down, small], axis=0)

    order = row_order[:, 0]
    n_n = order.shape[1]
    moved = order.reshape(4, 4, 4, own).transpose(0, 2, 1, 3).reshape(4, n_n)
    lens = jnp.pad(seq_lengths[:, 0].reshape(1, -1), ((0, 3), (0, n_n - 12)))
    meta_own = jnp.concatenate([order, lens, moved, jnp.zeros((4, n_n), jnp.int32)], axis=0)

    cut = (pack.shape[0] // 32) * 16
    gath, group, meta = comm_in(tokens_in, cotangent, pack, meta_own, cut)
    group = group.reshape(2, n_n, width)
    gg, dq, dkv, xm, da, op, dr1, y, vec = k1(gath, meta, group, head)
    tot_a, tot_w, rows = tail_out(gath, meta, dq, dkv, xm, da, op, dr1, y, vec, gg)

    g_a, g_up, g_down = tot_a[:wl], tot_w[:wl], tot_w[wl:]
    sv = lax.dynamic_slice(tot_a[wl:wl + 6], (0, fc * wl), (6, wl))
    ba = tot_a[wl + 6].reshape(4, heads_l, head)
    gb = lax.dynamic_slice(ba, (0, 0, fc * head_l), (4, heads_l, head_l))
    gu = lax.dynamic_slice(tot_a[wl + 7].reshape(heads_l, -1), (0, fc * up_l), (heads_l, up_l))
    return (rows[0], rows[1], g_a[:, hw:2 * hw], gb[1], g_a[:, 2 * hw:3 * hw], g_a[:, 3 * hw:], gb[3], g_a[:, :hw],
            sv[0], sv[1], sv[2], g_up, gu, g_down, sv[3], sv[4], sv[5])


def solution(mesh):
    ins, outs = specs()
    small_mesh = (mesh.shape["fsdp"], mesh.shape["ctx"], mesh.shape["tp"]) == (2, 4, 4)
    fn = quad_body if small_mesh else body
    return jax.shard_map(fn, mesh=mesh, in_specs=ins, out_specs=outs, check_vma=False)
```

```python
import functools

import jax
import jax.numpy as jnp
from jax import lax
from jax.experimental import pallas as pl
from jax.experimental.pallas import tpu as pltpu
from jax.sharding import PartitionSpec as P

EPS = 1e-06
MASKED = -1e30
ALL = ("fsdp", "ctx", "tp")
ROWS = ("fsdp", "ctx")
BF = jnp.bfloat16
F32 = jnp.float32


MESH = pl.DeviceIdType.MESH
def mm(a, b):
    return jnp.dot(a, b, preferred_element_type=F32)


def mm_rt(a, b):
    return lax.dot_general(a, b, (((1,), (1,)), ((), ())), preferred_element_type=F32)


def mm_lt(a, b):
    return lax.dot_general(a, b, (((0,), (0,)), ((), ())), preferred_element_type=F32)


def norm(u):
    centre = u - jnp.mean(u, axis=-1, keepdims=True)
    inv = lax.rsqrt(jnp.mean(centre * centre, axis=-1, keepdims=True) + EPS)
    return centre * inv, inv


def norm_back(d, gain, n, inv):
    e = d * gain
    return (e - jnp.mean(e, axis=-1, keepdims=True) - n * jnp.mean(e * n, axis=-1, keepdims=True)) * inv


def phi_both(u):
    cdf = 0.5 * (1.0 + lax.erf(u * 0.7071067811865476))
    pdf = 0.3989422804014327 * jnp.exp(-0.5 * u * u)
    return cdf, pdf


def gather_group(block):
    width = block.shape[-1]
    mine = lax.all_to_all(block, "ctx", 0, 0, tiled=True)
    whole = lax.all_gather(mine, "tp", axis=1, tiled=False)
    return whole.reshape(-1, width)


def scatter_group(rows, own_rows):
    ctx_n, tp_n = lax.axis_size("ctx"), lax.axis_size("tp")
    width = rows.shape[-1]
    blocks = rows.reshape(ctx_n, tp_n * own_rows, width)
    mine = lax.psum_scatter(blocks, "tp", scatter_dimension=1, tiled=True)
    return lax.all_to_all(mine, "ctx", 0, 0, tiled=True)


def body(tokens_in, cotangent, seq_lengths, row_order, w_query, b_query, w_key, w_value, b_value,
         w_out, b_out, mid_gain, mid_shift, w_up, b_up, w_down, b_down, end_gain, end_shift):
    ctx_n, tp_n, fsdp_n = lax.axis_size("ctx"), lax.axis_size("tp"), lax.axis_size("fsdp")
    rows_n = ctx_n * fsdp_n
    c, t = lax.axis_index("ctx"), lax.axis_index("tp")
    micro, own_rows, width = tokens_in.shape
    group_rows = own_rows * ctx_n * tp_n
    half_rows = group_rows // 2
    parts = tp_n // 2
    my_rows = half_rows // parts
    half, quarter = t // parts, t % parts
    heads_l, head_l = b_query.shape
    heads, head = heads_l * tp_n, head_l * rows_n

    mats = (w_query, w_key, w_value, w_out, w_up, w_down)
    widths = [m.shape[1] for m in mats]
    packed = lax.all_gather(jnp.concatenate(mats, axis=1), ALL, axis=0, tiled=False)
    full, at = [], 0
    for wd in widths:
        piece = packed[:, :, at:at + wd].reshape(rows_n, tp_n, -1, wd)
        full.append(piece.transpose(0, 2, 1, 3).reshape(width, tp_n * wd))
        at += wd
    wq, wk, wv, wo, wu, wd_ = full
    vecs = (b_out, mid_gain, mid_shift, b_down, end_gain, end_shift)
    bias = (b_query, b_value, b_up)
    vec_all = lax.all_gather(jnp.stack(vecs), ROWS, axis=1, tiled=True).astype(F32)
    bias_all = lax.all_gather(jnp.concatenate(bias, axis=1), ALL, axis=0, tiled=False).astype(F32)

    def whole_bias(at, wd):
        piece = bias_all[:, :, at:at + wd].reshape(rows_n, tp_n, heads_l, wd)
        return piece.transpose(1, 2, 0, 3).reshape(-1)

    bq = whole_bias(0, head_l)
    bv = whole_bias(head_l, head_l)
    bu = whole_bias(2 * head_l, b_up.shape[1])
    bo, mg, ms, bd, eg, es = (vec_all[i] for i in range(6))

    lens = lax.dynamic_index_in_dim(seq_lengths[:, 0], c, 0, keepdims=False)
    order = lax.dynamic_index_in_dim(row_order[:, 0], c, 0, keepdims=False)
    places = lax.iota(jnp.int32, lens.shape[0])
    longest = jnp.argmax(lens)
    first = jnp.sum(jnp.where(places < longest, lens, 0))
    start = lax.rem(first + half * half_rows, group_rows)
    ends = jnp.cumsum(lens)
    nat = lax.rem(start + lax.iota(jnp.int32, half_rows), group_rows)
    seg = jnp.sum((ends[None, :] <= nat[:, None]).astype(jnp.int32), axis=1)
    q_at = quarter * my_rows
    nat_q = lax.dynamic_slice_in_dim(nat, q_at, my_rows)
    seg_q = lax.dynamic_slice_in_dim(seg, q_at, my_rows)

    x_group = gather_group(tokens_in)
    c_group = gather_group(cotangent)
    x_twice = jnp.concatenate([x_group, x_group[:half_rows]], axis=0)
    x_half = lax.dynamic_slice_in_dim(x_twice, start, half_rows, 0)
    x_mine = lax.dynamic_slice_in_dim(x_half, q_at, my_rows, 0)
    pick = (order[:, None] == nat_q[None, :]).astype(BF)
    pick_nat = (lax.iota(jnp.int32, group_rows)[:, None] == nat_q[None, :]).astype(BF)
    dy = mm_lt(pick, c_group)

    x = x_mine.astype(F32)
    q = (mm(x_mine, wq) + bq).astype(BF).reshape(my_rows, heads, head)
    k = mm(x_half, wk).astype(BF).reshape(half_rows, heads, head)
    v = (mm(x_half, wv) + bv).astype(BF).reshape(half_rows, heads, head)
    same = seg_q[:, None] == seg[None, :]
    s = jnp.einsum("qhd,khd->hqk", q, k, preferred_element_type=F32) * 0.125
    s = jnp.where(same[None], s, MASKED)
    p = jnp.exp(s - jnp.max(s, axis=-1, keepdims=True))
    p = p / jnp.sum(p, axis=-1, keepdims=True)
    pb = p.astype(BF)
    o = jnp.einsum("hqk,khd->qhd", pb, v, preferred_element_type=F32).astype(BF)
    o2 = o.reshape(my_rows, heads * head)
    r1 = x + mm_rt(o2, wo) + bo
    n1, inv1 = norm(r1)
    middle = n1 * mg + ms
    mid_b = middle.astype(BF)
    pre = mm(mid_b, wu) + bu
    cdf, pdf = phi_both(pre)
    act = (pre * cdf).astype(BF)
    r2 = middle + mm_rt(act, wd_) + bd
    n2, inv2 = norm(r2)
    y = n2 * eg + es

    d_r2 = norm_back(dy, eg, n2, inv2)
    df = d_r2.astype(BF)
    d_pre = (mm(df, wd_) * (cdf + pre * pdf)).astype(BF)
    g_down = mm_lt(df, act)
    g_up = mm_lt(mid_b, d_pre)
    d_mid = d_r2 + mm_rt(d_pre, wu)
    d_r1 = norm_back(d_mid, mg, n1, inv1)
    da = d_r1.astype(BF)
    g_out = mm_lt(da, o2)
    d_o = mm(da, wo).astype(BF).reshape(my_rows, heads, head)
    dp = jnp.einsum("qhd,khd->hqk", d_o, v, preferred_element_type=F32)
    ds = (p * (dp - jnp.sum(p * dp, axis=-1, keepdims=True))).astype(BF)
    d_q = (jnp.einsum("hqk,khd->qhd", ds, k, preferred_element_type=F32) * 0.125).astype(BF)
    d_k = jnp.einsum("hqk,qhd->khd", ds, q, preferred_element_type=F32) * 0.125
    d_v = jnp.einsum("hqk,qhd->khd", pb, d_o, preferred_element_type=F32)
    d_q = d_q.reshape(my_rows, heads * head)
    d_kv = jnp.concatenate([d_k.reshape(half_rows, -1), d_v.reshape(half_rows, -1)], axis=1).astype(BF)
    pairs = [[h * parts + j for j in range(parts)] for h in range(tp_n // parts)]
    d_kv = lax.psum_scatter(d_kv.astype(F32), "tp", scatter_dimension=0, tiled=True, axis_index_groups=pairs)
    d_k, d_v = jnp.split(d_kv.astype(BF), 2, axis=1)
    g_q = mm_lt(x_mine, d_q)
    g_k = mm_lt(x_mine, d_k)
    g_v = mm_lt(x_mine, d_v)
    d_x = (d_r1 + mm_rt(d_q, wq) + mm_rt(d_k, wk) + mm_rt(d_v, wv)).astype(BF)

    layer_out = scatter_group(mm(pick, y.astype(BF)).astype(BF), own_rows)
    input_grad = scatter_group(mm(pick_nat, d_x).astype(BF), own_rows)

    outs = []
    for g, wd in zip((g_q, g_k, g_v, g_out, g_up, g_down), widths):
        outs.append(g.astype(BF).reshape(rows_n, width // rows_n, tp_n, wd).transpose(0, 2, 1, 3))
    packed_g = jnp.concatenate(outs, axis=3)
    packed_g = packed_g.reshape(rows_n * tp_n, width // rows_n, -1)
    mine_g = lax.psum_scatter(packed_g, ALL, scatter_dimension=0, tiled=True)[0].astype(F32)
    gm, at = [], 0
    for wd in widths:
        gm.append(mine_g[:, at:at + wd])
        at += wd

    def total(a):
        return jnp.sum(a.astype(F32), axis=0)

    def split_bias(a, wd):
        return a.reshape(tp_n, heads_l, rows_n, wd).transpose(2, 0, 1, 3).reshape(rows_n * tp_n, heads_l, wd)

    small_b = jnp.concatenate([
        split_bias(total(d_q), head_l), split_bias(total(d_v), head_l), split_bias(total(d_pre), b_up.shape[1])],
        axis=2).reshape(rows_n * tp_n, -1)
    vec_g = jnp.stack([total(d_r1), total(d_mid * n1), total(d_mid), total(d_r2), total(dy * n2), total(dy)])
    small_v = vec_g.reshape(6, rows_n, 1, width // rows_n).transpose(1, 2, 0, 3)
    small_v = jnp.broadcast_to(small_v, (rows_n, tp_n, 6, width // rows_n)).reshape(rows_n * tp_n, -1)
    small = jnp.concatenate([small_b, small_v], axis=1)
    small = lax.psum_scatter(small, ALL, scatter_dimension=0, tiled=True)[0]
    nb = small_b.shape[1]
    sb = small[:nb].reshape(heads_l, -1)
    sv = small[nb:].reshape(6, -1)
    return (layer_out, input_grad, gm[0], sb[:, :head_l], gm[1], gm[2], sb[:, head_l:2 * head_l], gm[3],
            sv[0], sv[1], sv[2], gm[4], sb[:, 2 * head_l:], gm[5], sv[3], sv[4], sv[5])


def specs():
    tok = P(None, ALL, None)
    grp = P(None, "fsdp", None)
    mat = P(ROWS, "tp")
    bias = P("tp", ROWS)
    vec = P(ROWS)
    ins = (tok, tok, grp, grp, mat, bias, mat, mat, bias, mat, vec, vec, vec, mat, bias, mat, vec, vec, vec)
    return ins, (tok, tok) + ins[4:]


CHUNK = 32
VMEM_MAX = 62 * 1024 * 1024


def row_facts(meta, group_n):
    c, t = lax.axis_index("ctx"), lax.axis_index("tp")
    lens = meta[4:5, :].astype(F32)
    lane = lax.broadcasted_iota(jnp.int32, lens.shape, 1)

    def one(k):
        return jnp.sum(jnp.where(lane == 3 * c + k, lens, 0.0), axis=1, keepdims=True).astype(jnp.int32)

    l0, l1 = one(0), one(1)
    half = group_n // 2
    first = jnp.where(l0 == half, 0, jnp.where(l1 == half, l0, l0 + l1))
    return first + (t % 2) * half, l0, l0 + l1


def wrap(v, group_n):
    return jnp.where(v >= group_n, v - group_n, v)


def pick_row(block, c):
    row = lax.broadcasted_iota(jnp.int32, block.shape, 0)
    return jnp.sum(jnp.where(row == c, block.astype(F32), 0.0), axis=0, keepdims=True).astype(jnp.int32)


def chunks(total, fn, size=CHUNK):
    def step(i, _):
        fn(pl.ds(pl.multiple_of(i * size, size), size))
        return 0
    lax.fori_loop(0, total // size, step, 0)


def each_t(fn):
    def step(t, _):
        fn(t)
        return 0
    lax.fori_loop(0, 4, step, 0)


def main_in_kernel(head, tok, cot, pack, meta, ga, gg, meta_all, dq_out, dkv_out, xm_out, da_out, op_out, dr1_out, y_out, vec_out,
                   gu, group, held, xh, dy, qkv, probs, sbuf, pb, pb2, acc, midb, n1, inv1, gelu_d, act, n2, df, big, bias,
                   g_u, g_d, sem_l, s_e, r_e, s_xg, r_xg, s_xf, s_m, r_m, *pass_sems):
    f, c, t_me = lax.axis_index("fsdp"), lax.axis_index("ctx"), lax.axis_index("tp")
    width = xh.shape[1]
    s_n, r_n = xh.shape[0], dy.shape[0]
    n_n = 2 * s_n
    wl = (gu.shape[2]) // 2
    hw = width // 4
    per_t = hw // head
    partner = (1 - f, c, t_me)
    slot = f * 4 + c
    cx = c + 1 - 2 * (c % 2)
    cy = (c + 2) % 4
    cd = (cx + 2) % 4
    x_nb, y_nb = (f, cx, t_me), (f, cy, t_me)
    near, far = 1 + f, 3 * f
    is_near = t_me == near
    receiver = (t_me // 2) == f

    barrier = pltpu.get_barrier_semaphore()
    peers = [partner] + [(f, (c + i) % 4, t_me) for i in (1, 2, 3)] + [(f, c, (t_me + i) % 4) for i in (1, 2, 3)]
    for p in peers:
        pl.semaphore_signal(barrier, inc=1, device_id=p, device_id_type=MESH)
    pl.semaphore_wait(barrier, len(peers))

    pending = []

    def send(src, dst, ssem, rsem, dev, pred=None):
        d = pltpu.make_async_remote_copy(src_ref=src, dst_ref=dst, send_sem=ssem, recv_sem=rsem,
                                         device_id=dev, device_id_type=MESH)
        if pred is None:
            d.start()
        else:
            pl.when(pred)(d.start)
        pending.append((pred, d))

    def arrived(dst, rsem, pred=None):
        d = pltpu.make_async_remote_copy(src_ref=dst, dst_ref=dst, send_sem=s_e.at[0, 0], recv_sem=rsem,
                                         device_id=partner, device_id_type=MESH)
        if pred is None:
            d.wait_recv()
        else:
            pl.when(pred)(d.wait_recv)

    def first_sends(ten, ref):
        for i in (1, 2, 3):
            to = (c + i) % 4
            send(ref.at[to], held.at[ten, c], s_e.at[ten, i], r_e.at[ten, c], (f, to, t_me))

    a_rows = ga.shape[2]
    w_rows = gu.shape[2]
    own_a, own_w = pack.at[pl.ds(0, a_rows)], pack.at[pl.ds(a_rows, w_rows)]
    first_sends(0, tok)
    local = [pltpu.make_async_copy(tok.at[c], held.at[0, c], sem_l.at[0]),
             pltpu.make_async_copy(cot.at[c], held.at[1, c], sem_l.at[1]),
             pltpu.make_async_copy(own_a, ga.at[t_me, slot], sem_l.at[2]),
             pltpu.make_async_copy(own_w, gu.at[t_me, slot], sem_l.at[3]),
             pltpu.make_async_copy(meta, meta_all.at[f], sem_l.at[8])]
    for d in local:
        d.start()
    send(meta, meta_all.at[f], s_m.at[0], r_m.at[0], partner)

    columns = [(t_me, None)]
    for d in (1, 2, 3):
        columns.append(((t_me - d + 4) % 4, t_me - d >= 0))
        columns.append(((t_me + d) % 4, t_me + d <= 3))

    def make_gather(gath, own, cut, sems):
        (s_z, r_z, s_x0, r_x0, s_y0, r_y0, s_y1, r_y1, s_x1, r_x1, s_c, r_c, s_c0, r_c0, s_c1, r_c1) = sems
        rows = gath.shape[2]
        h0, h1 = pl.ds(0, cut), pl.ds(cut, rows - cut)

        def have_column(src, tt, pred=None):
            send(src.at[h0], gath.at[tt, slot, h0], s_x0.at[tt], r_x0.at[tt], x_nb, pred)
            send(src.at[h1], gath.at[tt, slot, h1], s_y1.at[tt], r_y1.at[tt], y_nb, pred)
            send(src.at[h0], gath.at[tt, slot, h0], s_y0.at[0, tt], r_y0.at[0, tt], y_nb, pred)
            send(src.at[h1], gath.at[tt, slot, h1], s_x1.at[0, tt], r_x1.at[0, tt], x_nb, pred)
            send(src, gath.at[tt, slot], s_c.at[tt], r_c.at[tt], partner, pred)

        def begin():
            send(own, gath.at[t_me, slot], s_z.at[0, t_me], r_z.at[t_me], (f, c, (t_me + 1) % 4), t_me < 3)
            send(own, gath.at[t_me, slot], s_z.at[1, t_me], r_z.at[t_me], (f, c, (t_me + 3) % 4), t_me > 0)
            have_column(own, t_me)

        def z_step(d):
            for sign in (-1, 1):
                tt = t_me + sign * d
                there = tt >= 0 if sign < 0 else tt <= 3
                tt = (tt + 4) % 4
                arrived(gath.at[tt, slot], r_z.at[tt], there)
                on = t_me < 3 if sign < 0 else t_me > 0
                nxt = (t_me + 1) % 4 if sign < 0 else (t_me + 3) % 4
                if d < 3:
                    send(gath.at[tt, slot], gath.at[tt, slot], s_z.at[0 if sign < 0 else 1, tt], r_z.at[tt],
                         (f, c, nxt), jnp.logical_and(there, on))
                have_column(gath.at[tt, slot], tt, there)

        def mid_step(i):
            tt, pred = columns[i]
            a = gath.at[tt, f * 4 + cx, h0]
            arrived(a, r_x0.at[tt], pred)
            send(a, a, s_y0.at[1, tt], r_y0.at[1, tt], y_nb, pred)
            send(a, a, s_c0.at[0, tt], r_c0.at[0, tt], partner, pred)
            b = gath.at[tt, f * 4 + cy, h1]
            arrived(b, r_y1.at[tt], pred)
            send(b, b, s_x1.at[1, tt], r_x1.at[1, tt], x_nb, pred)
            send(b, b, s_c1.at[0, tt], r_c1.at[0, tt], partner, pred)

        def late_step(step, i):
            tt, pred = columns[i]
            a = gath.at[tt, f * 4 + (cy if step == 0 else cd), h0]
            arrived(a, r_y0.at[step, tt], pred)
            send(a, a, s_c0.at[1 + step, tt], r_c0.at[1 + step, tt], partner, pred)
            b = gath.at[tt, f * 4 + (cx if step == 0 else cd), h1]
            arrived(b, r_x1.at[step, tt], pred)
            send(b, b, s_c1.at[1 + step, tt], r_c1.at[1 + step, tt], partner, pred)

        def finish():
            other = (1 - f) * 4
            for tt in range(4):
                arrived(gath.at[tt, other + c], r_c.at[tt])
                for j, cc in enumerate((cx, cy, cd)):
                    arrived(gath.at[tt, other + cc, h0], r_c0.at[j, tt])
                for j, cc in enumerate((cy, cx, cd)):
                    arrived(gath.at[tt, other + cc, h1], r_c1.at[j, tt])
        return begin, z_step, mid_step, late_step, finish

    half_sems = len(pass_sems) // 2
    a_begin, a_z, a_mid, a_late, a_finish = make_gather(ga, own_a, (a_rows // 32) * 16, pass_sems[:half_sems])
    w_begin, w_z, w_mid, w_late, w_finish = make_gather(gu, own_w, w_rows // 2, pass_sems[half_sems:])

    def second_sends(ten):
        local[ten].wait()
        for i in (1, 2, 3):
            frm = (c + i) % 4
            arrived(held.at[ten, frm], r_e.at[ten, frm])
        blk = held.at[ten]
        dst = group.at[ten, :, t_me]
        to = jnp.where(is_near, far, near)
        send(blk, dst, s_xg.at[ten, t_me], r_xg.at[ten, t_me], (f, c, to))
        send(blk, dst, s_xf.at[ten, t_me], r_xg.at[ten, t_me], partner, receiver)
        keep = pltpu.make_async_copy(blk, dst, sem_l.at[4 + ten])
        pl.when(receiver)(keep.start)
        return keep

    def relay(ten):
        for i in (1, 2, 3):
            tt = (t_me + i) % 4
            arrived(group.at[ten, :, tt], r_xg.at[ten, tt], receiver)
            send(group.at[ten, :, tt], group.at[ten, :, tt], s_xg.at[ten, tt], r_xg.at[ten, tt], (f, c, far),
                 jnp.logical_and(is_near, tt != far))
            send(group.at[ten, :, tt], group.at[ten, :, tt], s_xf.at[ten, tt], r_xg.at[ten, tt], partner, receiver)

    def rows_here(ten, keep):
        for tt in range(4):
            arrived(group.at[ten, :, tt], r_xg.at[ten, tt], jnp.logical_not(receiver))
        pl.when(receiver)(keep.wait)

    def mat_of(ref, t, at):
        return ref[t, :, at:at + wl, :].reshape(ref.shape[1] * wl, width)

    a_begin()
    keep0 = second_sends(0)
    a_z(1)
    relay(0)
    a_z(2)
    a_z(3)
    for i in range(7):
        a_mid(i)
    first_sends(1, cot)
    w_begin()
    for step in (0, 1):
        for i in range(7):
            a_late(step, i)
    w_z(1)
    keep1 = second_sends(1)
    rows_here(0, keep0)
    arrived(meta_all.at[1 - f], r_m.at[0])
    local[4].wait()

    meta = meta_all[t_me // 2]
    start, e0, e1 = row_facts(meta, n_n)
    order = pick_row(meta[0:4, :], c)
    mine = pl.ds(pl.multiple_of(f * r_n, r_n), r_n)

    def half_rows(rows):
        nat = wrap(start + rows.start + lax.broadcasted_iota(jnp.int32, (rows.size, 1), 0), n_n)
        sel = (lax.broadcasted_iota(jnp.int32, (rows.size, n_n), 1) == nat).astype(F32).astype(BF)
        xh[rows, :] = mm(sel, group[0].reshape(n_n, width)).astype(BF)
    chunks(s_n, half_rows, 128)
    a_finish()
    local[2].wait()
    for t in range(4):
        bias[t] = jnp.sum(ga[t, :, wl:wl + 16, :].astype(F32), axis=0)
    vec = bias[0]
    bo, mg, ms, bd, eg, es = (vec[i:i + 1, :] for i in range(6))
    nat_row = wrap(start + lax.broadcasted_iota(jnp.int32, (1, s_n), 1), n_n)
    seg_row = (nat_row >= e0).astype(jnp.int32) + (nat_row >= e1).astype(jnp.int32)
    nat_q = wrap(start + f * r_n + lax.broadcasted_iota(jnp.int32, (r_n, 1), 0), n_n)
    same = ((nat_q >= e0).astype(jnp.int32) + (nat_q >= e1).astype(jnp.int32)) == seg_row

    def forward_t(t):
        row6 = bias[t][6:7, :]
        qkv[t] = (mm(xh[...], mat_of(ga, t, 0)) + row6).astype(BF)
        q3 = qkv[t, mine, :]
        kv = qkv[t]
        outs = []
        for h in range(per_t):
            lo = hw + h * head
            sbuf[...] = mm_rt(q3[:, lo:lo + head], kv[:, lo + hw:lo + hw + head])
            at = t * per_t + h

            s = jnp.where(same, sbuf[...] * 0.125, MASKED)
            p = jnp.exp(s - jnp.max(s, axis=1, keepdims=True))
            p = p * (1.0 / jnp.sum(p, axis=1, keepdims=True))
            probs[at] = p
            pb[...] = p.astype(BF)
            outs.append(mm(pb[...], kv[:, lo + 2 * hw:lo + 2 * hw + head]).astype(BF))
        outs.append(jnp.zeros((r_n, width - hw), BF))
        op_out[t] = jnp.concatenate(outs, axis=1)

    def two(first, fn):
        def step(t, _):
            fn(t)
            return 0
        lax.fori_loop(first, first + 2, step, 0)

    w_z(2)
    relay(1)
    two(0, forward_t)
    w_z(3)
    w_mid(0)
    w_mid(1)
    w_mid(2)
    two(2, forward_t)
    for i in range(3, 7):
        w_mid(i)
    xm_out[...] = xh[mine, :]
    acc[...] = xm_out[...].astype(F32) + bo

    def out_t(t):
        acc[...] += mm_rt(op_out[t], mat_of(ga, t, 0))
    each_t(out_t)
    w_late(0, 0)
    w_late(0, 1)
    w_late(0, 2)

    def norm_rows(u):
        centre = u - jnp.mean(u, axis=-1, keepdims=True)
        inv = lax.rsqrt(jnp.mean(centre * centre, axis=-1, keepdims=True) + EPS)
        return centre * inv, inv

    def first_norm(rows):
        n, inv = norm_rows(acc[rows, :])
        n1[rows, :] = n
        inv1[rows, :] = jnp.broadcast_to(inv, (rows.size, 128))
        m = n * mg + ms
        midb[rows, :] = m.astype(BF)
        acc[rows, :] = m + bd
    chunks(r_n, first_norm)
    rows_here(1, keep1)

    def quarter_rows(rows):
        nat = wrap(start + f * r_n + rows.start + lax.broadcasted_iota(jnp.int32, (rows.size, 1), 0), n_n)
        sel = (order == nat).astype(F32).astype(BF)
        dy[rows, :] = mm(sel, group[1].reshape(n_n, width))
    chunks(r_n, quarter_rows, 128)
    for i in range(3, 7):
        w_late(0, i)
    for i in range(7):
        w_late(1, i)
    w_finish()
    local[3].wait()

    def ffn_t(t):
        row7 = bias[t][7:8, :]
        big[...] = mm(midb[...], mat_of(gu, t, 0))

        def gelu(rows):
            u = big[rows, :] + row7
            cdf = 0.5 * (1.0 + lax.erf(u * 0.7071067811865476))
            pdf = 0.3989422804014327 * jnp.exp(-0.5 * u * u)
            act[t, rows, :] = (u * cdf).astype(BF)
            gelu_d[t, rows, :] = cdf + u * pdf
        chunks(r_n, gelu, 16)
        acc[...] += mm_rt(act[t], mat_of(gu, t, wl))
    each_t(ffn_t)

    vec_out[...] = jnp.zeros_like(vec_out)

    def add_vec(i, v):
        vec_out[i] += jnp.sum(v.reshape(-1, 8, v.shape[1]), axis=0)

    def second_norm(rows):
        n, inv = norm_rows(acc[rows, :])
        y_out[rows, :] = (n * eg + es).astype(BF)
        g = dy[rows, :]
        e = g * eg
        d = (e - jnp.mean(e, axis=-1, keepdims=True) - n * jnp.mean(e * n, axis=-1, keepdims=True)) * inv
        add_vec(3, d)
        add_vec(4, g * n)
        add_vec(5, g)
        df[rows, :] = d.astype(BF)
        acc[rows, :] = d
    chunks(r_n, second_norm)

    def ffn_back_t(t):
        big[...] = mm(df[...], mat_of(gu, t, wl))

        def times(rows):
            d = (big[rows, :] * gelu_d[t, rows, :]).astype(BF)
            n2[rows, :] = d
            add_vec(8 + t, d.astype(F32))
        chunks(r_n, times)
        acc[...] += mm_rt(n2[...], mat_of(gu, t, 0))
        g_d[t] = mm_lt(df[...], act[t]).astype(BF).reshape(g_d.shape[1:])
        g_u[t] = mm_lt(midb[...], n2[...]).astype(BF).reshape(g_u.shape[1:])
    each_t(ffn_back_t)
    stores = [pltpu.make_async_copy(g_u, gg.at[:, :, pl.ds(0, wl)], sem_l.at[6]),
              pltpu.make_async_copy(g_d, gg.at[:, :, pl.ds(wl, wl)], sem_l.at[7])]
    for d in stores:
        d.start()

    def first_norm_back(rows):
        g, n = acc[rows, :], n1[rows, :]
        e = g * mg
        d = (e - jnp.mean(e, axis=-1, keepdims=True) - n * jnp.mean(e * n, axis=-1, keepdims=True)) * inv1[rows, :][:, 0:1]
        add_vec(0, d)
        add_vec(1, g * n)
        add_vec(2, g)
        dr1_out[rows, :] = d
        da_out[rows, :] = d.astype(BF)
    chunks(r_n, first_norm_back)

    def attn_back_t(t):
        do = mm(da_out[...], mat_of(ga, t, 0)).astype(BF)
        q3 = qkv[t, mine, :]
        kv = qkv[t]
        dqs, dks, dvs = [], [], []
        for h in range(per_t):
            lo = hw + h * head
            at = t * per_t + h
            do_h = do[:, h * head:(h + 1) * head]
            sbuf[...] = mm_rt(do_h, kv[:, lo + 2 * hw:lo + 2 * hw + head])

            p, d = probs[at], sbuf[...]
            pb[...] = (p * (d - jnp.sum(p * d, axis=1, keepdims=True))).astype(BF)
            pb2[...] = p.astype(BF)
            dvs.append(mm_lt(pb2[...], do_h))
            dqs.append(mm(pb[...], kv[:, lo + hw:lo + hw + head]) * 0.125)
            dks.append(mm_lt(pb[...], q3[:, lo:lo + head]) * 0.125)
        dq_out[t] = jnp.concatenate([a.astype(BF) for a in dqs], axis=1)
        dkv_out[t] = jnp.concatenate([a.astype(BF) for a in dks + dvs], axis=1)
    each_t(attn_back_t)
    for d in stores:
        d.wait()


    for pred, d in pending:
        if pred is None:
            d.wait_send()
        else:
            pl.when(pred)(d.wait_send)


def main_in(tok, cot, pack, meta, head):
    own, width = tok.shape[1:]
    wl = (pack.shape[0] - 16) // 3
    n_n = own * 16
    s_n, r_n = n_n // 2, n_n // 4
    hw = width // 4
    heads = width // head
    v = pltpu.VMEM
    dma = pltpu.SemaphoreType.DMA
    sds = jax.ShapeDtypeStruct
    vm = pl.BlockSpec(memory_space=pltpu.VMEM)
    any_ = pl.BlockSpec(memory_space=pl.ANY)
    wshape = (4, 8, wl, width)
    pass_sems = [dma((2, 4)), dma((4,)), dma((4,)), dma((4,)), dma((2, 4)), dma((2, 4)), dma((4,)), dma((4,)),
                 dma((2, 4)), dma((2, 4)), dma((4,)), dma((4,)), dma((3, 4)), dma((3, 4)), dma((3, 4)), dma((3, 4))]
    return pl.pallas_call(
        functools.partial(main_in_kernel, head),
        out_shape=(sds((4, 8, wl + 16, width), BF), sds((4, 8, 2 * wl, width), BF), sds((2,) + meta.shape, jnp.int32),
                   sds((4, r_n, hw), BF), sds((4, s_n, 2 * hw), BF), sds((r_n, width), BF), sds((r_n, width), BF),
                   sds((4, r_n, width), BF), sds((r_n, width), F32), sds((r_n, width), BF), sds((16, 8, width), F32)),
        in_specs=[any_, any_, vm, vm],
        out_specs=(vm, any_) + (vm,) * 9,
        scratch_shapes=[
            v((4, 8, 2 * wl, width), BF), v((2, 4, 4, own, width), BF), v((2, 4, own, width), BF),
            v((s_n, width), BF), v((r_n, width), F32), v((4, s_n, width), BF), v((heads, r_n, s_n), F32),
            v((r_n, s_n), F32), v((r_n, s_n), BF), v((r_n, s_n), BF), v((r_n, width), F32), v((r_n, width), BF),
            v((r_n, width), F32), v((r_n, 128), F32), v((4, r_n, width), F32), v((4, r_n, width), BF),
            v((r_n, width), BF), v((r_n, width), BF), v((r_n, width), F32), v((4, 16, width), F32),
            v(wshape, BF), v(wshape, BF),
            dma((9,)), dma((2, 4)), dma((2, 4)), dma((2, 4)), dma((2, 4)), dma((2, 4)), dma((1,)), dma((1,))]
        + pass_sems + pass_sems,
        compiler_params=pltpu.CompilerParams(collective_id=0, has_side_effects=True, vmem_limit_bytes=VMEM_MAX),
        name="main_in",
    )(tok, cot, pack, meta)


def tail_out_kernel(w_a, meta_ref, dq, dkv, xm, da, op, dr1, y, vec, gg, tot_a, tot_w, rows_out,
                    g_a, acc, dqkv, dkv_in, place, pl1, pl2, own, w0, w1, w2, w3, a0, a1, a2, a3,
                    sem_l, s_d, r_d, s_u, r_u, s_o, r_o,
                    ws0, wr0, ws1, wr1, ws2, wr2, ws3, wr3, as0, ar0, as1, ar1, as2, ar2, as3, ar3):
    f, c, t = lax.axis_index("fsdp"), lax.axis_index("ctx"), lax.axis_index("tp")
    r_n, width = xm.shape
    n_n = 4 * r_n
    hw = width // 4
    wl = w_a.shape[2] - 16
    partner = (1 - f, c, t)
    cx = c + 1 - 2 * (c % 2)
    cy = (c + 2) % 4
    cd = (cx + 2) % 4
    x_nb, y_nb = (f, cx, t), (f, cy, t)
    par = t % 2
    z_nb = (f, c, t + 1 - 2 * par)
    to_f, to_t = t // 2, 2 * f + par
    stays = to_f == f

    turn = [(t + 2) % 4, (t + 1) % 4, (t + 3) % 4, t]
    loads = []
    for i, tt in enumerate(turn):
        d = pltpu.make_async_copy(gg.at[tt, pl.ds(pl.multiple_of(f * 4, 4), 4)], own.at[tt], sem_l.at[1 + i])
        d.start()
        loads.append(d)

    barrier = pltpu.get_barrier_semaphore()
    peers = [partner] + [(f, (c + i) % 4, t) for i in (1, 2, 3)] + [(f, c, (t + i) % 4) for i in (1, 2, 3)]
    for p in peers:
        pl.semaphore_signal(barrier, inc=1, device_id=p, device_id_type=MESH)

    @pl.when(jnp.logical_not(stays))
    def _():
        for i in range(4):
            pl.semaphore_signal(barrier, inc=1, device_id=(to_f, (c + i) % 4, to_t), device_id_type=MESH)
        pl.semaphore_wait(barrier, len(peers) + 4)

    @pl.when(stays)
    def _():
        pl.semaphore_wait(barrier, len(peers))

    pending = []

    def send(src, dst, ssem, rsem, dev, pred=None):
        d = pltpu.make_async_remote_copy(src_ref=src, dst_ref=dst, send_sem=ssem, recv_sem=rsem,
                                         device_id=dev, device_id_type=MESH)
        if pred is None:
            d.start()
        else:
            pl.when(pred)(d.start)
        pending.append((pred, d))

    def arrived(dst, rsem):
        pltpu.make_async_remote_copy(src_ref=dst, dst_ref=dst, send_sem=s_d, recv_sem=rsem,
                                     device_id=partner, device_id_type=MESH).wait_recv()

    def add_into(dst, src, off, n):
        def go(i, _):
            r = pl.ds(pl.multiple_of(off + i * 16, 16), 16)
            dst[r, :] = dst[r, :] + src[r, :]
            return 0
        lax.fori_loop(0, n // 16, go, 0)

    def make_pass(mine, theirs, g0, g1, g2, g3, cut, sems):
        q0, p0, q1, p1, q2, p2, q3, p3 = sems
        rows = g0.shape[2]
        h0, h1 = pl.ds(0, cut), pl.ds(cut, rows - cut)

        def roles(i):
            return (cy, cx, y_nb, x_nb) if i % 2 == 0 else (cx, cy, x_nb, y_nb)

        def stage0(i):
            tt = turn[i]
            for k in (1, 2, 3, 0):
                cc = (c + k) % 4
                send(theirs(tt, cc), g0.at[tt, cc], q0.at[tt, cc], p0.at[tt, cc], partner)

        def stage1(i):
            tt = turn[i]
            ca, cb, a_nb, b_nb = roles(i)
            for k in (1, 2, 3, 0):
                cc = (c + k) % 4
                arrived(g0.at[tt, cc], p0.at[tt, cc])
                add_into(mine(tt, cc), g0.at[tt, cc], 0, rows)
            for k, cc in enumerate((ca, cd)):
                send(mine(tt, cc).at[h0], g1.at[tt, k, h0], q1.at[0, k, tt], p1.at[0, k, tt], a_nb)
            for k, cc in enumerate((cb, cd)):
                send(mine(tt, cc).at[h1], g1.at[tt, k, h1], q1.at[1, k, tt], p1.at[1, k, tt], b_nb)

        def stage2(i):
            tt = turn[i]
            ca, cb, a_nb, b_nb = roles(i)
            arrived(g1.at[tt, 1, h0], p1.at[0, 1, tt])
            add_into(mine(tt, cb), g1.at[tt, 1], 0, cut)
            arrived(g1.at[tt, 1, h1], p1.at[1, 1, tt])
            add_into(mine(tt, ca), g1.at[tt, 1], cut, rows - cut)
            send(mine(tt, cb).at[h0], g2.at[tt, h0], q2.at[0, tt], p2.at[0, tt], b_nb)
            send(mine(tt, ca).at[h1], g2.at[tt, h1], q2.at[1, tt], p2.at[1, tt], a_nb)
            arrived(g1.at[tt, 0, h0], p1.at[0, 0, tt])
            add_into(mine(tt, c), g1.at[tt, 0], 0, cut)
            arrived(g1.at[tt, 0, h1], p1.at[1, 0, tt])
            add_into(mine(tt, c), g1.at[tt, 0], cut, rows - cut)

        def stage3(i):
            tt = turn[i]
            arrived(g2.at[tt, h0], p2.at[0, tt])
            arrived(g2.at[tt, h1], p2.at[1, tt])
            add_into(mine(tt, c), g2.at[tt], 0, rows)
            if i < 3:
                send(mine(tt, c), g3.at[t], q3.at[tt], p3.at[t], (f, c, tt))

        def finish(total, ls):
            keep = pltpu.make_async_copy(mine(t, c), g3.at[t], ls)
            keep.start()
            keep.wait()
            for tt in turn[:3]:
                arrived(g3.at[tt], p3.at[tt])

            def go(i, _):
                r = pl.ds(pl.multiple_of(i * 16, 16), 16)
                a, b, e, g = (g3[k, r, :].astype(F32) for k in range(4))
                total[r, :] = ((a + b) + e) + g
                return 0
            lax.fori_loop(0, rows // 16, go, 0)
        return stage0, stage1, stage2, stage3, finish

    wp = make_pass(lambda tt, cc: own.at[tt, cc], lambda tt, cc: gg.at[tt, 4 * (1 - f) + cc],
                   w0, w1, w2, w3, own.shape[2] // 2, (ws0, wr0, ws1, wr1, ws2, wr2, ws3, wr3))
    a_rows = g_a.shape[2]
    ap = make_pass(lambda tt, cc: g_a.at[tt, 4 * f + cc], lambda tt, cc: g_a.at[tt, 4 * (1 - f) + cc],
                   a0, a1, a2, a3, (a_rows // 32) * 16, (as0, ar0, as1, ar1, as2, ar2, as3, ar3))

    lo = pl.multiple_of(2 * f, 2)
    hi = pl.multiple_of(2 - 2 * f, 2)
    block = place.shape[3]
    moves = [pltpu.make_async_copy(pl2.at[ten, c], rows_out.at[ten, c], sem_l.at[5 + ten]) for ten in range(2)]

    def rows1(ten):
        send(place.at[ten, pl.ds(hi, 2)], pl1.at[ten], s_u.at[0, ten], r_u.at[0, ten], partner)

    def rows2(ten):
        arrived(pl1.at[ten], r_u.at[0, ten])
        for k in (0, 1):
            for j in range(4):
                add_into(pl1.at[ten, k, j], place.at[ten, lo + k, j], 0, block)
        send(pl1.at[ten, 1 - par], pl2.at[ten], s_u.at[1, ten], r_u.at[1, ten], z_nb)

    def rows3(ten):
        arrived(pl2.at[ten], r_u.at[1, ten])
        for j in range(4):
            add_into(pl2.at[ten, j], pl1.at[ten, par, j], 0, block)
        for i in range(4):
            cc = (c + i) % 4
            away = jnp.logical_not(stays) if i == 0 else None
            send(pl2.at[ten, cc], rows_out.at[ten, c], s_o.at[ten, i], r_o.at[ten, c], (to_f, cc, to_t), away)
        pl.when(stays)(moves[ten].start)

    meta = meta_ref[t // 2]
    start, _, _ = row_facts(meta, n_n)
    nat = wrap(start + f * r_n + lax.broadcasted_iota(jnp.int32, (r_n, 1), 0), n_n)
    mine_rows = pl.ds(pl.multiple_of(f * r_n, r_n), r_n)
    lane16 = lax.broadcasted_iota(jnp.int32, (16, width), 0)

    def grads_t(k):
        both = (dkv[k, mine_rows, :].astype(F32) + dkv_in[k].astype(F32)).astype(BF)
        dqkv[...] = jnp.concatenate([jnp.zeros((r_n, hw), BF), dq[k], both], axis=1)
        d = dqkv[...]
        acc[...] += mm_rt(d, w_a[k, :, 0:wl, :].reshape(w_a.shape[1] * wl, width))
        g_a[k, :, 0:wl, :] = (mm_lt(xm[...], d) + mm_lt(da[...], op[k])).astype(BF).reshape(g_a.shape[1], wl, width)
        sums = jnp.sum(vec[...], axis=1)
        base = jnp.where(lane16 < 6, sums, 0.0)
        base = base + jnp.where(lane16 == 6, jnp.sum(d.astype(F32), axis=0, keepdims=True), 0.0)
        base = base + jnp.where(lane16 == 7, jnp.sum(vec[8 + k], axis=0, keepdims=True), 0.0)
        g_a[k, :, wl:wl + 16, :] = jnp.broadcast_to(base.astype(BF)[None], (g_a.shape[1], 16, width))

    def two(first):
        def step(k, _):
            grads_t(k)
            return 0
        lax.fori_loop(first, first + 2, step, 0)

    n_d = dkv_in.shape[1]
    send(dkv.at[:, pl.ds(pl.multiple_of((1 - f) * n_d, n_d), n_d)], dkv_in, s_d, r_d, partner)
    wp[0](0)
    wp[0](1)
    order = pick_row(meta[8:12, :], c)
    pick = (order == nat).astype(F32).astype(BF)
    place[0] = mm_lt(pick, y[...]).astype(BF).reshape(place.shape[1:])
    acc[...] = dr1[...]
    wp[0](2)
    rows1(0)
    wp[0](3)
    loads[0].wait()
    wp[1](0)
    loads[1].wait()
    wp[1](1)
    arrived(dkv_in, r_d)
    two(0)
    rows2(0)
    wp[2](0)
    loads[2].wait()
    wp[1](2)
    two(2)
    wp[2](1)
    wp[3](0)
    loads[3].wait()
    wp[1](3)
    rows3(0)
    for i in range(4):
        ap[0](i)
    lane = lax.broadcasted_iota(jnp.int32, (1, n_n), 1)
    at = ((lane // block) % 4) * (4 * block) + (lane // (4 * block)) * block + lane % block
    pick2 = (at == nat).astype(F32).astype(BF)
    place[1] = mm_lt(pick2, acc[...].astype(BF)).astype(BF).reshape(place.shape[1:])
    wp[2](2)
    wp[3](1)
    rows1(1)
    ap[1](0)
    wp[2](3)
    wp[3](2)
    rows2(1)
    ap[1](1)
    ap[2](0)
    wp[3](3)
    rows3(1)
    ap[1](2)
    ap[2](1)
    ap[3](0)
    ap[1](3)
    wp[4](tot_w, sem_l.at[7])
    ap[2](2)
    ap[3](1)
    ap[2](3)
    ap[3](2)
    ap[3](3)
    ap[4](tot_a, sem_l.at[8])

    for ten in range(2):
        for i in range(4):
            cc = (c + i) % 4
            if i == 0:
                @pl.when(jnp.logical_not(stays))
                def _(ten=ten, cc=cc):
                    arrived(rows_out.at[ten, cc], r_o.at[ten, cc])
                pl.when(stays)(moves[ten].wait)
            else:
                arrived(rows_out.at[ten, cc], r_o.at[ten, cc])
    for pred, d in pending:
        if pred is None:
            d.wait_send()
        else:
            pl.when(pred)(d.wait_send)


def tail_out(gath, meta, dq, dkv, xm, da, op, dr1, y, vec, gg):
    n_t, n_fc, rows, width = gath.shape
    wl = rows - 16
    r_n = xm.shape[0]
    block = r_n // 4
    v = pltpu.VMEM
    dma = pltpu.SemaphoreType.DMA
    vm = pl.BlockSpec(memory_space=pltpu.VMEM)
    any_ = pl.BlockSpec(memory_space=pl.ANY)
    ra, rw = wl + 16, 2 * wl
    def bufs(n):
        return [v((4, 4, n, width), BF), v((4, 2, n, width), BF), v((4, n, width), BF), v((4, n, width), BF)]
    pass_sems = [dma((4, 4)), dma((4, 4)), dma((2, 2, 4)), dma((2, 2, 4)), dma((2, 4)), dma((2, 4)), dma((4,)), dma((4,))]
    return pl.pallas_call(
        tail_out_kernel,
        out_shape=(jax.ShapeDtypeStruct((ra, width), F32), jax.ShapeDtypeStruct((rw, width), F32),
                   jax.ShapeDtypeStruct((2, 4, block, width), BF)),
        in_specs=[vm] * 10 + [any_],
        out_specs=(vm, vm, vm),
        scratch_shapes=[v((n_t, n_fc, ra, width), BF), v((r_n, width), F32),
                        v((r_n, width), BF), v((n_t, r_n, dkv.shape[2]), BF), v((2, 4, 4, block, width), BF),
                        v((2, 2, 4, block, width), BF), v((2, 4, block, width), BF), v((4, 4, rw, width), BF)]
        + bufs(rw) + bufs(ra)
        + [dma((9,)), dma, dma, dma((2, 2)), dma((2, 2)), dma((2, 4)), dma((2, 4))] + pass_sems + pass_sems,
        compiler_params=pltpu.CompilerParams(collective_id=2, has_side_effects=True, vmem_limit_bytes=VMEM_MAX),
        name="tail_out",
    )(gath, meta, dq, dkv, xm, da, op, dr1, y, vec, gg)


def quad_body(tokens_in, cotangent, seq_lengths, row_order, w_query, b_query, w_key, w_value, b_value,
              w_out, b_out, mid_gain, mid_shift, w_up, b_up, w_down, b_down, end_gain, end_shift):
    f, c = lax.axis_index("fsdp"), lax.axis_index("ctx")
    fc = f * 4 + c
    own, width = tokens_in.shape[1:]
    wl = w_query.shape[0]
    heads_l, head_l = b_query.shape
    head = head_l * 8
    up_l = b_up.shape[1]
    hw = width // 4
    mat_a = jnp.concatenate([w_out, w_query, w_key, w_value], axis=1)

    vecs = jnp.stack([b_out, mid_gain, mid_shift, b_down, end_gain, end_shift])
    col = lax.broadcasted_iota(jnp.int32, (1, width), 1)
    row_v = jnp.where(col // wl == fc, jnp.tile(vecs, (1, 8)), 0)
    part = (col % head) // head_l == fc
    three = jnp.stack([jnp.zeros_like(b_query), b_query, jnp.zeros_like(b_query), b_value])
    row_a = jnp.where(part, jnp.tile(three, (1, 1, 8)).reshape(1, width), 0)
    row_u = jnp.where((col % (8 * up_l)) // up_l == fc, jnp.tile(b_up, (1, 8)).reshape(1, width), 0)
    small = jnp.concatenate([row_v, row_a, row_u, jnp.zeros((8, width), BF)], axis=0)
    pack = jnp.concatenate([mat_a, small, w_up, w_down], axis=0)

    order = row_order[:, 0]
    n_n = order.shape[1]
    moved = order.reshape(4, 4, 4, own).transpose(0, 2, 1, 3).reshape(4, n_n)
    lens = jnp.pad(seq_lengths[:, 0].reshape(1, -1), ((0, 3), (0, n_n - 12)))
    meta_own = jnp.concatenate([order, lens, moved, jnp.zeros((4, n_n), jnp.int32)], axis=0)

    ga, gg, meta, dq, dkv, xm, da, op, dr1, y, vec = main_in(tokens_in, cotangent, pack, meta_own, head)
    tot_a, tot_w, rows = tail_out(ga, meta, dq, dkv, xm, da, op, dr1, y, vec, gg)

    g_a, g_up, g_down = tot_a[:wl], tot_w[:wl], tot_w[wl:]
    sv = lax.dynamic_slice(tot_a[wl:wl + 6], (0, fc * wl), (6, wl))
    ba = tot_a[wl + 6].reshape(4, heads_l, head)
    gb = lax.dynamic_slice(ba, (0, 0, fc * head_l), (4, heads_l, head_l))
    gu = lax.dynamic_slice(tot_a[wl + 7].reshape(heads_l, -1), (0, fc * up_l), (heads_l, up_l))
    return (rows[0], rows[1], g_a[:, hw:2 * hw], gb[1], g_a[:, 2 * hw:3 * hw], g_a[:, 3 * hw:], gb[3], g_a[:, :hw],
            sv[0], sv[1], sv[2], g_up, gu, g_down, sv[3], sv[4], sv[5])


def solution(mesh):
    ins, outs = specs()
    small_mesh = (mesh.shape["fsdp"], mesh.shape["ctx"], mesh.shape["tp"]) == (2, 4, 4)
    fn = quad_body if small_mesh else body
    return jax.shard_map(fn, mesh=mesh, in_specs=ins, out_specs=outs, check_vma=False)
```

```python
import functools

import jax
import jax.numpy as jnp
from jax import lax
from jax.experimental import pallas as pl
from jax.experimental.pallas import tpu as pltpu
from jax.sharding import PartitionSpec as P

EPS = 1e-06
MASKED = -1e30
ALL = ("fsdp", "ctx", "tp")
ROWS = ("fsdp", "ctx")
BF = jnp.bfloat16
F32 = jnp.float32


MESH = pl.DeviceIdType.MESH
def mm(a, b):
    return jnp.dot(a, b, preferred_element_type=F32)


def mm_rt(a, b):
    return lax.dot_general(a, b, (((1,), (1,)), ((), ())), preferred_element_type=F32)


def mm_lt(a, b):
    return lax.dot_general(a, b, (((0,), (0,)), ((), ())), preferred_element_type=F32)


def norm(u):
    centre = u - jnp.mean(u, axis=-1, keepdims=True)
    inv = lax.rsqrt(jnp.mean(centre * centre, axis=-1, keepdims=True) + EPS)
    return centre * inv, inv


def norm_back(d, gain, n, inv):
    e = d * gain
    return (e - jnp.mean(e, axis=-1, keepdims=True) - n * jnp.mean(e * n, axis=-1, keepdims=True)) * inv


def phi_both(u):
    cdf = 0.5 * (1.0 + lax.erf(u * 0.7071067811865476))
    pdf = 0.3989422804014327 * jnp.exp(-0.5 * u * u)
    return cdf, pdf


def gather_group(block):
    width = block.shape[-1]
    mine = lax.all_to_all(block, "ctx", 0, 0, tiled=True)
    whole = lax.all_gather(mine, "tp", axis=1, tiled=False)
    return whole.reshape(-1, width)


def scatter_group(rows, own_rows):
    ctx_n, tp_n = lax.axis_size("ctx"), lax.axis_size("tp")
    width = rows.shape[-1]
    blocks = rows.reshape(ctx_n, tp_n * own_rows, width)
    mine = lax.psum_scatter(blocks, "tp", scatter_dimension=1, tiled=True)
    return lax.all_to_all(mine, "ctx", 0, 0, tiled=True)


def body(tokens_in, cotangent, seq_lengths, row_order, w_query, b_query, w_key, w_value, b_value,
         w_out, b_out, mid_gain, mid_shift, w_up, b_up, w_down, b_down, end_gain, end_shift):
    ctx_n, tp_n, fsdp_n = lax.axis_size("ctx"), lax.axis_size("tp"), lax.axis_size("fsdp")
    rows_n = ctx_n * fsdp_n
    c, t = lax.axis_index("ctx"), lax.axis_index("tp")
    micro, own_rows, width = tokens_in.shape
    group_rows = own_rows * ctx_n * tp_n
    half_rows = group_rows // 2
    parts = tp_n // 2
    my_rows = half_rows // parts
    half, quarter = t // parts, t % parts
    heads_l, head_l = b_query.shape
    heads, head = heads_l * tp_n, head_l * rows_n

    mats = (w_query, w_key, w_value, w_out, w_up, w_down)
    widths = [m.shape[1] for m in mats]
    packed = lax.all_gather(jnp.concatenate(mats, axis=1), ALL, axis=0, tiled=False)
    full, at = [], 0
    for wd in widths:
        piece = packed[:, :, at:at + wd].reshape(rows_n, tp_n, -1, wd)
        full.append(piece.transpose(0, 2, 1, 3).reshape(width, tp_n * wd))
        at += wd
    wq, wk, wv, wo, wu, wd_ = full
    vecs = (b_out, mid_gain, mid_shift, b_down, end_gain, end_shift)
    bias = (b_query, b_value, b_up)
    vec_all = lax.all_gather(jnp.stack(vecs), ROWS, axis=1, tiled=True).astype(F32)
    bias_all = lax.all_gather(jnp.concatenate(bias, axis=1), ALL, axis=0, tiled=False).astype(F32)

    def whole_bias(at, wd):
        piece = bias_all[:, :, at:at + wd].reshape(rows_n, tp_n, heads_l, wd)
        return piece.transpose(1, 2, 0, 3).reshape(-1)

    bq = whole_bias(0, head_l)
    bv = whole_bias(head_l, head_l)
    bu = whole_bias(2 * head_l, b_up.shape[1])
    bo, mg, ms, bd, eg, es = (vec_all[i] for i in range(6))

    lens = lax.dynamic_index_in_dim(seq_lengths[:, 0], c, 0, keepdims=False)
    order = lax.dynamic_index_in_dim(row_order[:, 0], c, 0, keepdims=False)
    places = lax.iota(jnp.int32, lens.shape[0])
    longest = jnp.argmax(lens)
    first = jnp.sum(jnp.where(places < longest, lens, 0))
    start = lax.rem(first + half * half_rows, group_rows)
    ends = jnp.cumsum(lens)
    nat = lax.rem(start + lax.iota(jnp.int32, half_rows), group_rows)
    seg = jnp.sum((ends[None, :] <= nat[:, None]).astype(jnp.int32), axis=1)
    q_at = quarter * my_rows
    nat_q = lax.dynamic_slice_in_dim(nat, q_at, my_rows)
    seg_q = lax.dynamic_slice_in_dim(seg, q_at, my_rows)

    x_group = gather_group(tokens_in)
    c_group = gather_group(cotangent)
    x_twice = jnp.concatenate([x_group, x_group[:half_rows]], axis=0)
    x_half = lax.dynamic_slice_in_dim(x_twice, start, half_rows, 0)
    x_mine = lax.dynamic_slice_in_dim(x_half, q_at, my_rows, 0)
    pick = (order[:, None] == nat_q[None, :]).astype(BF)
    pick_nat = (lax.iota(jnp.int32, group_rows)[:, None] == nat_q[None, :]).astype(BF)
    dy = mm_lt(pick, c_group)

    x = x_mine.astype(F32)
    q = (mm(x_mine, wq) + bq).astype(BF).reshape(my_rows, heads, head)
    k = mm(x_half, wk).astype(BF).reshape(half_rows, heads, head)
    v = (mm(x_half, wv) + bv).astype(BF).reshape(half_rows, heads, head)
    same = seg_q[:, None] == seg[None, :]
    s = jnp.einsum("qhd,khd->hqk", q, k, preferred_element_type=F32) * 0.125
    s = jnp.where(same[None], s, MASKED)
    p = jnp.exp(s - jnp.max(s, axis=-1, keepdims=True))
    p = p / jnp.sum(p, axis=-1, keepdims=True)
    pb = p.astype(BF)
    o = jnp.einsum("hqk,khd->qhd", pb, v, preferred_element_type=F32).astype(BF)
    o2 = o.reshape(my_rows, heads * head)
    r1 = x + mm_rt(o2, wo) + bo
    n1, inv1 = norm(r1)
    middle = n1 * mg + ms
    mid_b = middle.astype(BF)
    pre = mm(mid_b, wu) + bu
    cdf, pdf = phi_both(pre)
    act = (pre * cdf).astype(BF)
    r2 = middle + mm_rt(act, wd_) + bd
    n2, inv2 = norm(r2)
    y = n2 * eg + es

    d_r2 = norm_back(dy, eg, n2, inv2)
    df = d_r2.astype(BF)
    d_pre = (mm(df, wd_) * (cdf + pre * pdf)).astype(BF)
    g_down = mm_lt(df, act)
    g_up = mm_lt(mid_b, d_pre)
    d_mid = d_r2 + mm_rt(d_pre, wu)
    d_r1 = norm_back(d_mid, mg, n1, inv1)
    da = d_r1.astype(BF)
    g_out = mm_lt(da, o2)
    d_o = mm(da, wo).astype(BF).reshape(my_rows, heads, head)
    dp = jnp.einsum("qhd,khd->hqk", d_o, v, preferred_element_type=F32)
    ds = (p * (dp - jnp.sum(p * dp, axis=-1, keepdims=True))).astype(BF)
    d_q = (jnp.einsum("hqk,khd->qhd", ds, k, preferred_element_type=F32) * 0.125).astype(BF)
    d_k = jnp.einsum("hqk,qhd->khd", ds, q, preferred_element_type=F32) * 0.125
    d_v = jnp.einsum("hqk,qhd->khd", pb, d_o, preferred_element_type=F32)
    d_q = d_q.reshape(my_rows, heads * head)
    d_kv = jnp.concatenate([d_k.reshape(half_rows, -1), d_v.reshape(half_rows, -1)], axis=1).astype(BF)
    pairs = [[h * parts + j for j in range(parts)] for h in range(tp_n // parts)]
    d_kv = lax.psum_scatter(d_kv.astype(F32), "tp", scatter_dimension=0, tiled=True, axis_index_groups=pairs)
    d_k, d_v = jnp.split(d_kv.astype(BF), 2, axis=1)
    g_q = mm_lt(x_mine, d_q)
    g_k = mm_lt(x_mine, d_k)
    g_v = mm_lt(x_mine, d_v)
    d_x = (d_r1 + mm_rt(d_q, wq) + mm_rt(d_k, wk) + mm_rt(d_v, wv)).astype(BF)

    layer_out = scatter_group(mm(pick, y.astype(BF)).astype(BF), own_rows)
    input_grad = scatter_group(mm(pick_nat, d_x).astype(BF), own_rows)

    outs = []
    for g, wd in zip((g_q, g_k, g_v, g_out, g_up, g_down), widths):
        outs.append(g.astype(BF).reshape(rows_n, width // rows_n, tp_n, wd).transpose(0, 2, 1, 3))
    packed_g = jnp.concatenate(outs, axis=3)
    packed_g = packed_g.reshape(rows_n * tp_n, width // rows_n, -1)
    mine_g = lax.psum_scatter(packed_g, ALL, scatter_dimension=0, tiled=True)[0].astype(F32)
    gm, at = [], 0
    for wd in widths:
        gm.append(mine_g[:, at:at + wd])
        at += wd

    def total(a):
        return jnp.sum(a.astype(F32), axis=0)

    def split_bias(a, wd):
        return a.reshape(tp_n, heads_l, rows_n, wd).transpose(2, 0, 1, 3).reshape(rows_n * tp_n, heads_l, wd)

    small_b = jnp.concatenate([
        split_bias(total(d_q), head_l), split_bias(total(d_v), head_l), split_bias(total(d_pre), b_up.shape[1])],
        axis=2).reshape(rows_n * tp_n, -1)
    vec_g = jnp.stack([total(d_r1), total(d_mid * n1), total(d_mid), total(d_r2), total(dy * n2), total(dy)])
    small_v = vec_g.reshape(6, rows_n, 1, width // rows_n).transpose(1, 2, 0, 3)
    small_v = jnp.broadcast_to(small_v, (rows_n, tp_n, 6, width // rows_n)).reshape(rows_n * tp_n, -1)
    small = jnp.concatenate([small_b, small_v], axis=1)
    small = lax.psum_scatter(small, ALL, scatter_dimension=0, tiled=True)[0]
    nb = small_b.shape[1]
    sb = small[:nb].reshape(heads_l, -1)
    sv = small[nb:].reshape(6, -1)
    return (layer_out, input_grad, gm[0], sb[:, :head_l], gm[1], gm[2], sb[:, head_l:2 * head_l], gm[3],
            sv[0], sv[1], sv[2], gm[4], sb[:, 2 * head_l:], gm[5], sv[3], sv[4], sv[5])


def specs():
    tok = P(None, ALL, None)
    grp = P(None, "fsdp", None)
    mat = P(ROWS, "tp")
    bias = P("tp", ROWS)
    vec = P(ROWS)
    ins = (tok, tok, grp, grp, mat, bias, mat, mat, bias, mat, vec, vec, vec, mat, bias, mat, vec, vec, vec)
    return ins, (tok, tok) + ins[4:]


CHUNK = 32
VMEM_MAX = 62 * 1024 * 1024


def row_facts(meta, group_n):
    c, t = lax.axis_index("ctx"), lax.axis_index("tp")
    lens = meta[4:5, :].astype(F32)
    lane = lax.broadcasted_iota(jnp.int32, lens.shape, 1)

    def one(k):
        return jnp.sum(jnp.where(lane == 3 * c + k, lens, 0.0), axis=1, keepdims=True).astype(jnp.int32)

    l0, l1 = one(0), one(1)
    half = group_n // 2
    first = jnp.where(l0 == half, 0, jnp.where(l1 == half, l0, l0 + l1))
    return first + (t % 2) * half, l0, l0 + l1


def wrap(v, group_n):
    return jnp.where(v >= group_n, v - group_n, v)


def pick_row(block, c):
    row = lax.broadcasted_iota(jnp.int32, block.shape, 0)
    return jnp.sum(jnp.where(row == c, block.astype(F32), 0.0), axis=0, keepdims=True).astype(jnp.int32)


def chunks(total, fn, size=CHUNK):
    def step(i, _):
        fn(pl.ds(pl.multiple_of(i * size, size), size))
        return 0
    lax.fori_loop(0, total // size, step, 0)


def each_t(fn):
    def step(t, _):
        fn(t)
        return 0
    lax.fori_loop(0, 4, step, 0)


def main_in_kernel(head, tok, cot, pack, meta, up, down, ga, gg, meta_all, dq_out, dkv_out, xm_out, da_out, op_out, dr1_out, y_out, vec_out,
                   gu, group, held, xh, dy, qkv, probs, sbuf, pb, pb2, acc, midb, n1, inv1, gelu_d, act, n2, df, big, bias,
                   g_u, g_d, sem_l, s_e, r_e, s_xg, r_xg, s_xf, s_m, r_m, *pass_sems):
    f, c, t_me = lax.axis_index("fsdp"), lax.axis_index("ctx"), lax.axis_index("tp")
    width = xh.shape[1]
    s_n, r_n = xh.shape[0], dy.shape[0]
    n_n = 2 * s_n
    wl = (gu.shape[2]) // 2
    hw = width // 4
    per_t = hw // head
    partner = (1 - f, c, t_me)
    slot = f * 4 + c
    cx = c + 1 - 2 * (c % 2)
    cy = (c + 2) % 4
    cd = (cx + 2) % 4
    x_nb, y_nb = (f, cx, t_me), (f, cy, t_me)
    near, far = 1 + f, 3 * f
    is_near = t_me == near
    receiver = (t_me // 2) == f

    barrier = pltpu.get_barrier_semaphore()
    peers = [partner] + [(f, (c + i) % 4, t_me) for i in (1, 2, 3)] + [(f, c, (t_me + i) % 4) for i in (1, 2, 3)]
    for p in peers:
        pl.semaphore_signal(barrier, inc=1, device_id=p, device_id_type=MESH)
    pl.semaphore_wait(barrier, len(peers))

    pending = []

    def send(src, dst, ssem, rsem, dev, pred=None):
        d = pltpu.make_async_remote_copy(src_ref=src, dst_ref=dst, send_sem=ssem, recv_sem=rsem,
                                         device_id=dev, device_id_type=MESH)
        if pred is None:
            d.start()
        else:
            pl.when(pred)(d.start)
        pending.append((pred, d))

    def arrived(dst, rsem, pred=None):
        d = pltpu.make_async_remote_copy(src_ref=dst, dst_ref=dst, send_sem=s_e.at[0, 0], recv_sem=rsem,
                                         device_id=partner, device_id_type=MESH)
        if pred is None:
            d.wait_recv()
        else:
            pl.when(pred)(d.wait_recv)

    def first_sends(ten, ref):
        for i in (1, 2, 3):
            to = (c + i) % 4
            send(ref.at[to], held.at[ten, c], s_e.at[ten, i], r_e.at[ten, c], (f, to, t_me))

    a_rows = ga.shape[2]
    w_rows = gu.shape[2]
    own_a, own_w = pack, gu.at[t_me, slot]
    shards = [pltpu.make_async_copy(up, gu.at[t_me, slot, pl.ds(0, wl)], sem_l.at[3]),
              pltpu.make_async_copy(down, gu.at[t_me, slot, pl.ds(wl, wl)], sem_l.at[9])]
    first_sends(0, tok)
    local = [pltpu.make_async_copy(tok.at[c], held.at[0, c], sem_l.at[0]),
             pltpu.make_async_copy(cot.at[c], held.at[1, c], sem_l.at[1]),
             pltpu.make_async_copy(own_a, ga.at[t_me, slot], sem_l.at[2]),
             pltpu.make_async_copy(meta, meta_all.at[f], sem_l.at[8])]
    for d in local + shards:
        d.start()
    send(meta, meta_all.at[f], s_m.at[0], r_m.at[0], partner)

    columns = [(t_me, None)]
    for d in (1, 2, 3):
        columns.append(((t_me - d + 4) % 4, t_me - d >= 0))
        columns.append(((t_me + d) % 4, t_me + d <= 3))

    def make_gather(gath, own, cut, sems):
        (s_z, r_z, s_x0, r_x0, s_y0, r_y0, s_y1, r_y1, s_x1, r_x1, s_c, r_c, s_c0, r_c0, s_c1, r_c1) = sems
        rows = gath.shape[2]
        h0, h1 = pl.ds(0, cut), pl.ds(cut, rows - cut)

        def have_column(src, tt, pred=None):
            send(src.at[h0], gath.at[tt, slot, h0], s_x0.at[tt], r_x0.at[tt], x_nb, pred)
            send(src.at[h1], gath.at[tt, slot, h1], s_y1.at[tt], r_y1.at[tt], y_nb, pred)
            send(src.at[h0], gath.at[tt, slot, h0], s_y0.at[0, tt], r_y0.at[0, tt], y_nb, pred)
            send(src.at[h1], gath.at[tt, slot, h1], s_x1.at[0, tt], r_x1.at[0, tt], x_nb, pred)
            send(src, gath.at[tt, slot], s_c.at[tt], r_c.at[tt], partner, pred)

        def begin():
            send(own, gath.at[t_me, slot], s_z.at[0, t_me], r_z.at[t_me], (f, c, (t_me + 1) % 4), t_me < 3)
            send(own, gath.at[t_me, slot], s_z.at[1, t_me], r_z.at[t_me], (f, c, (t_me + 3) % 4), t_me > 0)
            have_column(own, t_me)

        def z_step(d):
            for sign in (-1, 1):
                tt = t_me + sign * d
                there = tt >= 0 if sign < 0 else tt <= 3
                tt = (tt + 4) % 4
                arrived(gath.at[tt, slot], r_z.at[tt], there)
                on = t_me < 3 if sign < 0 else t_me > 0
                nxt = (t_me + 1) % 4 if sign < 0 else (t_me + 3) % 4
                if d < 3:
                    send(gath.at[tt, slot], gath.at[tt, slot], s_z.at[0 if sign < 0 else 1, tt], r_z.at[tt],
                         (f, c, nxt), jnp.logical_and(there, on))
                have_column(gath.at[tt, slot], tt, there)

        def mid_step(i):
            tt, pred = columns[i]
            a = gath.at[tt, f * 4 + cx, h0]
            arrived(a, r_x0.at[tt], pred)
            send(a, a, s_y0.at[1, tt], r_y0.at[1, tt], y_nb, pred)
            send(a, a, s_c0.at[0, tt], r_c0.at[0, tt], partner, pred)
            b = gath.at[tt, f * 4 + cy, h1]
            arrived(b, r_y1.at[tt], pred)
            send(b, b, s_x1.at[1, tt], r_x1.at[1, tt], x_nb, pred)
            send(b, b, s_c1.at[0, tt], r_c1.at[0, tt], partner, pred)

        def late_step(step, i):
            tt, pred = columns[i]
            a = gath.at[tt, f * 4 + (cy if step == 0 else cd), h0]
            arrived(a, r_y0.at[step, tt], pred)
            send(a, a, s_c0.at[1 + step, tt], r_c0.at[1 + step, tt], partner, pred)
            b = gath.at[tt, f * 4 + (cx if step == 0 else cd), h1]
            arrived(b, r_x1.at[step, tt], pred)
            send(b, b, s_c1.at[1 + step, tt], r_c1.at[1 + step, tt], partner, pred)

        def finish():
            other = (1 - f) * 4
            for tt in range(4):
                arrived(gath.at[tt, other + c], r_c.at[tt])
                for j, cc in enumerate((cx, cy, cd)):
                    arrived(gath.at[tt, other + cc, h0], r_c0.at[j, tt])
                for j, cc in enumerate((cy, cx, cd)):
                    arrived(gath.at[tt, other + cc, h1], r_c1.at[j, tt])
        return begin, z_step, mid_step, late_step, finish

    half_sems = len(pass_sems) // 2
    a_begin, a_z, a_mid, a_late, a_finish = make_gather(ga, own_a, (a_rows // 32) * 16, pass_sems[:half_sems])
    w_begin, w_z, w_mid, w_late, w_finish = make_gather(gu, own_w, w_rows // 2, pass_sems[half_sems:])

    def second_sends(ten):
        local[ten].wait()
        for i in (1, 2, 3):
            frm = (c + i) % 4
            arrived(held.at[ten, frm], r_e.at[ten, frm])
        blk = held.at[ten]
        dst = group.at[ten, :, t_me]
        to = jnp.where(is_near, far, near)
        send(blk, dst, s_xg.at[ten, t_me], r_xg.at[ten, t_me], (f, c, to))
        send(blk, dst, s_xf.at[ten, t_me], r_xg.at[ten, t_me], partner, receiver)
        keep = pltpu.make_async_copy(blk, dst, sem_l.at[4 + ten])
        pl.when(receiver)(keep.start)
        return keep

    def relay(ten):
        for i in (1, 2, 3):
            tt = (t_me + i) % 4
            arrived(group.at[ten, :, tt], r_xg.at[ten, tt], receiver)
            send(group.at[ten, :, tt], group.at[ten, :, tt], s_xg.at[ten, tt], r_xg.at[ten, tt], (f, c, far),
                 jnp.logical_and(is_near, tt != far))
            send(group.at[ten, :, tt], group.at[ten, :, tt], s_xf.at[ten, tt], r_xg.at[ten, tt], partner, receiver)

    def rows_here(ten, keep):
        for tt in range(4):
            arrived(group.at[ten, :, tt], r_xg.at[ten, tt], jnp.logical_not(receiver))
        pl.when(receiver)(keep.wait)

    def mat_of(ref, t, at):
        return ref[t, :, at:at + wl, :].reshape(ref.shape[1] * wl, width)

    a_begin()
    keep0 = second_sends(0)
    a_z(1)
    for d in shards:
        d.wait()
    w_begin()
    relay(0)
    a_z(2)
    first_sends(1, cot)
    a_z(3)
    for i in range(5):
        a_mid(i)
    w_z(1)
    for i in range(5, 7):
        a_mid(i)
    for i in range(7):
        a_late(0, i)
    w_z(2)
    for i in range(7):
        a_late(1, i)
    keep1 = second_sends(1)
    rows_here(0, keep0)
    arrived(meta_all.at[1 - f], r_m.at[0])
    local[3].wait()

    meta = meta_all[t_me // 2]
    start, e0, e1 = row_facts(meta, n_n)
    order = pick_row(meta[0:4, :], c)
    mine = pl.ds(pl.multiple_of(f * r_n, r_n), r_n)

    def half_rows(rows):
        nat = wrap(start + rows.start + lax.broadcasted_iota(jnp.int32, (rows.size, 1), 0), n_n)
        sel = (lax.broadcasted_iota(jnp.int32, (rows.size, n_n), 1) == nat).astype(F32).astype(BF)
        xh[rows, :] = mm(sel, group[0].reshape(n_n, width)).astype(BF)
    chunks(s_n, half_rows, 128)
    a_finish()
    local[2].wait()
    for t in range(4):
        bias[t] = jnp.sum(ga[t, :, wl:wl + 16, :].astype(F32), axis=0)
    vec = bias[0]
    bo, mg, ms, bd, eg, es = (vec[i:i + 1, :] for i in range(6))
    nat_row = wrap(start + lax.broadcasted_iota(jnp.int32, (1, s_n), 1), n_n)
    seg_row = (nat_row >= e0).astype(jnp.int32) + (nat_row >= e1).astype(jnp.int32)
    nat_q = wrap(start + f * r_n + lax.broadcasted_iota(jnp.int32, (r_n, 1), 0), n_n)
    same = ((nat_q >= e0).astype(jnp.int32) + (nat_q >= e1).astype(jnp.int32)) == seg_row

    def forward_t(t):
        row6 = bias[t][6:7, :]
        qkv[t] = (mm(xh[...], mat_of(ga, t, 0)) + row6).astype(BF)
        q3 = qkv[t, mine, :]
        kv = qkv[t]
        outs = []
        for h in range(per_t):
            lo = hw + h * head
            sbuf[...] = mm_rt(q3[:, lo:lo + head], kv[:, lo + hw:lo + hw + head])
            at = t * per_t + h

            s = jnp.where(same, sbuf[...] * 0.125, MASKED)
            p = jnp.exp(s - jnp.max(s, axis=1, keepdims=True))
            p = p * (1.0 / jnp.sum(p, axis=1, keepdims=True))
            probs[at] = p
            pb[...] = p.astype(BF)
            outs.append(mm(pb[...], kv[:, lo + 2 * hw:lo + 2 * hw + head]).astype(BF))
        outs.append(jnp.zeros((r_n, width - hw), BF))
        op_out[t] = jnp.concatenate(outs, axis=1)

    def two(first, fn):
        def step(t, _):
            fn(t)
            return 0
        lax.fori_loop(first, first + 2, step, 0)

    relay(1)
    two(0, forward_t)
    w_z(3)
    w_mid(0)
    w_mid(1)
    w_mid(2)
    two(2, forward_t)
    for i in range(3, 7):
        w_mid(i)
    xm_out[...] = xh[mine, :]
    acc[...] = xm_out[...].astype(F32) + bo

    def out_t(t):
        acc[...] += mm_rt(op_out[t], mat_of(ga, t, 0))
    each_t(out_t)
    w_late(0, 0)
    w_late(0, 1)
    w_late(0, 2)

    def norm_rows(u):
        centre = u - jnp.mean(u, axis=-1, keepdims=True)
        inv = lax.rsqrt(jnp.mean(centre * centre, axis=-1, keepdims=True) + EPS)
        return centre * inv, inv

    def first_norm(rows):
        n, inv = norm_rows(acc[rows, :])
        n1[rows, :] = n
        inv1[rows, :] = jnp.broadcast_to(inv, (rows.size, 128))
        m = n * mg + ms
        midb[rows, :] = m.astype(BF)
        acc[rows, :] = m + bd
    chunks(r_n, first_norm)
    rows_here(1, keep1)

    def quarter_rows(rows):
        nat = wrap(start + f * r_n + rows.start + lax.broadcasted_iota(jnp.int32, (rows.size, 1), 0), n_n)
        sel = (order == nat).astype(F32).astype(BF)
        dy[rows, :] = mm(sel, group[1].reshape(n_n, width))
    chunks(r_n, quarter_rows, 128)
    for i in range(3, 7):
        w_late(0, i)
    for i in range(7):
        w_late(1, i)
    w_finish()

    def ffn_t(t):
        row7 = bias[t][7:8, :]
        big[...] = mm(midb[...], mat_of(gu, t, 0))

        def gelu(rows):
            u = big[rows, :] + row7
            cdf = 0.5 * (1.0 + lax.erf(u * 0.7071067811865476))
            pdf = 0.3989422804014327 * jnp.exp(-0.5 * u * u)
            act[t, rows, :] = (u * cdf).astype(BF)
            gelu_d[t, rows, :] = cdf + u * pdf
        chunks(r_n, gelu, 16)
        acc[...] += mm_rt(act[t], mat_of(gu, t, wl))
    each_t(ffn_t)

    vec_out[...] = jnp.zeros_like(vec_out)

    def add_vec(i, v):
        vec_out[i] += jnp.sum(v.reshape(-1, 8, v.shape[1]), axis=0)

    def second_norm(rows):
        n, inv = norm_rows(acc[rows, :])
        y_out[rows, :] = (n * eg + es).astype(BF)
        g = dy[rows, :]
        e = g * eg
        d = (e - jnp.mean(e, axis=-1, keepdims=True) - n * jnp.mean(e * n, axis=-1, keepdims=True)) * inv
        add_vec(3, d)
        add_vec(4, g * n)
        add_vec(5, g)
        df[rows, :] = d.astype(BF)
        acc[rows, :] = d
    chunks(r_n, second_norm)

    def ffn_back_t(t):
        big[...] = mm(df[...], mat_of(gu, t, wl))

        def times(rows):
            d = (big[rows, :] * gelu_d[t, rows, :]).astype(BF)
            n2[rows, :] = d
            add_vec(8 + t, d.astype(F32))
        chunks(r_n, times)
        acc[...] += mm_rt(n2[...], mat_of(gu, t, 0))
        g_d[t] = mm_lt(df[...], act[t]).astype(BF).reshape(g_d.shape[1:])
        g_u[t] = mm_lt(midb[...], n2[...]).astype(BF).reshape(g_u.shape[1:])
    each_t(ffn_back_t)
    stores = [pltpu.make_async_copy(g_u, gg.at[:, :, pl.ds(0, wl)], sem_l.at[6]),
              pltpu.make_async_copy(g_d, gg.at[:, :, pl.ds(wl, wl)], sem_l.at[7])]
    for d in stores:
        d.start()

    def first_norm_back(rows):
        g, n = acc[rows, :], n1[rows, :]
        e = g * mg
        d = (e - jnp.mean(e, axis=-1, keepdims=True) - n * jnp.mean(e * n, axis=-1, keepdims=True)) * inv1[rows, :][:, 0:1]
        add_vec(0, d)
        add_vec(1, g * n)
        add_vec(2, g)
        dr1_out[rows, :] = d
        da_out[rows, :] = d.astype(BF)
    chunks(r_n, first_norm_back)

    def attn_back_t(t):
        do = mm(da_out[...], mat_of(ga, t, 0)).astype(BF)
        q3 = qkv[t, mine, :]
        kv = qkv[t]
        dqs, dks, dvs = [], [], []
        for h in range(per_t):
            lo = hw + h * head
            at = t * per_t + h
            do_h = do[:, h * head:(h + 1) * head]
            sbuf[...] = mm_rt(do_h, kv[:, lo + 2 * hw:lo + 2 * hw + head])

            p, d = probs[at], sbuf[...]
            pb[...] = (p * (d - jnp.sum(p * d, axis=1, keepdims=True))).astype(BF)
            pb2[...] = p.astype(BF)
            dvs.append(mm_lt(pb2[...], do_h))
            dqs.append(mm(pb[...], kv[:, lo + hw:lo + hw + head]) * 0.125)
            dks.append(mm_lt(pb[...], q3[:, lo:lo + head]) * 0.125)
        dq_out[t] = jnp.concatenate([a.astype(BF) for a in dqs], axis=1)
        dkv_out[t] = jnp.concatenate([a.astype(BF) for a in dks + dvs], axis=1)
    each_t(attn_back_t)
    for d in stores:
        d.wait()


    for pred, d in pending:
        if pred is None:
            d.wait_send()
        else:
            pl.when(pred)(d.wait_send)


def main_in(tok, cot, pack, meta, up, down, head):
    own, width = tok.shape[1:]
    wl = up.shape[0]
    n_n = own * 16
    s_n, r_n = n_n // 2, n_n // 4
    hw = width // 4
    heads = width // head
    v = pltpu.VMEM
    dma = pltpu.SemaphoreType.DMA
    sds = jax.ShapeDtypeStruct
    vm = pl.BlockSpec(memory_space=pltpu.VMEM)
    any_ = pl.BlockSpec(memory_space=pl.ANY)
    wshape = (4, 8, wl, width)
    pass_sems = [dma((2, 4)), dma((4,)), dma((4,)), dma((4,)), dma((2, 4)), dma((2, 4)), dma((4,)), dma((4,)),
                 dma((2, 4)), dma((2, 4)), dma((4,)), dma((4,)), dma((3, 4)), dma((3, 4)), dma((3, 4)), dma((3, 4))]
    return pl.pallas_call(
        functools.partial(main_in_kernel, head),
        out_shape=(sds((4, 8, wl + 16, width), BF), sds((4, 8, 2 * wl, width), BF), sds((2,) + meta.shape, jnp.int32),
                   sds((4, r_n, hw), BF), sds((4, s_n, 2 * hw), BF), sds((r_n, width), BF), sds((r_n, width), BF),
                   sds((4, r_n, width), BF), sds((r_n, width), F32), sds((r_n, width), BF), sds((16, 8, width), F32)),
        in_specs=[any_, any_, vm, vm, any_, any_],
        out_specs=(vm, any_) + (vm,) * 9,
        scratch_shapes=[
            v((4, 8, 2 * wl, width), BF), v((2, 4, 4, own, width), BF), v((2, 4, own, width), BF),
            v((s_n, width), BF), v((r_n, width), F32), v((4, s_n, width), BF), v((heads, r_n, s_n), F32),
            v((r_n, s_n), F32), v((r_n, s_n), BF), v((r_n, s_n), BF), v((r_n, width), F32), v((r_n, width), BF),
            v((r_n, width), F32), v((r_n, 128), F32), v((4, r_n, width), F32), v((4, r_n, width), BF),
            v((r_n, width), BF), v((r_n, width), BF), v((r_n, width), F32), v((4, 16, width), F32),
            v(wshape, BF), v(wshape, BF),
            dma((10,)), dma((2, 4)), dma((2, 4)), dma((2, 4)), dma((2, 4)), dma((2, 4)), dma((1,)), dma((1,))]
        + pass_sems + pass_sems,
        compiler_params=pltpu.CompilerParams(collective_id=0, has_side_effects=True, vmem_limit_bytes=VMEM_MAX),
        name="main_in",
    )(tok, cot, pack, meta, up, down)


def tail_out_kernel(w_a, meta_ref, dq, dkv, xm, da, op, dr1, y, vec, gg, tot_a, tot_w, rows_out,
                    g_a, acc, dqkv, dkv_in, place, pl1, pl2, own, w0, w1, w2, w3, a0, a1, a2, a3,
                    sem_l, s_d, r_d, s_u, r_u, s_o, r_o,
                    ws0, wr0, ws1, wr1, ws2, wr2, ws3, wr3, as0, ar0, as1, ar1, as2, ar2, as3, ar3):
    f, c, t = lax.axis_index("fsdp"), lax.axis_index("ctx"), lax.axis_index("tp")
    r_n, width = xm.shape
    n_n = 4 * r_n
    hw = width // 4
    wl = w_a.shape[2] - 16
    partner = (1 - f, c, t)
    cx = c + 1 - 2 * (c % 2)
    cy = (c + 2) % 4
    cd = (cx + 2) % 4
    x_nb, y_nb = (f, cx, t), (f, cy, t)
    par = t % 2
    z_nb = (f, c, t + 1 - 2 * par)
    to_f, to_t = t // 2, 2 * f + par
    stays = to_f == f

    turn = [(t + 2) % 4, (t + 1) % 4, (t + 3) % 4, t]
    loads = []
    for i, tt in enumerate(turn):
        d = pltpu.make_async_copy(gg.at[tt, pl.ds(pl.multiple_of(f * 4, 4), 4)], own.at[tt], sem_l.at[1 + i])
        d.start()
        loads.append(d)

    barrier = pltpu.get_barrier_semaphore()
    peers = [partner] + [(f, (c + i) % 4, t) for i in (1, 2, 3)] + [(f, c, (t + i) % 4) for i in (1, 2, 3)]
    for p in peers:
        pl.semaphore_signal(barrier, inc=1, device_id=p, device_id_type=MESH)

    @pl.when(jnp.logical_not(stays))
    def _():
        for i in range(4):
            pl.semaphore_signal(barrier, inc=1, device_id=(to_f, (c + i) % 4, to_t), device_id_type=MESH)
        pl.semaphore_wait(barrier, len(peers) + 4)

    @pl.when(stays)
    def _():
        pl.semaphore_wait(barrier, len(peers))

    pending = []

    def send(src, dst, ssem, rsem, dev, pred=None):
        d = pltpu.make_async_remote_copy(src_ref=src, dst_ref=dst, send_sem=ssem, recv_sem=rsem,
                                         device_id=dev, device_id_type=MESH)
        if pred is None:
            d.start()
        else:
            pl.when(pred)(d.start)
        pending.append((pred, d))

    def arrived(dst, rsem):
        pltpu.make_async_remote_copy(src_ref=dst, dst_ref=dst, send_sem=s_d, recv_sem=rsem,
                                     device_id=partner, device_id_type=MESH).wait_recv()

    def add_into(dst, src, off, n):
        def go(i, _):
            r = pl.ds(pl.multiple_of(off + i * 16, 16), 16)
            dst[r, :] = dst[r, :] + src[r, :]
            return 0
        lax.fori_loop(0, n // 16, go, 0)

    def make_pass(mine, theirs, g0, g1, g2, g3, cut, sems):
        q0, p0, q1, p1, q2, p2, q3, p3 = sems
        rows = g0.shape[2]
        h0, h1 = pl.ds(0, cut), pl.ds(cut, rows - cut)

        def roles(i):
            return (cy, cx, y_nb, x_nb) if i % 2 == 0 else (cx, cy, x_nb, y_nb)

        def stage0(i):
            tt = turn[i]
            for k in (1, 2, 3, 0):
                cc = (c + k) % 4
                send(theirs(tt, cc), g0.at[tt, cc], q0.at[tt, cc], p0.at[tt, cc], partner)

        def stage1(i):
            tt = turn[i]
            ca, cb, a_nb, b_nb = roles(i)
            for k in (1, 2, 3, 0):
                cc = (c + k) % 4
                arrived(g0.at[tt, cc], p0.at[tt, cc])
                add_into(mine(tt, cc), g0.at[tt, cc], 0, rows)
            for k, cc in enumerate((ca, cd)):
                send(mine(tt, cc).at[h0], g1.at[tt, k, h0], q1.at[0, k, tt], p1.at[0, k, tt], a_nb)
            for k, cc in enumerate((cb, cd)):
                send(mine(tt, cc).at[h1], g1.at[tt, k, h1], q1.at[1, k, tt], p1.at[1, k, tt], b_nb)

        def stage2(i):
            tt = turn[i]
            ca, cb, a_nb, b_nb = roles(i)
            arrived(g1.at[tt, 1, h0], p1.at[0, 1, tt])
            add_into(mine(tt, cb), g1.at[tt, 1], 0, cut)
            arrived(g1.at[tt, 1, h1], p1.at[1, 1, tt])
            add_into(mine(tt, ca), g1.at[tt, 1], cut, rows - cut)
            send(mine(tt, cb).at[h0], g2.at[tt, h0], q2.at[0, tt], p2.at[0, tt], b_nb)
            send(mine(tt, ca).at[h1], g2.at[tt, h1], q2.at[1, tt], p2.at[1, tt], a_nb)
            arrived(g1.at[tt, 0, h0], p1.at[0, 0, tt])
            add_into(mine(tt, c), g1.at[tt, 0], 0, cut)
            arrived(g1.at[tt, 0, h1], p1.at[1, 0, tt])
            add_into(mine(tt, c), g1.at[tt, 0], cut, rows - cut)

        def stage3(i):
            tt = turn[i]
            arrived(g2.at[tt, h0], p2.at[0, tt])
            arrived(g2.at[tt, h1], p2.at[1, tt])
            add_into(mine(tt, c), g2.at[tt], 0, rows)
            if i < 3:
                send(mine(tt, c), g3.at[t], q3.at[tt], p3.at[t], (f, c, tt))

        def finish(total, ls):
            keep = pltpu.make_async_copy(mine(t, c), g3.at[t], ls)
            keep.start()
            keep.wait()
            for tt in turn[:3]:
                arrived(g3.at[tt], p3.at[tt])

            def go(i, _):
                r = pl.ds(pl.multiple_of(i * 16, 16), 16)
                a, b, e, g = (g3[k, r, :].astype(F32) for k in range(4))
                total[r, :] = ((a + b) + e) + g
                return 0
            lax.fori_loop(0, rows // 16, go, 0)
        return stage0, stage1, stage2, stage3, finish

    wp = make_pass(lambda tt, cc: own.at[tt, cc], lambda tt, cc: gg.at[tt, 4 * (1 - f) + cc],
                   w0, w1, w2, w3, own.shape[2] // 2, (ws0, wr0, ws1, wr1, ws2, wr2, ws3, wr3))
    a_rows = g_a.shape[2]
    ap = make_pass(lambda tt, cc: g_a.at[tt, 4 * f + cc], lambda tt, cc: g_a.at[tt, 4 * (1 - f) + cc],
                   a0, a1, a2, a3, (a_rows // 32) * 16, (as0, ar0, as1, ar1, as2, ar2, as3, ar3))

    lo = pl.multiple_of(2 * f, 2)
    hi = pl.multiple_of(2 - 2 * f, 2)
    block = place.shape[3]
    moves = [pltpu.make_async_copy(pl2.at[ten, c], rows_out.at[ten, c], sem_l.at[5 + ten]) for ten in range(2)]

    def rows1(ten):
        send(place.at[ten, pl.ds(hi, 2)], pl1.at[ten], s_u.at[0, ten], r_u.at[0, ten], partner)

    def rows2(ten):
        arrived(pl1.at[ten], r_u.at[0, ten])
        for k in (0, 1):
            for j in range(4):
                add_into(pl1.at[ten, k, j], place.at[ten, lo + k, j], 0, block)
        send(pl1.at[ten, 1 - par], pl2.at[ten], s_u.at[1, ten], r_u.at[1, ten], z_nb)

    def rows3(ten):
        arrived(pl2.at[ten], r_u.at[1, ten])
        for j in range(4):
            add_into(pl2.at[ten, j], pl1.at[ten, par, j], 0, block)
        for i in range(4):
            cc = (c + i) % 4
            away = jnp.logical_not(stays) if i == 0 else None
            send(pl2.at[ten, cc], rows_out.at[ten, c], s_o.at[ten, i], r_o.at[ten, c], (to_f, cc, to_t), away)
        pl.when(stays)(moves[ten].start)

    meta = meta_ref[t // 2]
    start, _, _ = row_facts(meta, n_n)
    nat = wrap(start + f * r_n + lax.broadcasted_iota(jnp.int32, (r_n, 1), 0), n_n)
    mine_rows = pl.ds(pl.multiple_of(f * r_n, r_n), r_n)
    lane16 = lax.broadcasted_iota(jnp.int32, (16, width), 0)

    def grads_t(k):
        both = (dkv[k, mine_rows, :].astype(F32) + dkv_in[k].astype(F32)).astype(BF)
        dqkv[...] = jnp.concatenate([jnp.zeros((r_n, hw), BF), dq[k], both], axis=1)
        d = dqkv[...]
        acc[...] += mm_rt(d, w_a[k, :, 0:wl, :].reshape(w_a.shape[1] * wl, width))
        g_a[k, :, 0:wl, :] = (mm_lt(xm[...], d) + mm_lt(da[...], op[k])).astype(BF).reshape(g_a.shape[1], wl, width)
        sums = jnp.sum(vec[...], axis=1)
        base = jnp.where(lane16 < 6, sums, 0.0)
        base = base + jnp.where(lane16 == 6, jnp.sum(d.astype(F32), axis=0, keepdims=True), 0.0)
        base = base + jnp.where(lane16 == 7, jnp.sum(vec[8 + k], axis=0, keepdims=True), 0.0)
        g_a[k, :, wl:wl + 16, :] = jnp.broadcast_to(base.astype(BF)[None], (g_a.shape[1], 16, width))

    def two(first):
        def step(k, _):
            grads_t(k)
            return 0
        lax.fori_loop(first, first + 2, step, 0)

    n_d = dkv_in.shape[1]
    send(dkv.at[:, pl.ds(pl.multiple_of((1 - f) * n_d, n_d), n_d)], dkv_in, s_d, r_d, partner)
    wp[0](0)
    wp[0](1)
    order = pick_row(meta[8:12, :], c)
    pick = (order == nat).astype(F32).astype(BF)
    place[0] = mm_lt(pick, y[...]).astype(BF).reshape(place.shape[1:])
    acc[...] = dr1[...]
    wp[0](2)
    rows1(0)
    wp[0](3)
    loads[0].wait()
    wp[1](0)
    loads[1].wait()
    wp[1](1)
    arrived(dkv_in, r_d)
    two(0)
    rows2(0)
    wp[2](0)
    loads[2].wait()
    wp[1](2)
    two(2)
    wp[2](1)
    wp[3](0)
    loads[3].wait()
    wp[1](3)
    rows3(0)
    for i in range(4):
        ap[0](i)
    lane = lax.broadcasted_iota(jnp.int32, (1, n_n), 1)
    at = ((lane // block) % 4) * (4 * block) + (lane // (4 * block)) * block + lane % block
    pick2 = (at == nat).astype(F32).astype(BF)
    place[1] = mm_lt(pick2, acc[...].astype(BF)).astype(BF).reshape(place.shape[1:])
    wp[2](2)
    wp[3](1)
    rows1(1)
    ap[1](0)
    wp[2](3)
    wp[3](2)
    rows2(1)
    ap[1](1)
    ap[2](0)
    wp[3](3)
    rows3(1)
    ap[1](2)
    ap[2](1)
    ap[3](0)
    ap[1](3)
    wp[4](tot_w, sem_l.at[7])
    ap[2](2)
    ap[3](1)
    ap[2](3)
    ap[3](2)
    ap[3](3)
    ap[4](tot_a, sem_l.at[8])

    for ten in range(2):
        for i in range(4):
            cc = (c + i) % 4
            if i == 0:
                @pl.when(jnp.logical_not(stays))
                def _(ten=ten, cc=cc):
                    arrived(rows_out.at[ten, cc], r_o.at[ten, cc])
                pl.when(stays)(moves[ten].wait)
            else:
                arrived(rows_out.at[ten, cc], r_o.at[ten, cc])
    for pred, d in pending:
        if pred is None:
            d.wait_send()
        else:
            pl.when(pred)(d.wait_send)


def tail_out(gath, meta, dq, dkv, xm, da, op, dr1, y, vec, gg):
    n_t, n_fc, rows, width = gath.shape
    wl = rows - 16
    r_n = xm.shape[0]
    block = r_n // 4
    v = pltpu.VMEM
    dma = pltpu.SemaphoreType.DMA
    vm = pl.BlockSpec(memory_space=pltpu.VMEM)
    any_ = pl.BlockSpec(memory_space=pl.ANY)
    ra, rw = wl + 16, 2 * wl
    def bufs(n):
        return [v((4, 4, n, width), BF), v((4, 2, n, width), BF), v((4, n, width), BF), v((4, n, width), BF)]
    pass_sems = [dma((4, 4)), dma((4, 4)), dma((2, 2, 4)), dma((2, 2, 4)), dma((2, 4)), dma((2, 4)), dma((4,)), dma((4,))]
    return pl.pallas_call(
        tail_out_kernel,
        out_shape=(jax.ShapeDtypeStruct((ra, width), F32), jax.ShapeDtypeStruct((rw, width), F32),
                   jax.ShapeDtypeStruct((2, 4, block, width), BF)),
        in_specs=[vm] * 10 + [any_],
        out_specs=(vm, vm, vm),
        scratch_shapes=[v((n_t, n_fc, ra, width), BF), v((r_n, width), F32),
                        v((r_n, width), BF), v((n_t, r_n, dkv.shape[2]), BF), v((2, 4, 4, block, width), BF),
                        v((2, 2, 4, block, width), BF), v((2, 4, block, width), BF), v((4, 4, rw, width), BF)]
        + bufs(rw) + bufs(ra)
        + [dma((9,)), dma, dma, dma((2, 2)), dma((2, 2)), dma((2, 4)), dma((2, 4))] + pass_sems + pass_sems,
        compiler_params=pltpu.CompilerParams(collective_id=2, has_side_effects=True, vmem_limit_bytes=VMEM_MAX),
        name="tail_out",
    )(gath, meta, dq, dkv, xm, da, op, dr1, y, vec, gg)


def quad_body(tokens_in, cotangent, seq_lengths, row_order, w_query, b_query, w_key, w_value, b_value,
              w_out, b_out, mid_gain, mid_shift, w_up, b_up, w_down, b_down, end_gain, end_shift):
    f, c = lax.axis_index("fsdp"), lax.axis_index("ctx")
    fc = f * 4 + c
    own, width = tokens_in.shape[1:]
    wl = w_query.shape[0]
    heads_l, head_l = b_query.shape
    head = head_l * 8
    up_l = b_up.shape[1]
    hw = width // 4
    mat_a = jnp.concatenate([w_out, w_query, w_key, w_value], axis=1)

    vecs = jnp.stack([b_out, mid_gain, mid_shift, b_down, end_gain, end_shift])
    col = lax.broadcasted_iota(jnp.int32, (1, width), 1)
    row_v = jnp.where(col // wl == fc, jnp.tile(vecs, (1, 8)), 0)
    part = (col % head) // head_l == fc
    three = jnp.stack([jnp.zeros_like(b_query), b_query, jnp.zeros_like(b_query), b_value])
    row_a = jnp.where(part, jnp.tile(three, (1, 1, 8)).reshape(1, width), 0)
    row_u = jnp.where((col % (8 * up_l)) // up_l == fc, jnp.tile(b_up, (1, 8)).reshape(1, width), 0)
    small = jnp.concatenate([row_v, row_a, row_u, jnp.zeros((8, width), BF)], axis=0)
    pack = jnp.concatenate([mat_a, small], axis=0)

    order = row_order[:, 0]
    n_n = order.shape[1]
    moved = order.reshape(4, 4, 4, own).transpose(0, 2, 1, 3).reshape(4, n_n)
    lens = jnp.pad(seq_lengths[:, 0].reshape(1, -1), ((0, 3), (0, n_n - 12)))
    meta_own = jnp.concatenate([order, lens, moved, jnp.zeros((4, n_n), jnp.int32)], axis=0)

    ga, gg, meta, dq, dkv, xm, da, op, dr1, y, vec = main_in(tokens_in, cotangent, pack, meta_own, w_up, w_down, head)
    tot_a, tot_w, rows = tail_out(ga, meta, dq, dkv, xm, da, op, dr1, y, vec, gg)

    g_a, g_up, g_down = tot_a[:wl], tot_w[:wl], tot_w[wl:]
    sv = lax.dynamic_slice(tot_a[wl:wl + 6], (0, fc * wl), (6, wl))
    ba = tot_a[wl + 6].reshape(4, heads_l, head)
    gb = lax.dynamic_slice(ba, (0, 0, fc * head_l), (4, heads_l, head_l))
    gu = lax.dynamic_slice(tot_a[wl + 7].reshape(heads_l, -1), (0, fc * up_l), (heads_l, up_l))
    return (rows[0], rows[1], g_a[:, hw:2 * hw], gb[1], g_a[:, 2 * hw:3 * hw], g_a[:, 3 * hw:], gb[3], g_a[:, :hw],
            sv[0], sv[1], sv[2], g_up, gu, g_down, sv[3], sv[4], sv[5])


def solution(mesh):
    ins, outs = specs()
    small_mesh = (mesh.shape["fsdp"], mesh.shape["ctx"], mesh.shape["tp"]) == (2, 4, 4)
    fn = quad_body if small_mesh else body
    return jax.shard_map(fn, mesh=mesh, in_specs=ins, out_specs=outs, check_vma=False)
```

```python
import functools

import jax
import jax.numpy as jnp
from jax import lax
from jax.experimental import pallas as pl
from jax.experimental.pallas import tpu as pltpu
from jax.sharding import PartitionSpec as P

EPS = 1e-06
MASKED = -1e30
ALL = ("fsdp", "ctx", "tp")
ROWS = ("fsdp", "ctx")
BF = jnp.bfloat16
F32 = jnp.float32


MESH = pl.DeviceIdType.MESH
def mm(a, b):
    return jnp.dot(a, b, preferred_element_type=F32)


def mm_rt(a, b):
    return lax.dot_general(a, b, (((1,), (1,)), ((), ())), preferred_element_type=F32)


def mm_lt(a, b):
    return lax.dot_general(a, b, (((0,), (0,)), ((), ())), preferred_element_type=F32)


def norm(u):
    centre = u - jnp.mean(u, axis=-1, keepdims=True)
    inv = lax.rsqrt(jnp.mean(centre * centre, axis=-1, keepdims=True) + EPS)
    return centre * inv, inv


def norm_back(d, gain, n, inv):
    e = d * gain
    return (e - jnp.mean(e, axis=-1, keepdims=True) - n * jnp.mean(e * n, axis=-1, keepdims=True)) * inv


def phi_both(u):
    cdf = 0.5 * (1.0 + lax.erf(u * 0.7071067811865476))
    pdf = 0.3989422804014327 * jnp.exp(-0.5 * u * u)
    return cdf, pdf


def gather_group(block):
    width = block.shape[-1]
    mine = lax.all_to_all(block, "ctx", 0, 0, tiled=True)
    whole = lax.all_gather(mine, "tp", axis=1, tiled=False)
    return whole.reshape(-1, width)


def scatter_group(rows, own_rows):
    ctx_n, tp_n = lax.axis_size("ctx"), lax.axis_size("tp")
    width = rows.shape[-1]
    blocks = rows.reshape(ctx_n, tp_n * own_rows, width)
    mine = lax.psum_scatter(blocks, "tp", scatter_dimension=1, tiled=True)
    return lax.all_to_all(mine, "ctx", 0, 0, tiled=True)


def body(tokens_in, cotangent, seq_lengths, row_order, w_query, b_query, w_key, w_value, b_value,
         w_out, b_out, mid_gain, mid_shift, w_up, b_up, w_down, b_down, end_gain, end_shift):
    ctx_n, tp_n, fsdp_n = lax.axis_size("ctx"), lax.axis_size("tp"), lax.axis_size("fsdp")
    rows_n = ctx_n * fsdp_n
    c, t = lax.axis_index("ctx"), lax.axis_index("tp")
    micro, own_rows, width = tokens_in.shape
    group_rows = own_rows * ctx_n * tp_n
    half_rows = group_rows // 2
    parts = tp_n // 2
    my_rows = half_rows // parts
    half, quarter = t // parts, t % parts
    heads_l, head_l = b_query.shape
    heads, head = heads_l * tp_n, head_l * rows_n

    mats = (w_query, w_key, w_value, w_out, w_up, w_down)
    widths = [m.shape[1] for m in mats]
    packed = lax.all_gather(jnp.concatenate(mats, axis=1), ALL, axis=0, tiled=False)
    full, at = [], 0
    for wd in widths:
        piece = packed[:, :, at:at + wd].reshape(rows_n, tp_n, -1, wd)
        full.append(piece.transpose(0, 2, 1, 3).reshape(width, tp_n * wd))
        at += wd
    wq, wk, wv, wo, wu, wd_ = full
    vecs = (b_out, mid_gain, mid_shift, b_down, end_gain, end_shift)
    bias = (b_query, b_value, b_up)
    vec_all = lax.all_gather(jnp.stack(vecs), ROWS, axis=1, tiled=True).astype(F32)
    bias_all = lax.all_gather(jnp.concatenate(bias, axis=1), ALL, axis=0, tiled=False).astype(F32)

    def whole_bias(at, wd):
        piece = bias_all[:, :, at:at + wd].reshape(rows_n, tp_n, heads_l, wd)
        return piece.transpose(1, 2, 0, 3).reshape(-1)

    bq = whole_bias(0, head_l)
    bv = whole_bias(head_l, head_l)
    bu = whole_bias(2 * head_l, b_up.shape[1])
    bo, mg, ms, bd, eg, es = (vec_all[i] for i in range(6))

    lens = lax.dynamic_index_in_dim(seq_lengths[:, 0], c, 0, keepdims=False)
    order = lax.dynamic_index_in_dim(row_order[:, 0], c, 0, keepdims=False)
    places = lax.iota(jnp.int32, lens.shape[0])
    longest = jnp.argmax(lens)
    first = jnp.sum(jnp.where(places < longest, lens, 0))
    start = lax.rem(first + half * half_rows, group_rows)
    ends = jnp.cumsum(lens)
    nat = lax.rem(start + lax.iota(jnp.int32, half_rows), group_rows)
    seg = jnp.sum((ends[None, :] <= nat[:, None]).astype(jnp.int32), axis=1)
    q_at = quarter * my_rows
    nat_q = lax.dynamic_slice_in_dim(nat, q_at, my_rows)
    seg_q = lax.dynamic_slice_in_dim(seg, q_at, my_rows)

    x_group = gather_group(tokens_in)
    c_group = gather_group(cotangent)
    x_twice = jnp.concatenate([x_group, x_group[:half_rows]], axis=0)
    x_half = lax.dynamic_slice_in_dim(x_twice, start, half_rows, 0)
    x_mine = lax.dynamic_slice_in_dim(x_half, q_at, my_rows, 0)
    pick = (order[:, None] == nat_q[None, :]).astype(BF)
    pick_nat = (lax.iota(jnp.int32, group_rows)[:, None] == nat_q[None, :]).astype(BF)
    dy = mm_lt(pick, c_group)

    x = x_mine.astype(F32)
    q = (mm(x_mine, wq) + bq).astype(BF).reshape(my_rows, heads, head)
    k = mm(x_half, wk).astype(BF).reshape(half_rows, heads, head)
    v = (mm(x_half, wv) + bv).astype(BF).reshape(half_rows, heads, head)
    same = seg_q[:, None] == seg[None, :]
    s = jnp.einsum("qhd,khd->hqk", q, k, preferred_element_type=F32) * 0.125
    s = jnp.where(same[None], s, MASKED)
    p = jnp.exp(s - jnp.max(s, axis=-1, keepdims=True))
    p = p / jnp.sum(p, axis=-1, keepdims=True)
    pb = p.astype(BF)
    o = jnp.einsum("hqk,khd->qhd", pb, v, preferred_element_type=F32).astype(BF)
    o2 = o.reshape(my_rows, heads * head)
    r1 = x + mm_rt(o2, wo) + bo
    n1, inv1 = norm(r1)
    middle = n1 * mg + ms
    mid_b = middle.astype(BF)
    pre = mm(mid_b, wu) + bu
    cdf, pdf = phi_both(pre)
    act = (pre * cdf).astype(BF)
    r2 = middle + mm_rt(act, wd_) + bd
    n2, inv2 = norm(r2)
    y = n2 * eg + es

    d_r2 = norm_back(dy, eg, n2, inv2)
    df = d_r2.astype(BF)
    d_pre = (mm(df, wd_) * (cdf + pre * pdf)).astype(BF)
    g_down = mm_lt(df, act)
    g_up = mm_lt(mid_b, d_pre)
    d_mid = d_r2 + mm_rt(d_pre, wu)
    d_r1 = norm_back(d_mid, mg, n1, inv1)
    da = d_r1.astype(BF)
    g_out = mm_lt(da, o2)
    d_o = mm(da, wo).astype(BF).reshape(my_rows, heads, head)
    dp = jnp.einsum("qhd,khd->hqk", d_o, v, preferred_element_type=F32)
    ds = (p * (dp - jnp.sum(p * dp, axis=-1, keepdims=True))).astype(BF)
    d_q = (jnp.einsum("hqk,khd->qhd", ds, k, preferred_element_type=F32) * 0.125).astype(BF)
    d_k = jnp.einsum("hqk,qhd->khd", ds, q, preferred_element_type=F32) * 0.125
    d_v = jnp.einsum("hqk,qhd->khd", pb, d_o, preferred_element_type=F32)
    d_q = d_q.reshape(my_rows, heads * head)
    d_kv = jnp.concatenate([d_k.reshape(half_rows, -1), d_v.reshape(half_rows, -1)], axis=1).astype(BF)
    pairs = [[h * parts + j for j in range(parts)] for h in range(tp_n // parts)]
    d_kv = lax.psum_scatter(d_kv.astype(F32), "tp", scatter_dimension=0, tiled=True, axis_index_groups=pairs)
    d_k, d_v = jnp.split(d_kv.astype(BF), 2, axis=1)
    g_q = mm_lt(x_mine, d_q)
    g_k = mm_lt(x_mine, d_k)
    g_v = mm_lt(x_mine, d_v)
    d_x = (d_r1 + mm_rt(d_q, wq) + mm_rt(d_k, wk) + mm_rt(d_v, wv)).astype(BF)

    layer_out = scatter_group(mm(pick, y.astype(BF)).astype(BF), own_rows)
    input_grad = scatter_group(mm(pick_nat, d_x).astype(BF), own_rows)

    outs = []
    for g, wd in zip((g_q, g_k, g_v, g_out, g_up, g_down), widths):
        outs.append(g.astype(BF).reshape(rows_n, width // rows_n, tp_n, wd).transpose(0, 2, 1, 3))
    packed_g = jnp.concatenate(outs, axis=3)
    packed_g = packed_g.reshape(rows_n * tp_n, width // rows_n, -1)
    mine_g = lax.psum_scatter(packed_g, ALL, scatter_dimension=0, tiled=True)[0].astype(F32)
    gm, at = [], 0
    for wd in widths:
        gm.append(mine_g[:, at:at + wd])
        at += wd

    def total(a):
        return jnp.sum(a.astype(F32), axis=0)

    def split_bias(a, wd):
        return a.reshape(tp_n, heads_l, rows_n, wd).transpose(2, 0, 1, 3).reshape(rows_n * tp_n, heads_l, wd)

    small_b = jnp.concatenate([
        split_bias(total(d_q), head_l), split_bias(total(d_v), head_l), split_bias(total(d_pre), b_up.shape[1])],
        axis=2).reshape(rows_n * tp_n, -1)
    vec_g = jnp.stack([total(d_r1), total(d_mid * n1), total(d_mid), total(d_r2), total(dy * n2), total(dy)])
    small_v = vec_g.reshape(6, rows_n, 1, width // rows_n).transpose(1, 2, 0, 3)
    small_v = jnp.broadcast_to(small_v, (rows_n, tp_n, 6, width // rows_n)).reshape(rows_n * tp_n, -1)
    small = jnp.concatenate([small_b, small_v], axis=1)
    small = lax.psum_scatter(small, ALL, scatter_dimension=0, tiled=True)[0]
    nb = small_b.shape[1]
    sb = small[:nb].reshape(heads_l, -1)
    sv = small[nb:].reshape(6, -1)
    return (layer_out, input_grad, gm[0], sb[:, :head_l], gm[1], gm[2], sb[:, head_l:2 * head_l], gm[3],
            sv[0], sv[1], sv[2], gm[4], sb[:, 2 * head_l:], gm[5], sv[3], sv[4], sv[5])


def specs():
    tok = P(None, ALL, None)
    grp = P(None, "fsdp", None)
    mat = P(ROWS, "tp")
    bias = P("tp", ROWS)
    vec = P(ROWS)
    ins = (tok, tok, grp, grp, mat, bias, mat, mat, bias, mat, vec, vec, vec, mat, bias, mat, vec, vec, vec)
    return ins, (tok, tok) + ins[4:]


CHUNK = 32
VMEM_MAX = 62 * 1024 * 1024


def row_facts(meta, group_n):
    c, t = lax.axis_index("ctx"), lax.axis_index("tp")
    lens = meta[4:5, :].astype(F32)
    lane = lax.broadcasted_iota(jnp.int32, lens.shape, 1)

    def one(k):
        return jnp.sum(jnp.where(lane == 3 * c + k, lens, 0.0), axis=1, keepdims=True).astype(jnp.int32)

    l0, l1 = one(0), one(1)
    half = group_n // 2
    first = jnp.where(l0 == half, 0, jnp.where(l1 == half, l0, l0 + l1))
    return first + (t % 2) * half, l0, l0 + l1


def wrap(v, group_n):
    return jnp.where(v >= group_n, v - group_n, v)


def pick_row(block, c):
    row = lax.broadcasted_iota(jnp.int32, block.shape, 0)
    return jnp.sum(jnp.where(row == c, block.astype(F32), 0.0), axis=0, keepdims=True).astype(jnp.int32)


def chunks(total, fn, size=CHUNK):
    def step(i, _):
        fn(pl.ds(pl.multiple_of(i * size, size), size))
        return 0
    lax.fori_loop(0, total // size, step, 0)


def each_t(fn):
    def step(t, _):
        fn(t)
        return 0
    lax.fori_loop(0, 4, step, 0)


def main_in_kernel(head, tok, cot, pack, meta, up, down, ga, gg, meta_all, dq_out, dkv_out, xm_out, da_out, op_out, dr1_out, y_out, vec_out,
                   gu, group, held, xh, dy, qkv, probs, sbuf, pb, pb2, acc, midb, n1, inv1, gelu_d, act, n2, df, big, bias,
                   g_u, g_d, sem_l, s_e, r_e, s_xg, r_xg, s_xf, s_m, r_m, *pass_sems):
    f, c, t_me = lax.axis_index("fsdp"), lax.axis_index("ctx"), lax.axis_index("tp")
    width = xh.shape[1]
    s_n, r_n = xh.shape[0], dy.shape[0]
    n_n = 2 * s_n
    wl = (gu.shape[2]) // 2
    hw = width // 4
    per_t = hw // head
    partner = (1 - f, c, t_me)
    slot = f * 4 + c
    cx = c + 1 - 2 * (c % 2)
    cy = (c + 2) % 4
    cd = (cx + 2) % 4
    x_nb, y_nb = (f, cx, t_me), (f, cy, t_me)
    near, far = 1 + f, 3 * f
    is_near = t_me == near
    receiver = (t_me // 2) == f

    barrier = pltpu.get_barrier_semaphore()
    peers = [partner] + [(f, (c + i) % 4, t_me) for i in (1, 2, 3)] + [(f, c, (t_me + i) % 4) for i in (1, 2, 3)]
    for p in peers:
        pl.semaphore_signal(barrier, inc=1, device_id=p, device_id_type=MESH)
    pl.semaphore_wait(barrier, len(peers))

    pending = []

    def send(src, dst, ssem, rsem, dev, pred=None):
        d = pltpu.make_async_remote_copy(src_ref=src, dst_ref=dst, send_sem=ssem, recv_sem=rsem,
                                         device_id=dev, device_id_type=MESH)
        if pred is None:
            d.start()
        else:
            pl.when(pred)(d.start)
        pending.append((pred, d))

    def arrived(dst, rsem, pred=None):
        d = pltpu.make_async_remote_copy(src_ref=dst, dst_ref=dst, send_sem=s_e.at[0, 0], recv_sem=rsem,
                                         device_id=partner, device_id_type=MESH)
        if pred is None:
            d.wait_recv()
        else:
            pl.when(pred)(d.wait_recv)

    def first_sends(ten, ref):
        for i in (1, 2, 3):
            to = (c + i) % 4
            send(ref.at[to], held.at[ten, c], s_e.at[ten, i], r_e.at[ten, c], (f, to, t_me))

    a_rows = ga.shape[2]
    w_rows = gu.shape[2]
    own_a, own_w = pack, gu.at[t_me, slot]
    shards = [pltpu.make_async_copy(up, gu.at[t_me, slot, pl.ds(0, wl)], sem_l.at[3]),
              pltpu.make_async_copy(down, gu.at[t_me, slot, pl.ds(wl, wl)], sem_l.at[9])]
    first_sends(0, tok)
    local = [pltpu.make_async_copy(tok.at[c], held.at[0, c], sem_l.at[0]),
             pltpu.make_async_copy(cot.at[c], held.at[1, c], sem_l.at[1]),
             pltpu.make_async_copy(own_a, ga.at[t_me, slot], sem_l.at[2]),
             pltpu.make_async_copy(meta, meta_all.at[f], sem_l.at[8])]
    for d in local + shards:
        d.start()
    send(meta, meta_all.at[f], s_m.at[0], r_m.at[0], partner)

    columns = [(t_me, None)]
    for d in (1, 2, 3):
        columns.append(((t_me - d + 4) % 4, t_me - d >= 0))
        columns.append(((t_me + d) % 4, t_me + d <= 3))

    def make_gather(gath, own, cut, sems):
        (s_z, r_z, s_x0, r_x0, s_y0, r_y0, s_y1, r_y1, s_x1, r_x1, s_c, r_c, s_c0, r_c0, s_c1, r_c1) = sems
        rows = gath.shape[2]
        h0, h1 = pl.ds(0, cut), pl.ds(cut, rows - cut)

        def have_column(src, tt, pred=None):
            send(src.at[h0], gath.at[tt, slot, h0], s_x0.at[tt], r_x0.at[tt], x_nb, pred)
            send(src.at[h1], gath.at[tt, slot, h1], s_y1.at[tt], r_y1.at[tt], y_nb, pred)
            send(src.at[h0], gath.at[tt, slot, h0], s_y0.at[0, tt], r_y0.at[0, tt], y_nb, pred)
            send(src.at[h1], gath.at[tt, slot, h1], s_x1.at[0, tt], r_x1.at[0, tt], x_nb, pred)
            send(src, gath.at[tt, slot], s_c.at[tt], r_c.at[tt], partner, pred)

        def begin():
            send(own, gath.at[t_me, slot], s_z.at[0, t_me], r_z.at[t_me], (f, c, (t_me + 1) % 4), t_me < 3)
            send(own, gath.at[t_me, slot], s_z.at[1, t_me], r_z.at[t_me], (f, c, (t_me + 3) % 4), t_me > 0)
            have_column(own, t_me)

        def z_step(d):
            for sign in (-1, 1):
                tt = t_me + sign * d
                there = tt >= 0 if sign < 0 else tt <= 3
                tt = (tt + 4) % 4
                arrived(gath.at[tt, slot], r_z.at[tt], there)
                on = t_me < 3 if sign < 0 else t_me > 0
                nxt = (t_me + 1) % 4 if sign < 0 else (t_me + 3) % 4
                if d < 3:
                    send(gath.at[tt, slot], gath.at[tt, slot], s_z.at[0 if sign < 0 else 1, tt], r_z.at[tt],
                         (f, c, nxt), jnp.logical_and(there, on))
                have_column(gath.at[tt, slot], tt, there)

        def mid_step(i):
            tt, pred = columns[i]
            a = gath.at[tt, f * 4 + cx, h0]
            arrived(a, r_x0.at[tt], pred)
            send(a, a, s_y0.at[1, tt], r_y0.at[1, tt], y_nb, pred)
            send(a, a, s_c0.at[0, tt], r_c0.at[0, tt], partner, pred)
            b = gath.at[tt, f * 4 + cy, h1]
            arrived(b, r_y1.at[tt], pred)
            send(b, b, s_x1.at[1, tt], r_x1.at[1, tt], x_nb, pred)
            send(b, b, s_c1.at[0, tt], r_c1.at[0, tt], partner, pred)

        def late_step(step, i):
            tt, pred = columns[i]
            a = gath.at[tt, f * 4 + (cy if step == 0 else cd), h0]
            arrived(a, r_y0.at[step, tt], pred)
            send(a, a, s_c0.at[1 + step, tt], r_c0.at[1 + step, tt], partner, pred)
            b = gath.at[tt, f * 4 + (cx if step == 0 else cd), h1]
            arrived(b, r_x1.at[step, tt], pred)
            send(b, b, s_c1.at[1 + step, tt], r_c1.at[1 + step, tt], partner, pred)

        def finish():
            other = (1 - f) * 4
            for tt in range(4):
                arrived(gath.at[tt, other + c], r_c.at[tt])
                for j, cc in enumerate((cx, cy, cd)):
                    arrived(gath.at[tt, other + cc, h0], r_c0.at[j, tt])
                for j, cc in enumerate((cy, cx, cd)):
                    arrived(gath.at[tt, other + cc, h1], r_c1.at[j, tt])
        return begin, z_step, mid_step, late_step, finish

    half_sems = len(pass_sems) // 2
    a_begin, a_z, a_mid, a_late, a_finish = make_gather(ga, own_a, (a_rows // 32) * 16, pass_sems[:half_sems])
    w_begin, w_z, w_mid, w_late, w_finish = make_gather(gu, own_w, w_rows // 2, pass_sems[half_sems:])

    def second_sends(ten):
        local[ten].wait()
        for i in (1, 2, 3):
            frm = (c + i) % 4
            arrived(held.at[ten, frm], r_e.at[ten, frm])
        blk = held.at[ten]
        dst = group.at[ten, :, t_me]
        to = jnp.where(is_near, far, near)
        send(blk, dst, s_xg.at[ten, t_me], r_xg.at[ten, t_me], (f, c, to))
        send(blk, dst, s_xf.at[ten, t_me], r_xg.at[ten, t_me], partner, receiver)
        keep = pltpu.make_async_copy(blk, dst, sem_l.at[4 + ten])
        pl.when(receiver)(keep.start)
        return keep

    def relay(ten):
        for i in (1, 2, 3):
            tt = (t_me + i) % 4
            arrived(group.at[ten, :, tt], r_xg.at[ten, tt], receiver)
            send(group.at[ten, :, tt], group.at[ten, :, tt], s_xg.at[ten, tt], r_xg.at[ten, tt], (f, c, far),
                 jnp.logical_and(is_near, tt != far))
            send(group.at[ten, :, tt], group.at[ten, :, tt], s_xf.at[ten, tt], r_xg.at[ten, tt], partner, receiver)

    def rows_here(ten, keep):
        for tt in range(4):
            arrived(group.at[ten, :, tt], r_xg.at[ten, tt], jnp.logical_not(receiver))
        pl.when(receiver)(keep.wait)

    def mat_of(ref, t, at):
        return ref[t, :, at:at + wl, :].reshape(ref.shape[1] * wl, width)

    a_begin()
    keep0 = second_sends(0)
    a_z(1)
    for d in shards:
        d.wait()
    w_begin()
    relay(0)
    a_z(2)
    first_sends(1, cot)
    a_z(3)
    for i in range(5):
        a_mid(i)
    w_z(1)
    for i in range(5, 7):
        a_mid(i)
    for i in range(7):
        a_late(0, i)
    w_z(2)
    for i in range(7):
        a_late(1, i)
    keep1 = second_sends(1)
    rows_here(0, keep0)
    arrived(meta_all.at[1 - f], r_m.at[0])
    local[3].wait()

    meta = meta_all[t_me // 2]
    start, e0, e1 = row_facts(meta, n_n)
    order = pick_row(meta[0:4, :], c)
    mine = pl.ds(pl.multiple_of(f * r_n, r_n), r_n)

    def half_rows(rows):
        nat = wrap(start + rows.start + lax.broadcasted_iota(jnp.int32, (rows.size, 1), 0), n_n)
        sel = (lax.broadcasted_iota(jnp.int32, (rows.size, n_n), 1) == nat).astype(F32).astype(BF)
        xh[rows, :] = mm(sel, group[0].reshape(n_n, width)).astype(BF)
    chunks(s_n, half_rows, 128)
    a_finish()
    local[2].wait()
    for t in range(4):
        bias[t] = jnp.sum(ga[t, :, wl:wl + 16, :].astype(F32), axis=0)
    vec = bias[0]
    bo, mg, ms, bd, eg, es = (vec[i:i + 1, :] for i in range(6))
    nat_row = wrap(start + lax.broadcasted_iota(jnp.int32, (1, s_n), 1), n_n)
    seg_row = (nat_row >= e0).astype(jnp.int32) + (nat_row >= e1).astype(jnp.int32)
    nat_q = wrap(start + f * r_n + lax.broadcasted_iota(jnp.int32, (r_n, 1), 0), n_n)
    same = ((nat_q >= e0).astype(jnp.int32) + (nat_q >= e1).astype(jnp.int32)) == seg_row

    def forward_t(t):
        row6 = bias[t][6:7, :]
        qkv[t] = (mm(xh[...], mat_of(ga, t, 0)) + row6).astype(BF)
        q3 = qkv[t, mine, :]
        kv = qkv[t]
        outs = []
        for h in range(per_t):
            lo = hw + h * head
            sbuf[...] = mm_rt(q3[:, lo:lo + head], kv[:, lo + hw:lo + hw + head])
            at = t * per_t + h

            s = jnp.where(same, sbuf[...] * 0.125, MASKED)
            p = jnp.exp(s - jnp.max(s, axis=1, keepdims=True))
            p = p * (1.0 / jnp.sum(p, axis=1, keepdims=True))
            probs[at] = p
            pb[...] = p.astype(BF)
            outs.append(mm(pb[...], kv[:, lo + 2 * hw:lo + 2 * hw + head]).astype(BF))
        outs.append(jnp.zeros((r_n, width - hw), BF))
        op_out[t] = jnp.concatenate(outs, axis=1)

    def two(first, fn):
        def step(t, _):
            fn(t)
            return 0
        lax.fori_loop(first, first + 2, step, 0)

    relay(1)
    two(0, forward_t)
    w_z(3)
    w_mid(0)
    w_mid(1)
    w_mid(2)
    two(2, forward_t)
    for i in range(3, 7):
        w_mid(i)
    xm_out[...] = xh[mine, :]
    acc[...] = xm_out[...].astype(F32) + bo

    def out_t(t):
        acc[...] += mm_rt(op_out[t], mat_of(ga, t, 0))
    each_t(out_t)
    w_late(0, 0)
    w_late(0, 1)
    w_late(0, 2)

    def norm_rows(u):
        centre = u - jnp.mean(u, axis=-1, keepdims=True)
        inv = lax.rsqrt(jnp.mean(centre * centre, axis=-1, keepdims=True) + EPS)
        return centre * inv, inv

    def first_norm(rows):
        n, inv = norm_rows(acc[rows, :])
        n1[rows, :] = n
        inv1[rows, :] = jnp.broadcast_to(inv, (rows.size, 128))
        m = n * mg + ms
        midb[rows, :] = m.astype(BF)
        acc[rows, :] = m + bd
    chunks(r_n, first_norm)
    rows_here(1, keep1)

    def quarter_rows(rows):
        nat = wrap(start + f * r_n + rows.start + lax.broadcasted_iota(jnp.int32, (rows.size, 1), 0), n_n)
        sel = (order == nat).astype(F32).astype(BF)
        dy[rows, :] = mm(sel, group[1].reshape(n_n, width))
    chunks(r_n, quarter_rows, 128)
    for i in range(3, 7):
        w_late(0, i)
    for i in range(7):
        w_late(1, i)
    w_finish()

    def ffn_t(t):
        row7 = bias[t][7:8, :]
        big[...] = mm(midb[...], mat_of(gu, t, 0))

        def gelu(rows):
            u = big[rows, :] + row7
            cdf = 0.5 * (1.0 + lax.erf(u * 0.7071067811865476))
            pdf = 0.3989422804014327 * jnp.exp(-0.5 * u * u)
            act[t, rows, :] = (u * cdf).astype(BF)
            gelu_d[t, rows, :] = cdf + u * pdf
        chunks(r_n, gelu, 16)
        acc[...] += mm_rt(act[t], mat_of(gu, t, wl))
    each_t(ffn_t)

    vec_out[...] = jnp.zeros_like(vec_out)

    def add_vec(i, v):
        vec_out[i] += jnp.sum(v.reshape(-1, 8, v.shape[1]), axis=0)

    def second_norm(rows):
        n, inv = norm_rows(acc[rows, :])
        y_out[rows, :] = (n * eg + es).astype(BF)
        g = dy[rows, :]
        e = g * eg
        d = (e - jnp.mean(e, axis=-1, keepdims=True) - n * jnp.mean(e * n, axis=-1, keepdims=True)) * inv
        add_vec(3, d)
        add_vec(4, g * n)
        add_vec(5, g)
        df[rows, :] = d.astype(BF)
        acc[rows, :] = d
    chunks(r_n, second_norm)

    def ffn_back_t(t):
        big[...] = mm(df[...], mat_of(gu, t, wl))

        def times(rows):
            d = (big[rows, :] * gelu_d[t, rows, :]).astype(BF)
            n2[rows, :] = d
            add_vec(8 + t, d.astype(F32))
        chunks(r_n, times)
        acc[...] += mm_rt(n2[...], mat_of(gu, t, 0))
        g_d[t] = mm_lt(df[...], act[t]).astype(BF).reshape(g_d.shape[1:])
        g_u[t] = mm_lt(midb[...], n2[...]).astype(BF).reshape(g_u.shape[1:])
    each_t(ffn_back_t)
    stores = [pltpu.make_async_copy(g_u, gg.at[:, :, pl.ds(0, wl)], sem_l.at[6]),
              pltpu.make_async_copy(g_d, gg.at[:, :, pl.ds(wl, wl)], sem_l.at[7])]
    for d in stores:
        d.start()

    def first_norm_back(rows):
        g, n = acc[rows, :], n1[rows, :]
        e = g * mg
        d = (e - jnp.mean(e, axis=-1, keepdims=True) - n * jnp.mean(e * n, axis=-1, keepdims=True)) * inv1[rows, :][:, 0:1]
        add_vec(0, d)
        add_vec(1, g * n)
        add_vec(2, g)
        dr1_out[rows, :] = d
        da_out[rows, :] = d.astype(BF)
    chunks(r_n, first_norm_back)

    def attn_back_t(t):
        do = mm(da_out[...], mat_of(ga, t, 0)).astype(BF)
        q3 = qkv[t, mine, :]
        kv = qkv[t]
        dqs, dks, dvs = [], [], []
        for h in range(per_t):
            lo = hw + h * head
            at = t * per_t + h
            do_h = do[:, h * head:(h + 1) * head]
            sbuf[...] = mm_rt(do_h, kv[:, lo + 2 * hw:lo + 2 * hw + head])

            p, d = probs[at], sbuf[...]
            pb[...] = (p * (d - jnp.sum(p * d, axis=1, keepdims=True))).astype(BF)
            pb2[...] = p.astype(BF)
            dvs.append(mm_lt(pb2[...], do_h))
            dqs.append(mm(pb[...], kv[:, lo + hw:lo + hw + head]) * 0.125)
            dks.append(mm_lt(pb[...], q3[:, lo:lo + head]) * 0.125)
        dq_out[t] = jnp.concatenate([a.astype(BF) for a in dqs], axis=1)
        dkv_out[t] = jnp.concatenate([a.astype(BF) for a in dks + dvs], axis=1)
    each_t(attn_back_t)
    for d in stores:
        d.wait()


    for pred, d in pending:
        if pred is None:
            d.wait_send()
        else:
            pl.when(pred)(d.wait_send)


def main_in(tok, cot, pack, meta, up, down, head):
    own, width = tok.shape[1:]
    wl = up.shape[0]
    n_n = own * 16
    s_n, r_n = n_n // 2, n_n // 4
    hw = width // 4
    heads = width // head
    v = pltpu.VMEM
    dma = pltpu.SemaphoreType.DMA
    sds = jax.ShapeDtypeStruct
    vm = pl.BlockSpec(memory_space=pltpu.VMEM)
    any_ = pl.BlockSpec(memory_space=pl.ANY)
    wshape = (4, 8, wl, width)
    pass_sems = [dma((2, 4)), dma((4,)), dma((4,)), dma((4,)), dma((2, 4)), dma((2, 4)), dma((4,)), dma((4,)),
                 dma((2, 4)), dma((2, 4)), dma((4,)), dma((4,)), dma((3, 4)), dma((3, 4)), dma((3, 4)), dma((3, 4))]
    return pl.pallas_call(
        functools.partial(main_in_kernel, head),
        out_shape=(sds((4, 8, wl + 16, width), BF), sds((4, 8, 2 * wl, width), BF), sds((2,) + meta.shape, jnp.int32),
                   sds((4, r_n, hw), BF), sds((4, s_n, 2 * hw), BF), sds((r_n, width), BF), sds((r_n, width), BF),
                   sds((4, r_n, width), BF), sds((r_n, width), F32), sds((r_n, width), BF), sds((16, 8, width), F32)),
        in_specs=[any_, any_, vm, vm, any_, any_],
        out_specs=(vm, any_) + (vm,) * 9,
        scratch_shapes=[
            v((4, 8, 2 * wl, width), BF), v((2, 4, 4, own, width), BF), v((2, 4, own, width), BF),
            v((s_n, width), BF), v((r_n, width), F32), v((4, s_n, width), BF), v((heads, r_n, s_n), F32),
            v((r_n, s_n), F32), v((r_n, s_n), BF), v((r_n, s_n), BF), v((r_n, width), F32), v((r_n, width), BF),
            v((r_n, width), F32), v((r_n, 128), F32), v((4, r_n, width), F32), v((4, r_n, width), BF),
            v((r_n, width), BF), v((r_n, width), BF), v((r_n, width), F32), v((4, 16, width), F32),
            v(wshape, BF), v(wshape, BF),
            dma((10,)), dma((2, 4)), dma((2, 4)), dma((2, 4)), dma((2, 4)), dma((2, 4)), dma((1,)), dma((1,))]
        + pass_sems + pass_sems,
        compiler_params=pltpu.CompilerParams(collective_id=0, has_side_effects=True, vmem_limit_bytes=VMEM_MAX),
        name="main_in",
    )(tok, cot, pack, meta, up, down)


def tail_out_kernel(w_a, meta_ref, dq, dkv, xm, da, op, dr1, y, vec, gg, tot_a, tot_w, rows_out,
                    g_a, acc, dqkv, dkv_in, place, pl1, pl2, own, w0, w1, w2, w3, a0, a1, a2, a3,
                    sem_l, s_d, r_d, s_u, r_u, s_o, r_o,
                    ws0, wr0, ws1, wr1, ws2, wr2, ws3, wr3, as0, ar0, as1, ar1, as2, ar2, as3, ar3):
    f, c, t = lax.axis_index("fsdp"), lax.axis_index("ctx"), lax.axis_index("tp")
    r_n, width = xm.shape
    n_n = 4 * r_n
    hw = width // 4
    wl = w_a.shape[2] - 16
    partner = (1 - f, c, t)
    cx = c + 1 - 2 * (c % 2)
    cy = (c + 2) % 4
    cd = (cx + 2) % 4
    x_nb, y_nb = (f, cx, t), (f, cy, t)
    par = t % 2
    z_nb = (f, c, t + 1 - 2 * par)
    to_f, to_t = t // 2, 2 * f + par
    stays = to_f == f

    turn = [(t + 2) % 4, (t + 1) % 4, (t + 3) % 4, t]
    loads = []
    for i, tt in enumerate(turn):
        d = pltpu.make_async_copy(gg.at[tt, pl.ds(pl.multiple_of(f * 4, 4), 4)], own.at[tt], sem_l.at[1 + i])
        d.start()
        loads.append(d)

    barrier = pltpu.get_barrier_semaphore()
    peers = [partner] + [(f, (c + i) % 4, t) for i in (1, 2, 3)] + [(f, c, (t + i) % 4) for i in (1, 2, 3)]
    for p in peers:
        pl.semaphore_signal(barrier, inc=1, device_id=p, device_id_type=MESH)

    @pl.when(jnp.logical_not(stays))
    def _():
        for i in range(4):
            pl.semaphore_signal(barrier, inc=1, device_id=(to_f, (c + i) % 4, to_t), device_id_type=MESH)
        pl.semaphore_wait(barrier, len(peers) + 4)

    @pl.when(stays)
    def _():
        pl.semaphore_wait(barrier, len(peers))

    pending = []

    def send(src, dst, ssem, rsem, dev, pred=None):
        d = pltpu.make_async_remote_copy(src_ref=src, dst_ref=dst, send_sem=ssem, recv_sem=rsem,
                                         device_id=dev, device_id_type=MESH)
        if pred is None:
            d.start()
        else:
            pl.when(pred)(d.start)
        pending.append((pred, d))

    def arrived(dst, rsem):
        pltpu.make_async_remote_copy(src_ref=dst, dst_ref=dst, send_sem=s_d, recv_sem=rsem,
                                     device_id=partner, device_id_type=MESH).wait_recv()

    def add_into(dst, src, off, n):
        def go(i, _):
            r = pl.ds(pl.multiple_of(off + i * 16, 16), 16)
            dst[r, :] = dst[r, :] + src[r, :]
            return 0
        lax.fori_loop(0, n // 16, go, 0)

    def make_pass(mine, theirs, g0, g1, g2, g3, cut, sems):
        q0, p0, q1, p1, q2, p2, q3, p3 = sems
        rows = g0.shape[2]
        h0, h1 = pl.ds(0, cut), pl.ds(cut, rows - cut)

        def roles(i):
            return (cy, cx, y_nb, x_nb) if i % 2 == 0 else (cx, cy, x_nb, y_nb)

        def stage0(i):
            tt = turn[i]
            for k in (1, 2, 3, 0):
                cc = (c + k) % 4
                send(theirs(tt, cc), g0.at[tt, cc], q0.at[tt, cc], p0.at[tt, cc], partner)

        def stage1(i):
            tt = turn[i]
            ca, cb, a_nb, b_nb = roles(i)
            for k in (1, 2, 3, 0):
                cc = (c + k) % 4
                arrived(g0.at[tt, cc], p0.at[tt, cc])
                add_into(mine(tt, cc), g0.at[tt, cc], 0, rows)
            for k, cc in enumerate((ca, cd)):
                send(mine(tt, cc).at[h0], g1.at[tt, k, h0], q1.at[0, k, tt], p1.at[0, k, tt], a_nb)
            for k, cc in enumerate((cb, cd)):
                send(mine(tt, cc).at[h1], g1.at[tt, k, h1], q1.at[1, k, tt], p1.at[1, k, tt], b_nb)

        def stage2(i):
            tt = turn[i]
            ca, cb, a_nb, b_nb = roles(i)
            arrived(g1.at[tt, 1, h0], p1.at[0, 1, tt])
            add_into(mine(tt, cb), g1.at[tt, 1], 0, cut)
            arrived(g1.at[tt, 1, h1], p1.at[1, 1, tt])
            add_into(mine(tt, ca), g1.at[tt, 1], cut, rows - cut)
            send(mine(tt, cb).at[h0], g2.at[tt, h0], q2.at[0, tt], p2.at[0, tt], b_nb)
            send(mine(tt, ca).at[h1], g2.at[tt, h1], q2.at[1, tt], p2.at[1, tt], a_nb)
            arrived(g1.at[tt, 0, h0], p1.at[0, 0, tt])
            add_into(mine(tt, c), g1.at[tt, 0], 0, cut)
            arrived(g1.at[tt, 0, h1], p1.at[1, 0, tt])
            add_into(mine(tt, c), g1.at[tt, 0], cut, rows - cut)

        def stage3(i):
            tt = turn[i]
            arrived(g2.at[tt, h0], p2.at[0, tt])
            arrived(g2.at[tt, h1], p2.at[1, tt])
            add_into(mine(tt, c), g2.at[tt], 0, rows)
            if i < 3:
                send(mine(tt, c), g3.at[t], q3.at[tt], p3.at[t], (f, c, tt))

        def finish(total, ls):
            keep = pltpu.make_async_copy(mine(t, c), g3.at[t], ls)
            keep.start()
            keep.wait()
            for tt in turn[:3]:
                arrived(g3.at[tt], p3.at[tt])

            def go(i, _):
                r = pl.ds(pl.multiple_of(i * 16, 16), 16)
                a, b, e, g = (g3[k, r, :].astype(F32) for k in range(4))
                total[r, :] = ((a + b) + e) + g
                return 0
            lax.fori_loop(0, rows // 16, go, 0)
        return stage0, stage1, stage2, stage3, finish

    wp = make_pass(lambda tt, cc: own.at[tt, cc], lambda tt, cc: gg.at[tt, 4 * (1 - f) + cc],
                   w0, w1, w2, w3, own.shape[2] // 2, (ws0, wr0, ws1, wr1, ws2, wr2, ws3, wr3))
    a_rows = g_a.shape[2]
    ap = make_pass(lambda tt, cc: g_a.at[tt, 4 * f + cc], lambda tt, cc: g_a.at[tt, 4 * (1 - f) + cc],
                   a0, a1, a2, a3, (a_rows // 32) * 16, (as0, ar0, as1, ar1, as2, ar2, as3, ar3))

    lo = pl.multiple_of(2 * f, 2)
    hi = pl.multiple_of(2 - 2 * f, 2)
    block = place.shape[3]
    moves = [pltpu.make_async_copy(pl2.at[ten, c], rows_out.at[ten, c], sem_l.at[5 + ten]) for ten in range(2)]

    def rows1(ten):
        send(place.at[ten, pl.ds(hi, 2)], pl1.at[ten], s_u.at[0, ten], r_u.at[0, ten], partner)

    def rows2(ten):
        arrived(pl1.at[ten], r_u.at[0, ten])
        for k in (0, 1):
            for j in range(4):
                add_into(pl1.at[ten, k, j], place.at[ten, lo + k, j], 0, block)
        send(pl1.at[ten, 1 - par], pl2.at[ten], s_u.at[1, ten], r_u.at[1, ten], z_nb)

    def rows3(ten):
        arrived(pl2.at[ten], r_u.at[1, ten])
        for j in range(4):
            add_into(pl2.at[ten, j], pl1.at[ten, par, j], 0, block)
        for i in range(4):
            cc = (c + i) % 4
            away = jnp.logical_not(stays) if i == 0 else None
            send(pl2.at[ten, cc], rows_out.at[ten, c], s_o.at[ten, i], r_o.at[ten, c], (to_f, cc, to_t), away)
        pl.when(stays)(moves[ten].start)

    meta = meta_ref[t // 2]
    start, _, _ = row_facts(meta, n_n)
    nat = wrap(start + f * r_n + lax.broadcasted_iota(jnp.int32, (r_n, 1), 0), n_n)
    mine_rows = pl.ds(pl.multiple_of(f * r_n, r_n), r_n)
    lane16 = lax.broadcasted_iota(jnp.int32, (16, width), 0)

    def grads_t(k):
        both = (dkv[k, mine_rows, :].astype(F32) + dkv_in[k].astype(F32)).astype(BF)
        dqkv[...] = jnp.concatenate([jnp.zeros((r_n, hw), BF), dq[k], both], axis=1)
        d = dqkv[...]
        acc[...] += mm_rt(d, w_a[k, :, 0:wl, :].reshape(w_a.shape[1] * wl, width))
        g_a[k, :, 0:wl, :] = (mm_lt(xm[...], d) + mm_lt(da[...], op[k])).astype(BF).reshape(g_a.shape[1], wl, width)
        sums = jnp.sum(vec[...], axis=1)
        base = jnp.where(lane16 < 6, sums, 0.0)
        base = base + jnp.where(lane16 == 6, jnp.sum(d.astype(F32), axis=0, keepdims=True), 0.0)
        base = base + jnp.where(lane16 == 7, jnp.sum(vec[8 + k], axis=0, keepdims=True), 0.0)
        g_a[k, :, wl:wl + 16, :] = jnp.broadcast_to(base.astype(BF)[None], (g_a.shape[1], 16, width))

    def two(first):
        def step(k, _):
            grads_t(k)
            return 0
        lax.fori_loop(first, first + 2, step, 0)

    n_d = dkv_in.shape[1]
    send(dkv.at[:, pl.ds(pl.multiple_of((1 - f) * n_d, n_d), n_d)], dkv_in, s_d, r_d, partner)
    wp[0](0)
    wp[0](1)
    wp[0](2)
    wp[0](3)
    loads[0].wait()
    wp[1](0)
    loads[1].wait()
    wp[1](1)
    order = pick_row(meta[8:12, :], c)
    pick = (order == nat).astype(F32).astype(BF)
    place[0] = mm_lt(pick, y[...]).astype(BF).reshape(place.shape[1:])
    acc[...] = dr1[...]
    rows1(0)
    arrived(dkv_in, r_d)
    two(0)
    wp[2](0)
    loads[2].wait()
    wp[1](2)
    two(2)
    for i in range(4):
        ap[0](i)
    rows2(0)
    wp[2](1)
    wp[3](0)
    loads[3].wait()
    wp[1](3)
    lane = lax.broadcasted_iota(jnp.int32, (1, n_n), 1)
    at = ((lane // block) % 4) * (4 * block) + (lane // (4 * block)) * block + lane % block
    pick2 = (at == nat).astype(F32).astype(BF)
    place[1] = mm_lt(pick2, acc[...].astype(BF)).astype(BF).reshape(place.shape[1:])
    rows1(1)
    rows3(0)
    wp[2](2)
    ap[1](0)
    wp[3](1)
    wp[2](3)
    ap[1](1)
    wp[3](2)
    rows2(1)
    ap[1](2)
    ap[2](0)
    ap[1](3)
    wp[3](3)
    rows3(1)
    ap[2](1)
    ap[3](0)
    ap[2](2)
    ap[3](1)
    ap[2](3)
    ap[3](2)
    ap[3](3)
    wp[4](tot_w, sem_l.at[7])
    ap[4](tot_a, sem_l.at[8])

    for ten in range(2):
        for i in range(4):
            cc = (c + i) % 4
            if i == 0:
                @pl.when(jnp.logical_not(stays))
                def _(ten=ten, cc=cc):
                    arrived(rows_out.at[ten, cc], r_o.at[ten, cc])
                pl.when(stays)(moves[ten].wait)
            else:
                arrived(rows_out.at[ten, cc], r_o.at[ten, cc])
    for pred, d in pending:
        if pred is None:
            d.wait_send()
        else:
            pl.when(pred)(d.wait_send)


def tail_out(gath, meta, dq, dkv, xm, da, op, dr1, y, vec, gg):
    n_t, n_fc, rows, width = gath.shape
    wl = rows - 16
    r_n = xm.shape[0]
    block = r_n // 4
    v = pltpu.VMEM
    dma = pltpu.SemaphoreType.DMA
    vm = pl.BlockSpec(memory_space=pltpu.VMEM)
    any_ = pl.BlockSpec(memory_space=pl.ANY)
    ra, rw = wl + 16, 2 * wl
    def bufs(n):
        return [v((4, 4, n, width), BF), v((4, 2, n, width), BF), v((4, n, width), BF), v((4, n, width), BF)]
    pass_sems = [dma((4, 4)), dma((4, 4)), dma((2, 2, 4)), dma((2, 2, 4)), dma((2, 4)), dma((2, 4)), dma((4,)), dma((4,))]
    return pl.pallas_call(
        tail_out_kernel,
        out_shape=(jax.ShapeDtypeStruct((ra, width), F32), jax.ShapeDtypeStruct((rw, width), F32),
                   jax.ShapeDtypeStruct((2, 4, block, width), BF)),
        in_specs=[vm] * 10 + [any_],
        out_specs=(vm, vm, vm),
        scratch_shapes=[v((n_t, n_fc, ra, width), BF), v((r_n, width), F32),
                        v((r_n, width), BF), v((n_t, r_n, dkv.shape[2]), BF), v((2, 4, 4, block, width), BF),
                        v((2, 2, 4, block, width), BF), v((2, 4, block, width), BF), v((4, 4, rw, width), BF)]
        + bufs(rw) + bufs(ra)
        + [dma((9,)), dma, dma, dma((2, 2)), dma((2, 2)), dma((2, 4)), dma((2, 4))] + pass_sems + pass_sems,
        compiler_params=pltpu.CompilerParams(collective_id=2, has_side_effects=True, vmem_limit_bytes=VMEM_MAX),
        name="tail_out",
    )(gath, meta, dq, dkv, xm, da, op, dr1, y, vec, gg)


def quad_body(tokens_in, cotangent, seq_lengths, row_order, w_query, b_query, w_key, w_value, b_value,
              w_out, b_out, mid_gain, mid_shift, w_up, b_up, w_down, b_down, end_gain, end_shift):
    f, c = lax.axis_index("fsdp"), lax.axis_index("ctx")
    fc = f * 4 + c
    own, width = tokens_in.shape[1:]
    wl = w_query.shape[0]
    heads_l, head_l = b_query.shape
    head = head_l * 8
    up_l = b_up.shape[1]
    hw = width // 4
    mat_a = jnp.concatenate([w_out, w_query, w_key, w_value], axis=1)

    vecs = jnp.stack([b_out, mid_gain, mid_shift, b_down, end_gain, end_shift])
    col = lax.broadcasted_iota(jnp.int32, (1, width), 1)
    row_v = jnp.where(col // wl == fc, jnp.tile(vecs, (1, 8)), 0)
    part = (col % head) // head_l == fc
    three = jnp.stack([jnp.zeros_like(b_query), b_query, jnp.zeros_like(b_query), b_value])
    row_a = jnp.where(part, jnp.tile(three, (1, 1, 8)).reshape(1, width), 0)
    row_u = jnp.where((col % (8 * up_l)) // up_l == fc, jnp.tile(b_up, (1, 8)).reshape(1, width), 0)
    small = jnp.concatenate([row_v, row_a, row_u, jnp.zeros((8, width), BF)], axis=0)
    pack = jnp.concatenate([mat_a, small], axis=0)

    order = row_order[:, 0]
    n_n = order.shape[1]
    moved = order.reshape(4, 4, 4, own).transpose(0, 2, 1, 3).reshape(4, n_n)
    lens = jnp.pad(seq_lengths[:, 0].reshape(1, -1), ((0, 3), (0, n_n - 12)))
    meta_own = jnp.concatenate([order, lens, moved, jnp.zeros((4, n_n), jnp.int32)], axis=0)

    ga, gg, meta, dq, dkv, xm, da, op, dr1, y, vec = main_in(tokens_in, cotangent, pack, meta_own, w_up, w_down, head)
    tot_a, tot_w, rows = tail_out(ga, meta, dq, dkv, xm, da, op, dr1, y, vec, gg)

    g_a, g_up, g_down = tot_a[:wl], tot_w[:wl], tot_w[wl:]
    sv = lax.dynamic_slice(tot_a[wl:wl + 6], (0, fc * wl), (6, wl))
    ba = tot_a[wl + 6].reshape(4, heads_l, head)
    gb = lax.dynamic_slice(ba, (0, 0, fc * head_l), (4, heads_l, head_l))
    gu = lax.dynamic_slice(tot_a[wl + 7].reshape(heads_l, -1), (0, fc * up_l), (heads_l, up_l))
    return (rows[0], rows[1], g_a[:, hw:2 * hw], gb[1], g_a[:, 2 * hw:3 * hw], g_a[:, 3 * hw:], gb[3], g_a[:, :hw],
            sv[0], sv[1], sv[2], g_up, gu, g_down, sv[3], sv[4], sv[5])


def solution(mesh):
    ins, outs = specs()
    small_mesh = (mesh.shape["fsdp"], mesh.shape["ctx"], mesh.shape["tp"]) == (2, 4, 4)
    fn = quad_body if small_mesh else body
    return jax.shard_map(fn, mesh=mesh, in_specs=ins, out_specs=outs, check_vma=False)
```
